32 devices in a mesh: layer: 2 (over y), gx: 4 (over z), gy: 4 (over x, core).
Axes of the slice: x: 2, y: 2, z: 4, core: 2. Of those that a mesh axis runs over, the one named last changes fastest.
Arguments:
- rhs: float32 [2, 512, 512], P('layer', 'gx', 'gy'), may hold values from -7 to 7
- start: float32 [2, 512, 512], P('layer', 'gx', 'gy'), may hold values from -4 to 4
- valid: int32 [8, 512, 512], P(None, 'gx', 'gy'), may hold values 0 or 1
- reg: float32 [2], P('layer'), may hold values from 0.25 to 2
- shifts: int32 [8, 2, 2], replicated, may hold values from -16 to 16, as said below
- frac: int32 [8, 2, 2], replicated, may hold values from 0 to 255
Outputs:
- solution: float32 [2, 512, 512], P('layer', 'gx', 'gy')
- residual: float32 [2, 512, 512], P('layer', 'gx', 'gy')
The draws below stay inside these ranges and needn't reach their ends.
Inputs may be any that keep to these rules, and one draw needn't show every extreme that they name: `shifts`: offsets in whole grid points; some guide star reaches offset 16 along the first dimension and minus 16 along the second on some layer.
All inputs are finite; a program needn't handle non-finite values. No bound on the sum of `valid` on one device may be relied on, other than what follows from the above.
Results may differ from the reference program's by a relative error of at most 0.00011.
Values sent between devices are 32-bit elements; how exact they have to be, the bound alone decides.
No kernel may reach another device: no remote copies, remote signals or barrier semaphores. Data moves between devices by JAX's collectives and lax.ppermute only.
A program may use at most 64 MiB of HBM per device.

```python
import math
import jax
import jax.numpy as jnp
from jax import lax

GUIDES = 8
SHIFT_MAX = 16
LEVELS = 3
ITERS = 2
LAYERS = 2
NX = 512
NY = 512


def draw_shifts(key, part):
    values = jax.random.randint(key, (GUIDES, LAYERS, 2), -SHIFT_MAX, SHIFT_MAX + 1, dtype=jnp.int32)
    values = values.at[0, LAYERS - 1, 0].set(SHIFT_MAX)
    return values.at[GUIDES - 1, LAYERS - 1, 1].set(-SHIFT_MAX)


def block_field(key, amp_low, amp_high):
    stride = 2 ** (LEVELS - 1)
    key_sign, key_size = jax.random.split(key)
    coarse_shape = (LAYERS, NX // stride, NY // stride)
    signs = jax.random.rademacher(key_sign, coarse_shape, dtype=jnp.float32)
    amounts = jax.random.uniform(key_size, coarse_shape, jnp.float32, amp_low, amp_high)
    coarse = signs * amounts
    return jnp.repeat(jnp.repeat(coarse, stride, axis=1), stride, axis=2)


def draw_rhs(key, part):
    key = jax.random.fold_in(key, 11)
    key_fine, key_block = jax.random.split(key)
    fine = jnp.clip(jax.random.normal(key_fine, (LAYERS, NX, NY), jnp.float32), -4.0, 4.0)
    blocks = block_field(key_block, 1.5, 3.0)
    return (fine + blocks).astype(jnp.float32)


def draw_start(key, part):
    key = jax.random.fold_in(key, 23)
    key_fine, key_block = jax.random.split(key)
    fine = 0.5 * jnp.clip(jax.random.normal(key_fine, (LAYERS, NX, NY), jnp.float32), -5.0, 5.0)
    blocks = block_field(key_block, 0.5, 1.0)
    return (fine + blocks).astype(jnp.float32)


def touch_ends(drawn, own_key, low, top_value):
    longest = drawn.shape.index(max(drawn.shape))
    spots = []
    for shift in (0, 1):
        where = [jax.random.randint(jax.random.fold_in(own_key, axis), (), 0, length) for axis, length in enumerate(drawn.shape)]
        where[longest] = (where[longest] + shift) % drawn.shape[longest]
        spots.append(tuple(where))
    return drawn.at[spots[0]].set(low).at[spots[1]].set(top_value)


def steps_of(rng, extent, cuts, low, top_value):
    level = 1.0
    for axis_at, blocks in cuts:
        steps = jax.random.uniform(jax.random.fold_in(jax.random.fold_in(rng, 6), axis_at), (blocks,), jnp.float32, low / len(cuts), top_value / len(cuts))
        level = level * jnp.repeat(jnp.exp(steps), extent[axis_at] // blocks).reshape((-1,) + (1,) * (len(extent) - 1 - axis_at))
    return level


def setup_inputs(seed: int = 0) -> dict:
    seeds = jax.random.split(jax.random.key(seed), 7)
    return {
        "rhs": draw_rhs(jax.random.fold_in(seeds[6], 71), 0),
        "start": draw_start(jax.random.fold_in(seeds[6], 71), 0),
        "valid": touch_ends((jax.random.randint(seeds[2], (GUIDES, NX, NY), 0, 8) < 7).astype(jnp.int32), jax.random.fold_in(seeds[2], 1), 0, 1),
        "reg": jnp.clip(jnp.exp(math.log(2.0) - 2.0794415 * jax.random.uniform(seeds[3], (LAYERS,), jnp.float32) ** steps_of(seeds[3], (LAYERS,), ((0, 2),), -0.2, 0.2)), 0.25, 2.0),
        "shifts": draw_shifts(jax.random.fold_in(seeds[6], 71), 0),
        "frac": touch_ends(jax.random.randint(seeds[5], (GUIDES, LAYERS, 2), 0, 256), jax.random.fold_in(seeds[5], 1), 0, 255).astype(jnp.int32),
    }


def interp(plane, offset, fraction, sign, tile_rows, tile_cols):
    width = SHIFT_MAX + 1
    frac_row = fraction[0].astype(jnp.float32) / 256.0
    frac_col = fraction[1].astype(jnp.float32) / 256.0
    result = jnp.zeros((tile_rows, tile_cols), jnp.float32)
    for step_row, step_col, factor in ((0, 0, (1.0 - frac_row) * (1.0 - frac_col)), (1, 0, frac_row * (1.0 - frac_col)), (0, 1, (1.0 - frac_row) * frac_col), (1, 1, frac_row * frac_col)):
        begin_row = (width + sign * (offset[0] + step_row)).astype(jnp.int32)
        begin_col = (width + sign * (offset[1] + step_col)).astype(jnp.int32)
        pieces = lax.dynamic_slice(plane, (begin_row, begin_col), (tile_rows, tile_cols))
        result = result + factor * pieces
    return result


def laplace(values):
    padded = jnp.pad(values, ((0, 0), (1, 1), (1, 1)))
    return padded[:, 2:, 1:-1] + padded[:, :-2, 1:-1] + padded[:, 1:-1, 2:] + padded[:, 1:-1, :-2] - 4.0 * values


def bilaplace(values):
    return laplace(laplace(values))


def operator_a(field, valid, weight, shifts, frac):
    width = SHIFT_MAX + 1
    padded = jnp.pad(field, ((0, 0), (width, width), (width, width)))
    footprints = []
    for guide in range(GUIDES):
        summed = jnp.zeros((NX, NY), jnp.float32)
        for layer in range(LAYERS):
            summed = summed + interp(padded[layer], shifts[guide, layer], frac[guide, layer], 1, NX, NY)
        footprints.append(summed)
    measured = jnp.stack(footprints) * valid.astype(jnp.float32)
    padded_m = jnp.pad(measured, ((0, 0), (width, width), (width, width)))
    backs = []
    for layer in range(LAYERS):
        summed = jnp.zeros((NX, NY), jnp.float32)
        for guide in range(GUIDES):
            summed = summed + interp(padded_m[guide], shifts[guide, layer], frac[guide, layer], -1, NX, NY)
        backs.append(summed)
    return jnp.stack(backs) + weight * bilaplace(field) + 0.1 * field


def level_op(values, weight, level):
    return 4.0 * values + weight * bilaplace(values) / (16.0 ** level)


def vcycle(right, weight, level):
    diag = 4.0 + 20.0 * weight / (16.0 ** level)
    guess = 0.5 * right / diag
    if level == LEVELS - 1:
        return guess + 0.5 * (right - level_op(guess, weight, level)) / diag
    leftover = right - level_op(guess, weight, level)
    layers, rows_now, cols_now = leftover.shape
    coarse = leftover.reshape(layers, rows_now // 2, 2, cols_now // 2, 2).sum(axis=(2, 4)) * 0.25
    correction = vcycle(coarse, weight, level + 1)
    guess = guess + jnp.repeat(jnp.repeat(correction, 2, axis=1), 2, axis=2)
    return guess + 0.5 * (right - level_op(guess, weight, level)) / diag


def reference(rhs, start, valid, reg, shifts, frac):
    weight = reg[:, None, None]
    solution = start
    residual = rhs - operator_a(solution, valid, weight, shifts, frac)
    precond = vcycle(residual, weight, 0)
    direction = precond
    rz_now = jnp.sum(residual * precond)
    for step in range(ITERS):
        image = operator_a(direction, valid, weight, shifts, frac)
        alpha = rz_now / jnp.sum(direction * image)
        solution = solution + alpha * direction
        residual = residual - alpha * image
        if step + 1 < ITERS:
            precond = vcycle(residual, weight, 0)
            rz_next = jnp.sum(residual * precond)
            direction = precond + (rz_next / rz_now) * direction
            rz_now = rz_next
    return solution, residual
```

```python
import functools

import jax
import jax.numpy as jnp
from jax import lax
from jax.experimental import pallas as pl
from jax.experimental.pallas import tpu as pltpu
from jax.sharding import PartitionSpec as P

GUIDES = 8
SHIFT_MAX = 16
LANES = 128
HALF = LANES // 2
QUART = LANES // 4
VROWS = 72
F32 = jnp.float32
BF16 = jnp.bfloat16
DOT = functools.partial(jnp.dot, preferred_element_type=F32)


def lane_iota(shape=(1, LANES)):
    return lax.broadcasted_iota(jnp.int32, shape, len(shape) - 1)


def roll(x, amount):
    amount = amount % LANES if isinstance(amount, int) else amount & (LANES - 1)
    if isinstance(amount, int) and amount == 0:
        return x
    return pltpu.roll(x, amount, x.ndim - 1)


def spans(low, high, size):
    return [(r, min(size, high - r)) for r in range(low, high, size)]


def order_matrix(inverse):
    source = lax.broadcasted_iota(jnp.int32, (LANES, LANES), 0)
    target = lax.broadcasted_iota(jnp.int32, (LANES, LANES), 1)
    if inverse:
        source, target = target, source
    wanted = 2 * (target & (HALF - 1)) + (target >= HALF).astype(jnp.int32)
    return (source == wanted).astype(F32).astype(BF16)


def exact_dot(values, matrix):
    high = values.astype(BF16)
    rest = values - high.astype(F32)
    mid = rest.astype(BF16)
    low = (rest - mid.astype(F32)).astype(BF16)
    return DOT(high, matrix) + (DOT(mid, matrix) + DOT(low, matrix))


def pack_inputs(start_ref, rhs_ref, valid_ref, reg_ref, xr_ref, own_ref, up_ref, down_ref):
    rows = start_ref.shape[1]
    matrix = order_matrix(False)
    xr_ref[pl.ds(0, rows), :] = exact_dot(start_ref[0], matrix)
    xr_ref[pl.ds(rows, rows), :] = exact_dot(rhs_ref[0], matrix)
    xr_ref[pl.ds(2 * rows, 8), :] = jnp.full((8, LANES), reg_ref[0], F32)
    for g in range(valid_ref.shape[0]):
        plane = DOT(valid_ref[g].astype(F32).astype(BF16), matrix)
        own_ref[g] = plane
        up_ref[pl.ds(g * VROWS, VROWS), :] = plane[:VROWS]
        down_ref[pl.ds(g * VROWS, VROWS), :] = plane[rows - VROWS :]


def pair_strips(first, second):
    keep = (lane_iota() & (HALF - 1)) < QUART
    left = jnp.where(keep, first, roll(second, QUART))
    right = jnp.where(keep, roll(first, -QUART), second)
    return left, right


def pack_pairs(meta_ref, parts, out_left, out_right, base, halo, rows):
    top_ok = meta_ref[0].astype(F32)
    bottom_ok = meta_ref[1].astype(F32)
    total = rows + 2 * halo
    for k in range((len(parts) + 1) // 2):
        pair = (parts[2 * k], parts[min(2 * k + 1, len(parts) - 1)])
        for at, low, high, which, scale in (
            (0, 0, halo, 0, top_ok),
            (halo, 0, rows, 1, None),
            (halo + rows, 0, halo, 2, bottom_ok),
        ):
            for r, n in spans(low, high, 32):
                first, second = (part[which](r, n) for part in pair)
                left, right = pair_strips(first, second)
                if scale is not None:
                    left, right = left * scale, right * scale
                out_left[pl.ds(base + k * total + at + r, n), :] = left
                out_right[pl.ds(base + k * total + at + r, n), :] = right
    return base + ((len(parts) + 1) // 2) * total


def rows_of(ref, start):
    return lambda r, n: ref[pl.ds(start + r, n), :]


def planes_of(meta_ref, part, position, left_of, right_of, halo, rows):
    top_ok = meta_ref[0].astype(F32)
    bottom_ok = meta_ref[1].astype(F32)
    left_ok = meta_ref[2].astype(F32)
    right_ok = meta_ref[3].astype(F32)
    lane = lane_iota()
    for at, count, which, scale in ((0, halo, 0, top_ok), (halo, rows, 1, None), (halo + rows, halo, 2, bottom_ok)):
        for r, n in spans(0, count, 32):
            own = part[which](r, n)
            if scale is not None:
                own = own * scale
            left = left_of(at + r, n) * left_ok
            right = right_of(at + r, n) * right_ok
            back = QUART * position
            even = jnp.where(
                lane < QUART,
                roll(left, -back),
                jnp.where(lane < 3 * QUART, roll(own, QUART), roll(right, 3 * QUART - back)),
            )
            odd = jnp.where(
                lane < QUART,
                roll(left, HALF - back),
                jnp.where(lane < 3 * QUART, roll(own, -QUART), roll(right, QUART - back)),
            )
            yield at + r - halo, n, even, odd


def five_point(ref, at, n):
    even, odd = ref[0, pl.ds(at, n), :], ref[1, pl.ds(at, n), :]
    sum_even = ref[0, pl.ds(at - 1, n), :] + ref[0, pl.ds(at + 1, n), :] + (odd + roll(odd, 1))
    sum_odd = ref[1, pl.ds(at - 1, n), :] + ref[1, pl.ds(at + 1, n), :] + (even + roll(even, -1))
    return sum_even - 4.0 * even, sum_odd - 4.0 * odd, even, odd


def five_coarse(ref, at, n, step):
    here = ref[pl.ds(at, n), :]
    sides = roll(here, step) + roll(here, -step)
    return ref[pl.ds(at - 1, n), :] + ref[pl.ds(at + 1, n), :] + sides - 4.0 * here, here


def mask_rows(meta_ref, row_at, n, rows):
    top_ok = meta_ref[0].astype(F32)
    bottom_ok = meta_ref[1].astype(F32)
    left_ok = meta_ref[2].astype(F32)
    right_ok = meta_ref[3].astype(F32)
    row = row_at + lax.broadcasted_iota(jnp.int32, (n, LANES), 0)
    lane = lane_iota((n, LANES))
    by_row = jnp.where(row < 0, top_ok, jnp.where(row >= rows, bottom_ok, 1.0))
    return by_row * jnp.where(lane < QUART, left_ok, jnp.where(lane >= 3 * QUART, right_ok, 1.0))


def guide_loop(meta_ref, shifts_ref, frac_ref, x_ref, x_base, valid_ref, m_ref, m_base, acc_ref, acc_base, p_rows, outs, slots, out_slots, square_ref=None, rows=None):
    count = slots

    def coefficients(g, slot):
        layer = lax.rem(meta_ref[4] - slot + count, count)
        at = (g * count + layer) * 2
        return (
            shifts_ref[at],
            shifts_ref[at + 1],
            frac_ref[at].astype(F32) * (1.0 / 256.0),
            frac_ref[at + 1].astype(F32) * (1.0 / 256.0),
        )

    def taps(ref, index, at, u, odd, column, n, step):
        first = pl.ds(at, n)
        second = pl.ds(at + step, n)
        here = ref[index + (odd, first, slice(None))]
        plane_a = here + u * (ref[index + (odd, second, slice(None))] - here)
        here = ref[index + (1 - odd, first, slice(None))]
        plane_b = here + u * (ref[index + (1 - odd, second, slice(None))] - here)
        return (
            roll(plane_a, LANES - column),
            roll(plane_b, LANES - column - odd),
            roll(plane_a, LANES - column - 1),
        )

    def body(g, carry):
        fixed = []
        for slot in range(count):
            a, b, u, v = coefficients(g, slot)
            fixed.append((a, u, v, b & 1, lax.shift_right_arithmetic(b, 1)))
        for r, n in spans(*p_rows, 16):
            even = odd = None
            for slot in range(count):
                a, u, v, parity, column = fixed[slot]
                q0, q1, q2 = taps(x_ref, (slot,), r + x_base + a, u, parity, column, n, 1)
                this_even = q0 + v * (q1 - q0)
                this_odd = q1 + v * (q2 - q1)
                even = this_even if even is None else even + this_even
                odd = this_odd if odd is None else odd + this_odd
            m_even = even * valid_ref[g, 0, pl.ds(r + VROWS, n), :]
            m_odd = odd * valid_ref[g, 1, pl.ds(r + VROWS, n), :]
            m_ref[0, pl.ds(r + m_base, n), :] = m_even
            m_ref[1, pl.ds(r + m_base, n), :] = m_odd
            if square_ref is not None:
                for k in range(0, n, 8):
                    if 0 <= r + k < rows:
                        sl = slice(k, k + 8)
                        square_ref[...] += m_even[sl] * even[sl] + m_odd[sl] * odd[sl]
        for slot in range(out_slots):
            a, b, u, v = coefficients(g, slot)
            back = -b - 1
            parity, column = back & 1, lax.shift_right_arithmetic(back, 1)
            for r, n in spans(*outs, 16):
                q0, q1, q2 = taps(m_ref, (), r + m_base - a, u, parity, column, n, -1)
                acc_ref[slot, 0, pl.ds(r + acc_base, n), :] += q1 + v * (q0 - q1)
                acc_ref[slot, 1, pl.ds(r + acc_base, n), :] += q2 + v * (q1 - q2)
        return carry

    lax.fori_loop(0, valid_ref.shape[0], body, 0)


def zero_rows(ref, index, ranges):
    for low, high in ranges:
        if high > low:
            ref[index + (pl.ds(low, high - low), slice(None))] = jnp.zeros((high - low, LANES), F32)


def clear_planes(ref, index):
    for plane in range(2):
        for r, n in spans(0, ref.shape[-2], 64):
            ref[index + (plane, pl.ds(r, n), slice(None))] = jnp.zeros((n, LANES), F32)


def vcycle(h_ref, out_ref, weight, depth, rows, masks, work):
    g_ref, w_ref, t_ref, h1, g1, w1, t1, h2, g2 = work
    mask0, mask1, mask2 = masks
    size0 = rows + 2 * depth
    size1, size2 = size0 // 2, size0 // 4
    lane = lane_iota()
    s0 = 0.5 / (4.0 + 20.0 * weight)
    weight1, weight2 = weight * (1.0 / 16.0), weight * (1.0 / 256.0)
    s1 = 0.5 / (4.0 + 20.0 * weight1)
    s2 = 0.5 / (4.0 + 20.0 * weight2)

    for r, n in spans(8, 8 + size0, 16):
        lap_even, lap_odd, _, _ = five_point(h_ref, r, n)
        mask = mask0[pl.ds(r, n), :]
        g_ref[0, pl.ds(r, n), :] = mask * lap_even
        g_ref[1, pl.ds(r, n), :] = mask * lap_odd
    for r, n in spans(8, 8 + size0, 16):
        bi_even, bi_odd, _, _ = five_point(g_ref, r, n)
        h_both = h_ref[0, pl.ds(r, n), :] + h_ref[1, pl.ds(r, n), :]
        t_ref[pl.ds(r, n), :] = mask0[pl.ds(r, n), :] * (
            h_both - s0 * (4.0 * h_both + weight * (bi_even + bi_odd))
        )
    h1[pl.ds(8, size1), :] = 0.25 * (t_ref[pl.ds(8, size1, stride=2), :] + t_ref[pl.ds(9, size1, stride=2), :])
    for r, n in spans(8, 8 + size1, 32):
        lap, _ = five_coarse(h1, r, n, 1)
        g1[pl.ds(r, n), :] = mask1[pl.ds(r, n), :] * lap
    for r, n in spans(8, 8 + size1, 32):
        bi, _ = five_coarse(g1, r, n, 1)
        here = h1[pl.ds(r, n), :]
        t1[pl.ds(r, n), :] = mask1[pl.ds(r, n), :] * (here - s1 * (4.0 * here + weight1 * bi))
    both = t1[pl.ds(8, size2, stride=2), :] + t1[pl.ds(9, size2, stride=2), :]
    h2[pl.ds(8, size2), :] = 0.25 * (both + jnp.where((lane & 1) == 0, roll(both, -1), roll(both, 1)))
    lap, _ = five_coarse(h2, 8, size2, 2)
    g2[pl.ds(8, size2), :] = mask2[pl.ds(8, size2), :] * lap
    bi, _ = five_coarse(g2, 8, size2, 2)
    here = h2[pl.ds(8, size2), :]
    e2 = mask2[pl.ds(8, size2), :] * (s2 * (2.0 * here - s2 * (4.0 * here + weight2 * bi)))
    t1[pl.ds(8, size2, stride=2), :] = e2
    t1[pl.ds(9, size2, stride=2), :] = e2
    for r, n in spans(8, 8 + size1, 32):
        w1[pl.ds(r, n), :] = s1 * h1[pl.ds(r, n), :] + t1[pl.ds(r, n), :]
    for r, n in spans(8, 8 + size1, 32):
        lap, _ = five_coarse(w1, r, n, 1)
        g1[pl.ds(r, n), :] = mask1[pl.ds(r, n), :] * lap
    for r, n in spans(8, 8 + size1, 32):
        bi, _ = five_coarse(g1, r, n, 1)
        here = w1[pl.ds(r, n), :]
        t1[pl.ds(r, n), :] = mask1[pl.ds(r, n), :] * (
            here + s1 * (h1[pl.ds(r, n), :] - 4.0 * here - weight1 * bi)
        )
    e1 = t1[pl.ds(8, size1), :]
    t_ref[pl.ds(8, size1, stride=2), :] = e1
    t_ref[pl.ds(9, size1, stride=2), :] = e1
    for r, n in spans(8, 8 + size0, 16):
        copied = t_ref[pl.ds(r, n), :]
        for plane in range(2):
            w_ref[plane, pl.ds(r, n), :] = s0 * h_ref[plane, pl.ds(r, n), :] + copied
    for r, n in spans(8, 8 + size0, 16):
        lap_even, lap_odd, _, _ = five_point(w_ref, r, n)
        mask = mask0[pl.ds(r, n), :]
        g_ref[0, pl.ds(r, n), :] = mask * lap_even
        g_ref[1, pl.ds(r, n), :] = mask * lap_odd
    for r, n in spans(8, 8 + size0, 16):
        bi = five_point(g_ref, r, n)[:2]
        mask = mask0[pl.ds(r, n), :]
        for plane in range(2):
            here = w_ref[plane, pl.ds(r, n), :]
            out_ref[plane, pl.ds(r, n), :] = mask * (
                here + s0 * (h_ref[plane, pl.ds(r, n), :] - 4.0 * here - weight * bi[plane])
            )


def vcycle_scratch(depth, rows):
    size0 = rows + 2 * depth
    one = lambda size: pltpu.VMEM((size + 16, LANES), F32)
    two = pltpu.VMEM((2, size0 + 16, LANES), F32)
    size1, size2 = size0 // 2, size0 // 4
    work = [two, two, one(size0), one(size1), one(size1), one(size1), one(size1), one(size2), one(size2)]
    return work, [one(size0), one(size1), one(size2)]


def prepare_vcycle(meta_ref, depth, rows, masks, work):
    size0 = rows + 2 * depth
    sizes = (size0, size0 // 2, size0 // 4)
    for level, (mask, size) in enumerate(zip(masks, sizes)):
        for r, n in spans(0, size + 16, 64):
            mask[pl.ds(r, n), :] = mask_rows(meta_ref, r - 8 - (depth >> level), n, rows >> level)
    g_ref, w_ref, t_ref, h1, g1, w1, t1, h2, g2 = work
    for ref in (g_ref, w_ref):
        for plane in range(2):
            zero_rows(ref, (plane,), ((0, 8), (size0 + 8, size0 + 16)))
    for ref, size in ((h1, sizes[1]), (g1, sizes[1]), (w1, sizes[1]), (h2, sizes[2]), (g2, sizes[2])):
        zero_rows(ref, (), ((0, 8), (size + 8, size + 16)))


def bilaplace_into(x_ref, x_base, g_ref, low, high, mask_of):
    for r, n in spans(low - 8, high + 8, 16):
        lap_even, lap_odd, _, _ = five_point(x_ref, r + x_base, n)
        mask = mask_of(r, n)
        g_ref[0, pl.ds(r - low + 8, n), :] = mask * lap_even
        g_ref[1, pl.ds(r - low + 8, n), :] = mask * lap_odd


def tile_of(even, odd):
    return jnp.where(lane_iota() < HALF, roll(even, -QUART), roll(odd, QUART))


def fold(values):
    total = values[0:8]
    for k in range(8, values.shape[0], 8):
        total = total + values[k : k + 8]
    return total


def inner_mask():
    lane = lane_iota()
    return ((lane >= QUART) & (lane < 3 * QUART)).astype(F32)


X_HALO, R_HALO, Z_HALO = 56, 24, 88
DEPTH1, DEPTH2 = 24, 56
Y_HALO = 40


def first_parts(xr_refs, top_ref, bottom_ref, rows, what):
    halo, skip = (X_HALO, 0) if what == 0 else (R_HALO, X_HALO)
    parts = []
    for k, ref in enumerate(xr_refs):
        at = k * (X_HALO + R_HALO) + skip
        parts.append((rows_of(top_ref, at), rows_of(ref, what * rows), rows_of(bottom_ref, at)))
    return parts


def pack_first(slots, rows, meta_ref, *refs):
    xr_refs, (top_ref, bottom_ref, left_ref, right_ref) = refs[:slots], refs[slots:]
    base = pack_pairs(
        meta_ref, first_parts(xr_refs, top_ref, bottom_ref, rows, 0), left_ref, right_ref, 0, X_HALO, rows
    )
    pack_pairs(
        meta_ref, first_parts(xr_refs, top_ref, bottom_ref, rows, 1), left_ref, right_ref, base, R_HALO, rows
    )


def valid_parts(own_ref, top_ref, bottom_ref):
    return [
        (
            rows_of(top_ref, g * VROWS),
            (lambda g: lambda r, n: own_ref[g, pl.ds(r, n), :])(g),
            rows_of(bottom_ref, g * VROWS),
        )
        for g in range(own_ref.shape[0])
    ]


def pack_valid(meta_ref, own_ref, top_ref, bottom_ref, left_ref, right_ref):
    pack_pairs(
        meta_ref, valid_parts(own_ref, top_ref, bottom_ref), left_ref, right_ref, 0, VROWS, own_ref.shape[1]
    )


def spread_valid(meta_ref, own_ref, top_ref, bottom_ref, left_ref, right_ref, out_ref):
    rows = own_ref.shape[1]
    total = rows + 2 * VROWS
    for g, part in enumerate(valid_parts(own_ref, top_ref, bottom_ref)):
        base = (g // 2) * total
        for r, n, even, odd in planes_of(
            meta_ref, part, g % 2, rows_of(left_ref, base), rows_of(right_ref, base), VROWS, rows
        ):
            out_ref[g, 0, pl.ds(r + VROWS, n), :] = even
            out_ref[g, 1, pl.ds(r + VROWS, n), :] = odd


def stage_first(slots, rows, meta_ref, shifts_ref, frac_ref, *refs):
    xr_refs, refs = refs[:slots], refs[slots:]
    top_ref, bottom_ref, left_ref, right_ref, valid_ref = refs[:5]
    z_ref, up_ref, down_ref, res_ref, dot_ref = refs[5:10]
    x_ref, m_ref, acc_ref, z_planes, *rest = refs[10:]
    work, masks = rest[:9], rest[9:12]
    x_base, m_base, acc_base = X_HALO + 8, 48, DEPTH1 + 8
    prepare_vcycle(meta_ref, DEPTH1, rows, masks, work)
    total = rows + 2 * X_HALO
    for k, part in enumerate(first_parts(xr_refs, top_ref, bottom_ref, rows, 0)):
        base = (k // 2) * total
        for r, n, even, odd in planes_of(
            meta_ref, part, k % 2, rows_of(left_ref, base), rows_of(right_ref, base), X_HALO, rows
        ):
            x_ref[k, 0, pl.ds(r + x_base, n), :] = even
            x_ref[k, 1, pl.ds(r + x_base, n), :] = odd
        for plane in range(2):
            zero_rows(x_ref, (k, plane), ((0, 8), (total + 8, total + 16)))
        clear_planes(acc_ref, (k,))
    for plane in range(2):
        zero_rows(m_ref, (plane,), ((0, 8), (rows + 88, rows + 96)))
    guide_loop(
        meta_ref, shifts_ref, frac_ref, x_ref, x_base, valid_ref, m_ref, m_base, acc_ref, acc_base,
        (-40, rows + 40), (-DEPTH1, rows + DEPTH1), slots, slots,
    )
    first_total = ((slots + 1) // 2) * total
    total_r = rows + 2 * R_HALO
    g_ref = work[0]
    dot_ref[...] = jnp.zeros((8, LANES), F32)
    inner = inner_mask()
    for k, part in enumerate(first_parts(xr_refs, top_ref, bottom_ref, rows, 1)):
        weight = xr_refs[k][pl.ds(2 * rows, 1), :]
        bilaplace_into(
            x_ref.at[k], x_base, g_ref, -DEPTH1, rows + DEPTH1,
            lambda r, n: masks[0][pl.ds(r + DEPTH1 + 8, n), :],
        )
        base = first_total + (k // 2) * total_r
        h_ref = acc_ref.at[k]
        for r, n, even, odd in planes_of(
            meta_ref, part, k % 2, rows_of(left_ref, base), rows_of(right_ref, base), R_HALO, rows
        ):
            at = r + DEPTH1 + 8
            bi = five_point(g_ref, at, n)[:2]
            mask = masks[0][pl.ds(at, n), :]
            for plane, right in enumerate((even, odd)):
                h_ref[plane, pl.ds(at, n), :] = mask * (
                    right
                    - acc_ref[k, plane, pl.ds(at, n), :]
                    - weight * bi[plane]
                    - 0.1 * x_ref[k, plane, pl.ds(r + x_base, n), :]
                )
        for plane in range(2):
            zero_rows(g_ref, (plane,), ((0, 8), (rows + 2 * DEPTH1 + 8, rows + 2 * DEPTH1 + 16)))
        vcycle(h_ref, z_planes, weight, DEPTH1, rows, masks, work)
        for r, n in spans(0, rows, 32):
            at = r + DEPTH1 + 8
            res = h_ref[0, pl.ds(at, n), :], h_ref[1, pl.ds(at, n), :]
            z = z_planes[0, pl.ds(at, n), :], z_planes[1, pl.ds(at, n), :]
            dot_ref[...] += inner * fold(res[0] * z[0] + res[1] * z[1])
            z_ref[k, pl.ds(r, n), :] = tile_of(*z)
            if k == 0:
                res_ref[pl.ds(r, n), :] = tile_of(*res)
        up_ref[pl.ds(k * Z_HALO, Z_HALO), :] = z_ref[k, pl.ds(0, Z_HALO), :]
        down_ref[pl.ds(k * Z_HALO, Z_HALO), :] = z_ref[k, pl.ds(rows - Z_HALO, Z_HALO), :]


def second_parts(z_ref, top_ref, bottom_ref):
    return [
        (
            rows_of(top_ref, k * Z_HALO),
            (lambda k: lambda r, n: z_ref[k, pl.ds(r, n), :])(k),
            rows_of(bottom_ref, k * Z_HALO),
        )
        for k in range(z_ref.shape[0])
    ]


def pack_second(meta_ref, z_ref, top_ref, bottom_ref, left_ref, right_ref):
    pack_pairs(
        meta_ref, second_parts(z_ref, top_ref, bottom_ref), left_ref, right_ref, 0, Z_HALO, z_ref.shape[1]
    )


def stage_second(slots, rows, meta_ref, shifts_ref, frac_ref, *refs):
    xr_refs, refs = refs[:slots], refs[slots:]
    z_ref, top_ref, bottom_ref, left_ref, right_ref, valid_ref = refs[:6]
    y_ref, out_left, out_right, image_ref, dot_zq, dot_yq = refs[6:12]
    x_ref, m_ref, acc_ref, y_planes, *rest = refs[12:]
    work, masks = rest[:9], rest[9:12]
    x_base, m_base, acc_base = Z_HALO, 80, DEPTH2 + 8
    prepare_vcycle(meta_ref, DEPTH2, rows, masks, work)
    total = rows + 2 * Z_HALO
    for k, part in enumerate(second_parts(z_ref, top_ref, bottom_ref)):
        base = (k // 2) * total
        for r, n, even, odd in planes_of(
            meta_ref, part, k % 2, rows_of(left_ref, base), rows_of(right_ref, base), Z_HALO, rows
        ):
            x_ref[k, 0, pl.ds(r + x_base, n), :] = even
            x_ref[k, 1, pl.ds(r + x_base, n), :] = odd
        for plane in range(2):
            zero_rows(x_ref, (k, plane), ((total, total + 8),))
        clear_planes(acc_ref, (k,))
    for plane in range(2):
        zero_rows(m_ref, (plane,), ((0, 8), (rows + 152, rows + 160)))
    guide_loop(
        meta_ref, shifts_ref, frac_ref, x_ref, x_base, valid_ref, m_ref, m_base, acc_ref, acc_base,
        (-VROWS, rows + VROWS), (-DEPTH2, rows + DEPTH2), slots, slots,
    )
    g_ref = work[0]
    dot_zq[...] = jnp.zeros((8, LANES), F32)
    dot_yq[...] = jnp.zeros((8, LANES), F32)
    inner = inner_mask()
    for k in range(slots):
        weight = xr_refs[k][pl.ds(2 * rows, 1), :]
        bilaplace_into(
            x_ref.at[k], x_base, g_ref, -DEPTH2, rows + DEPTH2,
            lambda r, n: masks[0][pl.ds(r + DEPTH2 + 8, n), :],
        )
        h_ref = acc_ref.at[k]
        for r, n in spans(-DEPTH2, rows + DEPTH2, 16):
            at = r + DEPTH2 + 8
            bi = five_point(g_ref, at, n)[:2]
            mask = masks[0][pl.ds(at, n), :]
            for plane in range(2):
                h_ref[plane, pl.ds(at, n), :] = mask * (
                    acc_ref[k, plane, pl.ds(at, n), :]
                    + weight * bi[plane]
                    + 0.1 * x_ref[k, plane, pl.ds(r + x_base, n), :]
                )
        for plane in range(2):
            zero_rows(g_ref, (plane,), ((0, 8), (rows + 2 * DEPTH2 + 8, rows + 2 * DEPTH2 + 16)))
        vcycle(h_ref, y_planes.at[k], weight, DEPTH2, rows, masks, work)
        for r, n in spans(0, rows, 32):
            at = r + DEPTH2 + 8
            q = h_ref[0, pl.ds(at, n), :], h_ref[1, pl.ds(at, n), :]
            y = y_planes[k, 0, pl.ds(at, n), :], y_planes[k, 1, pl.ds(at, n), :]
            z = x_ref[k, 0, pl.ds(r + x_base, n), :], x_ref[k, 1, pl.ds(r + x_base, n), :]
            dot_zq[...] += inner * fold(z[0] * q[0] + z[1] * q[1])
            dot_yq[...] += inner * fold(y[0] * q[0] + y[1] * q[1])
            if k == 0:
                image_ref[pl.ds(r, n), :] = tile_of(*q)
        for r, n in spans(-Y_HALO, rows + Y_HALO, 16):
            for plane in range(2):
                y_ref[k, plane, pl.ds(r + Y_HALO, n), :] = y_planes[k, plane, pl.ds(r + DEPTH2 + 8, n), :]
    lane = lane_iota()
    total_y = rows + 2 * Y_HALO
    for pair in range((slots + 1) // 2):
        first, second = 2 * pair, min(2 * pair + 1, slots - 1)
        for r, n in spans(0, total_y, 16):
            e0, o0 = y_ref[first, 0, pl.ds(r, n), :], y_ref[first, 1, pl.ds(r, n), :]
            e1, o1 = y_ref[second, 0, pl.ds(r, n), :], y_ref[second, 1, pl.ds(r, n), :]
            out_left[pl.ds(pair * total_y + r, n), :] = jnp.where(
                lane < HALF,
                jnp.where(lane < QUART, roll(e0, -QUART), e1),
                jnp.where(lane < 3 * QUART, roll(o0, QUART), roll(o1, HALF)),
            )
            out_right[pl.ds(pair * total_y + r, n), :] = jnp.where(
                lane < HALF,
                jnp.where(lane < QUART, roll(e0, HALF), roll(e1, -QUART)),
                jnp.where(lane < 3 * QUART, o0, roll(o1, QUART)),
            )


def stage_third(slots, rows, meta_ref, shifts_ref, frac_ref, *refs):
    xr_refs, refs = refs[:slots], refs[slots:]
    y_ref, left_ref, right_ref, valid_ref, dot_rz, dot_zq, dot_yq = refs[:7]
    image_ref, sums_ref = refs[7:9]
    x_ref, m_ref, acc_ref, g_ref, square_ref, mask_ref = refs[9:]
    x_base, m_base = Y_HALO, 24
    left_ok = meta_ref[2].astype(F32)
    right_ok = meta_ref[3].astype(F32)
    lane = lane_iota()
    total = rows + 2 * Y_HALO
    for k in range(slots):
        base = (k // 2) * total
        back = QUART * (k % 2)
        for r, n in spans(0, total, 16):
            left = left_ref[pl.ds(base + r, n), :] * left_ok
            right = right_ref[pl.ds(base + r, n), :] * right_ok
            x_ref[k, 0, pl.ds(r, n), :] = jnp.where(
                lane < QUART,
                roll(left, -back),
                jnp.where(lane < 3 * QUART, y_ref[k, 0, pl.ds(r, n), :], roll(right, 3 * QUART - back)),
            )
            x_ref[k, 1, pl.ds(r, n), :] = jnp.where(
                lane < QUART,
                roll(left, HALF - back),
                jnp.where(lane < 3 * QUART, y_ref[k, 1, pl.ds(r, n), :], roll(right, QUART - back)),
            )
        for plane in range(2):
            zero_rows(x_ref, (k, plane), ((total, total + 8),))
    clear_planes(acc_ref, (0,))
    square_ref[...] = jnp.zeros((8, LANES), F32)
    for r, n in spans(-8, rows + 8, 48):
        mask_ref[pl.ds(r + 8, n), :] = mask_rows(meta_ref, r, n, rows)
    guide_loop(
        meta_ref, shifts_ref, frac_ref, x_ref, x_base, valid_ref, m_ref, m_base, acc_ref, 0,
        (-24, rows + 24), (0, rows), slots, 1, square_ref, rows,
    )
    for k in reversed(range(slots)):
        weight = xr_refs[k][pl.ds(2 * rows, 1), :]
        bilaplace_into(x_ref.at[k], x_base, g_ref, 0, rows, lambda r, n: mask_ref[pl.ds(r + 8, n), :])
        for r, n in spans(0, rows, 16):
            x = x_ref[k, 0, pl.ds(r + x_base, n), :], x_ref[k, 1, pl.ds(r + x_base, n), :]
            bi_even, bi_odd, g_even, g_odd = five_point(g_ref, r + 8, n)
            square_ref[...] += fold(
                weight * (g_even * g_even + g_odd * g_odd) + 0.1 * (x[0] * x[0] + x[1] * x[1])
            )
            if k == 0:
                image_ref[pl.ds(r, n), :] = tile_of(
                    acc_ref[0, 0, pl.ds(r, n), :] + weight * bi_even + 0.1 * x[0],
                    acc_ref[0, 1, pl.ds(r, n), :] + weight * bi_odd + 0.1 * x[1],
                )
    row = lax.broadcasted_iota(jnp.int32, (8, LANES), 0)
    packed = jnp.zeros((8, LANES), F32)
    for at, part in enumerate((dot_rz[...], dot_zq[...], dot_yq[...], square_ref[...] * inner_mask())):
        packed = jnp.where(row == at, jnp.sum(part, axis=0, keepdims=True), packed)
    for d in range(sums_ref.shape[0]):
        sums_ref[d] = packed


def finish(start_ref, z_ref, res_ref, q_ref, y_ref, p_ref, sums_ref, solution_ref, residual_ref):
    rows = start_ref.shape[1]
    total = sums_ref[0]
    for d in range(1, sums_ref.shape[0]):
        total = total + sums_ref[d]
    total = jnp.sum(total, axis=1, keepdims=True)
    rz, zq, yq, yp = (total[k : k + 1] for k in range(4))
    alpha = rz / zq
    rz_next = alpha * alpha * yq - rz
    grown = 1.0 + rz_next / rz
    alpha_next = rz_next / (grown * grown * zq - 2.0 * alpha * grown * yq + alpha * alpha * yp)
    matrix = order_matrix(True)
    c_z = alpha + alpha_next * grown
    c_y = alpha_next * alpha
    y = tile_of(y_ref[0, 0, pl.ds(Y_HALO, rows), :], y_ref[0, 1, pl.ds(Y_HALO, rows), :])
    solution_ref[0] = start_ref[0] + exact_dot(c_z * z_ref[0] - c_y * y, matrix)
    residual_ref[0] = exact_dot(res_ref[...] - (c_z * q_ref[...] - c_y * p_ref[...]), matrix)


def call(kernel, outs, *args, scratch=(), scalars=0):
    space = lambda k: pltpu.SMEM if k < scalars else pltpu.VMEM
    shapes = [jax.ShapeDtypeStruct(shape, F32) for shape in outs]
    return pl.pallas_call(
        kernel,
        out_shape=shapes,
        in_specs=[pl.BlockSpec(memory_space=space(k)) for k in range(len(args))],
        out_specs=[pl.BlockSpec(memory_space=pltpu.VMEM)] * len(outs),
        scratch_shapes=list(scratch),
    )(*args)


def around(up, down, axis):
    n = lax.axis_size(axis)
    before = lax.ppermute(down, axis, [(i, (i + 1) % n) for i in range(n)])
    after = lax.ppermute(up, axis, [(i, (i - 1) % n) for i in range(n)])
    return before, after


def shards(rhs, start, valid, reg, shifts, frac):
    rows = rhs.shape[1]
    guides = valid.shape[0]
    slots = lax.axis_size("layer")
    gx, gy = lax.axis_index("gx"), lax.axis_index("gy")
    n_gx, n_gy = lax.axis_size("gx"), lax.axis_size("gy")
    at = jnp.arange(8, dtype=jnp.int32)
    meta = jnp.where(
        at == 4,
        lax.axis_index("layer"),
        jnp.where(
            at == 0,
            (gx > 0).astype(jnp.int32),
            jnp.where(
                at == 1,
                (gx < n_gx - 1).astype(jnp.int32),
                jnp.where(at == 2, (gy > 0).astype(jnp.int32), (gy < n_gy - 1).astype(jnp.int32)),
            ),
        ),
    )
    shifts, frac = shifts.reshape(-1), frac.reshape(-1)
    pairs = (slots + 1) // 2
    vmem = lambda *shape: pltpu.VMEM(shape, F32)

    packed = pl.pallas_call(
        pack_inputs,
        out_shape=[
            jax.ShapeDtypeStruct(shape, F32)
            for shape in ((2 * rows + 8, LANES), (guides, rows, LANES), (guides * VROWS, LANES), (guides * VROWS, LANES))
        ],
        in_specs=[pl.BlockSpec(memory_space=pltpu.VMEM)] * 3 + [pl.BlockSpec(memory_space=pltpu.SMEM)],
        out_specs=[pl.BlockSpec(memory_space=pltpu.VMEM)] * 4,
    )(start, rhs, valid, reg)
    xr, valid_own, valid_up, valid_down = packed
    xrs = [xr] + [
        lax.ppermute(xr, "layer", [(i, (i + k) % slots) for i in range(slots)]) for k in range(1, slots)
    ]
    valid_top, valid_bottom = around(valid_up, valid_down, "gx")
    up = jnp.concatenate([part for x in xrs for part in (x[:X_HALO], x[rows : rows + R_HALO])])
    down = jnp.concatenate(
        [part for x in xrs for part in (x[rows - X_HALO : rows], x[2 * rows - R_HALO : 2 * rows])]
    )
    top, bottom = around(up, down, "gx")
    strip = (pairs * (2 * rows + 2 * X_HALO + 2 * R_HALO), LANES)
    left, right = call(
        functools.partial(pack_first, slots, rows), (strip, strip), meta, *xrs, top, bottom, scalars=1
    )
    left, right = around(left, right, "gy")
    strip = ((guides + 1) // 2 * (rows + 2 * VROWS), LANES)
    valid_left, valid_right = call(
        pack_valid, (strip, strip), meta, valid_own, valid_top, valid_bottom, scalars=1
    )
    valid_left, valid_right = around(valid_left, valid_right, "gy")
    (spread,) = call(
        spread_valid,
        ((guides, 2, rows + 2 * VROWS, LANES),),
        meta, valid_own, valid_top, valid_bottom, valid_left, valid_right,
        scalars=1,
    )

    work, masks = vcycle_scratch(DEPTH1, rows)
    size = rows + 2 * DEPTH1 + 16
    z, z_up, z_down, res, dot_rz = call(
        functools.partial(stage_first, slots, rows),
        ((slots, rows, LANES), (slots * Z_HALO, LANES), (slots * Z_HALO, LANES), (rows, LANES), (8, LANES)),
        meta, shifts, frac, *xrs, top, bottom, left, right, spread,
        scalars=3,
        scratch=[
            vmem(slots, 2, rows + 2 * X_HALO + 16, LANES),
            vmem(2, rows + 96, LANES),
            vmem(slots, 2, size, LANES),
            vmem(2, size, LANES),
            *work, *masks,
        ],
    )
    z_top, z_bottom = around(z_up, z_down, "gx")
    strip = (pairs * (rows + 2 * Z_HALO), LANES)
    z_left, z_right = call(pack_second, (strip, strip), meta, z, z_top, z_bottom, scalars=1)
    z_left, z_right = around(z_left, z_right, "gy")

    work, masks = vcycle_scratch(DEPTH2, rows)
    size = rows + 2 * DEPTH2 + 16
    strip = (pairs * (rows + 2 * Y_HALO), LANES)
    y, y_left, y_right, image, dot_zq, dot_yq = call(
        functools.partial(stage_second, slots, rows),
        ((slots, 2, rows + 2 * Y_HALO, LANES), strip, strip, (rows, LANES), (8, LANES), (8, LANES)),
        meta, shifts, frac, *xrs, z, z_top, z_bottom, z_left, z_right, spread,
        scalars=3,
        scratch=[
            vmem(slots, 2, rows + 2 * Z_HALO + 8, LANES),
            vmem(2, rows + 160, LANES),
            vmem(slots, 2, size, LANES),
            vmem(slots, 2, size, LANES),
            *work, *masks,
        ],
    )
    y_left, y_right = around(y_left, y_right, "gy")

    image_y, sums = call(
        functools.partial(stage_third, slots, rows),
        ((rows, LANES), (n_gx * n_gy, 8, LANES)),
        meta, shifts, frac, *xrs, y, y_left, y_right, spread, dot_rz, dot_zq, dot_yq,
        scalars=3,
        scratch=[
            vmem(slots, 2, rows + 2 * Y_HALO + 8, LANES),
            vmem(2, rows + 48, LANES),
            vmem(1, 2, rows, LANES),
            vmem(2, rows + 16, LANES),
            vmem(8, LANES),
            vmem(rows + 16, LANES),
        ],
    )
    sums = lax.all_to_all(sums, ("gx", "gy"), 0, 0)
    return call(
        finish, ((1, rows, LANES), (1, rows, LANES)), start, z, res, image, y, image_y, sums
    )


def solution(mesh):
    in_specs = (
        P("layer", "gx", "gy"),
        P("layer", "gx", "gy"),
        P(None, "gx", "gy"),
        P("layer"),
        P(),
        P(),
    )
    out_specs = (P("layer", "gx", "gy"), P("layer", "gx", "gy"))

    def run(*args):
        return tuple(jax.shard_map(shards, mesh=mesh, in_specs=in_specs, out_specs=out_specs, check_vma=False)(*args))

    return run
```

```python
import functools

import jax
import jax.numpy as jnp
from jax import lax
from jax.experimental import pallas as pl
from jax.experimental.pallas import tpu as pltpu
from jax.sharding import PartitionSpec as P

GUIDES = 8
SHIFT_MAX = 16
LANES = 128
HALF = LANES // 2
QUART = LANES // 4
F32 = jnp.float32
BF16 = jnp.bfloat16
DOT = functools.partial(jnp.dot, preferred_element_type=F32)

X_HALO, R_HALO, V_HALO, V_NEAR, Z_HALO, Y_HALO = 56, 24, 72, 40, 88, 40
DEPTH1, DEPTH2 = 24, 56


def lane_iota(shape=(1, LANES)):
    return lax.broadcasted_iota(jnp.int32, shape, len(shape) - 1)


def roll(x, amount):
    amount = amount % LANES if isinstance(amount, int) else amount & (LANES - 1)
    if isinstance(amount, int) and amount == 0:
        return x
    return pltpu.roll(x, amount, x.ndim - 1)


def spans(low, high, size):
    return [(r, min(size, high - r)) for r in range(low, high, size)]


class Meta:
    def __init__(self, ref):
        self.top_ok, self.bottom_ok, self.left_ok, self.right_ok = (ref[k].astype(F32) for k in range(4))
        self.layer, self.gx_odd, self.gy_odd = ref[4], ref[5], ref[6]


def exact_dot(values, matrix):
    high = values.astype(BF16)
    rest = values - high.astype(F32)
    mid = rest.astype(BF16)
    low = (rest - mid.astype(F32)).astype(BF16)
    return DOT(high, matrix) + (DOT(mid, matrix) + DOT(low, matrix))


def selection(shape, wanted_of):
    source = lax.broadcasted_iota(jnp.int32, shape, 0)
    target = lax.broadcasted_iota(jnp.int32, shape, 1)
    return wanted_of(source, target).astype(F32).astype(BF16)


def send_rows(meta, own_of, halo, rows, out_a, out_b, base):
    for r, n in spans(0, halo, 32):
        up, down = own_of(r, n), own_of(rows - halo + r, n)
        odd = meta.gx_odd == 1
        out_a[pl.ds(base + r, n), :] = jnp.where(odd, up, down)
        out_b[pl.ds(base + r, n), :] = jnp.where(odd, down, up)


def rows_with_halo(meta, own_of, a_of, b_of, skip, halo, rows, size=16):
    odd = meta.gx_odd == 1
    for r, n in spans(0, halo, size):
        yield r - halo, n, lambda t, r=r, n=n: jnp.where(odd, a_of(t, skip + r, n), b_of(t, skip + r, n)) * meta.top_ok
    for r, n in spans(0, rows, size):
        yield r, n, lambda t, r=r, n=n: own_of(t, r, n)
    for r, n in spans(0, halo, size):
        yield rows + r, n, lambda t, r=r, n=n: jnp.where(odd, b_of(t, r, n), a_of(t, r, n)) * meta.bottom_ok


def side_mask(meta):
    return ((lane_iota() >> 5) & 1) == meta.gy_odd


def send_columns(mask, even, odd):
    moved = roll(odd, -QUART)
    return jnp.where(mask, moved, even), jnp.where(mask, even, moved)


def with_columns(meta, mask, even, odd, from_a, from_b):
    lane = lane_iota()
    near = ((lane >> 5) & 1) == 0
    side_even = jnp.where(mask, from_a, from_b) * jnp.where(near, meta.right_ok, meta.left_ok)
    side_odd = jnp.where(mask, from_b, from_a) * jnp.where(near, meta.left_ok, meta.right_ok)
    side_even, side_odd = roll(side_even, HALF), roll(side_odd, -QUART)
    low = lane < HALF
    return (
        (jnp.where(low, even, side_even), jnp.where(low, odd, side_odd)),
        (jnp.where(low, side_even, even), jnp.where(low, side_odd, odd)),
    )


def merge(first, second):
    return jnp.where(lane_iota() < HALF, first, second)


def rows_of(ref, start):
    return lambda r, n: ref[pl.ds(start + r, n), :]


def five_point(ref, at, n):
    even, odd = ref[0, pl.ds(at, n), :], ref[1, pl.ds(at, n), :]
    sum_even = ref[0, pl.ds(at - 1, n), :] + ref[0, pl.ds(at + 1, n), :] + (odd + roll(odd, 1))
    sum_odd = ref[1, pl.ds(at - 1, n), :] + ref[1, pl.ds(at + 1, n), :] + (even + roll(even, -1))
    return sum_even - 4.0 * even, sum_odd - 4.0 * odd, even, odd


def five_coarse(ref, at, n, step):
    here = ref[pl.ds(at, n), :]
    sides = roll(here, step) + roll(here, -step)
    return ref[pl.ds(at - 1, n), :] + ref[pl.ds(at + 1, n), :] + sides - 4.0 * here, here


def mask_rows(meta, position, row_at, n, rows):
    row = row_at + lax.broadcasted_iota(jnp.int32, (n, LANES), 0)
    lane = (lane_iota((n, LANES)) - HALF * position) & (LANES - 1)
    by_row = jnp.where(row < 0, meta.top_ok, jnp.where(row >= rows, meta.bottom_ok, 1.0))
    return by_row * jnp.where(lane < HALF, 1.0, jnp.where(lane < 3 * QUART, meta.right_ok, meta.left_ok))


def guide_loop(meta, shifts_ref, frac_ref, x, valid, m, acc, p_rows, outs, slots, out_slots, square_ref=None, rows=None):
    (x_ref, x_base), (valid_ref, v_base), (m_ref, m_base), (acc_ref, acc_base) = x, valid, m, acc

    def coefficients(g, slot):
        layer = lax.rem(meta.layer - slot + slots, slots)
        at = (g * slots + layer) * 2
        return (
            shifts_ref[at],
            shifts_ref[at + 1],
            frac_ref[at].astype(F32) * (1.0 / 256.0),
            frac_ref[at + 1].astype(F32) * (1.0 / 256.0),
        )

    def between(ref, index, at, step, n, u):
        here = ref[index + (pl.ds(at, n), slice(None))]
        return here + u * (ref[index + (pl.ds(at + step, n), slice(None))] - here)

    def body(g, carry):
        home = HALF * (g & 1)
        fixed = []
        for slot in range(slots):
            a, b, u, v = coefficients(g, slot)
            amount = home - HALF * (slot & 1) - lax.shift_right_arithmetic(b, 1)
            fixed.append((a, u, v, b & 1, amount & (LANES - 1)))
        for r, n in spans(*p_rows, 16):
            even = odd = None
            for slot in range(slots):
                a, u, v, parity, amount = fixed[slot]
                c0, c1, c2 = (between(x_ref, (slot, parity + k), r + x_base + a, 1, n, u) for k in range(3))
                this_even = roll(c0 + v * (c1 - c0), amount)
                this_odd = roll(c1 + v * (c2 - c1), amount)
                even = this_even if even is None else even + this_even
                odd = this_odd if odd is None else odd + this_odd
            m_even = even * valid_ref[g, 0, pl.ds(r + v_base, n), :]
            m_odd = odd * valid_ref[g, 1, pl.ds(r + v_base, n), :]
            m_ref[0, pl.ds(r + m_base, n), :] = m_even
            m_ref[1, pl.ds(r + m_base, n), :] = m_odd
            if square_ref is not None:
                own = (((lane_iota() - home) & (LANES - 1)) < HALF).astype(F32)
                for k in range(0, n, 8):
                    if 0 <= r + k < rows:
                        sl = slice(k, k + 8)
                        square_ref[...] += own * (m_even[sl] * even[sl] + m_odd[sl] * odd[sl])
        for slot in range(out_slots):
            a, b, u, v = coefficients(g, slot)
            back = -b - 1
            parity = back & 1
            amount = HALF * (slot & 1) - home - lax.shift_right_arithmetic(back, 1)
            for r, n in spans(*outs, 16):
                at = r + m_base - a
                plane_a = between(m_ref, (parity,), at, -1, n, u)
                plane_b = between(m_ref, (1 - parity,), at, -1, n, u)
                q0, q1, q2 = roll(plane_a, amount), roll(plane_b, amount - parity), roll(plane_a, amount - 1)
                acc_ref[slot, 0, pl.ds(r + acc_base, n), :] += q1 + v * (q0 - q1)
                acc_ref[slot, 1, pl.ds(r + acc_base, n), :] += q2 + v * (q1 - q2)
        return carry

    lax.fori_loop(0, valid_ref.shape[0], body, 0)


def store_field(x_ref, slot, at, n, even, odd):
    for plane, value in enumerate((even, odd, roll(even, -1), roll(odd, -1))):
        x_ref[slot, plane, pl.ds(at, n), :] = value


def zero_rows(ref, index, ranges):
    for low, high in ranges:
        if high > low:
            ref[index + (pl.ds(low, high - low), slice(None))] = jnp.zeros((high - low, LANES), F32)


def clear_planes(ref, index):
    for plane in range(2):
        for r, n in spans(0, ref.shape[-2], 64):
            ref[index + (plane, pl.ds(r, n), slice(None))] = jnp.zeros((n, LANES), F32)


def vcycle(h_ref, out_ref, weight, depth, rows, masks, work):
    g_ref, w_ref, t_ref, h1, g1, w1, t1, h2, g2 = work
    mask0, mask1, mask2 = masks
    size0 = rows + 2 * depth
    size1, size2 = size0 // 2, size0 // 4
    lane = lane_iota()
    s0 = 0.5 / (4.0 + 20.0 * weight)
    weight1, weight2 = weight * (1.0 / 16.0), weight * (1.0 / 256.0)
    s1 = 0.5 / (4.0 + 20.0 * weight1)
    s2 = 0.5 / (4.0 + 20.0 * weight2)

    for r, n in spans(8, 8 + size0, 16):
        lap_even, lap_odd, _, _ = five_point(h_ref, r, n)
        mask = mask0[pl.ds(r, n), :]
        g_ref[0, pl.ds(r, n), :] = mask * lap_even
        g_ref[1, pl.ds(r, n), :] = mask * lap_odd
    for r, n in spans(8, 8 + size0, 16):
        bi_even, bi_odd, _, _ = five_point(g_ref, r, n)
        h_both = h_ref[0, pl.ds(r, n), :] + h_ref[1, pl.ds(r, n), :]
        t_ref[pl.ds(r, n), :] = mask0[pl.ds(r, n), :] * (
            h_both - s0 * (4.0 * h_both + weight * (bi_even + bi_odd))
        )
    h1[pl.ds(8, size1), :] = 0.25 * (t_ref[pl.ds(8, size1, stride=2), :] + t_ref[pl.ds(9, size1, stride=2), :])
    for r, n in spans(8, 8 + size1, 32):
        lap, _ = five_coarse(h1, r, n, 1)
        g1[pl.ds(r, n), :] = mask1[pl.ds(r, n), :] * lap
    for r, n in spans(8, 8 + size1, 32):
        bi, _ = five_coarse(g1, r, n, 1)
        here = h1[pl.ds(r, n), :]
        t1[pl.ds(r, n), :] = mask1[pl.ds(r, n), :] * (here - s1 * (4.0 * here + weight1 * bi))
    both = t1[pl.ds(8, size2, stride=2), :] + t1[pl.ds(9, size2, stride=2), :]
    h2[pl.ds(8, size2), :] = 0.25 * (both + jnp.where((lane & 1) == 0, roll(both, -1), roll(both, 1)))
    lap, _ = five_coarse(h2, 8, size2, 2)
    g2[pl.ds(8, size2), :] = mask2[pl.ds(8, size2), :] * lap
    bi, _ = five_coarse(g2, 8, size2, 2)
    here = h2[pl.ds(8, size2), :]
    e2 = mask2[pl.ds(8, size2), :] * (s2 * (2.0 * here - s2 * (4.0 * here + weight2 * bi)))
    t1[pl.ds(8, size2, stride=2), :] = e2
    t1[pl.ds(9, size2, stride=2), :] = e2
    for r, n in spans(8, 8 + size1, 32):
        w1[pl.ds(r, n), :] = s1 * h1[pl.ds(r, n), :] + t1[pl.ds(r, n), :]
    for r, n in spans(8, 8 + size1, 32):
        lap, _ = five_coarse(w1, r, n, 1)
        g1[pl.ds(r, n), :] = mask1[pl.ds(r, n), :] * lap
    for r, n in spans(8, 8 + size1, 32):
        bi, _ = five_coarse(g1, r, n, 1)
        here = w1[pl.ds(r, n), :]
        t1[pl.ds(r, n), :] = mask1[pl.ds(r, n), :] * (
            here + s1 * (h1[pl.ds(r, n), :] - 4.0 * here - weight1 * bi)
        )
    e1 = t1[pl.ds(8, size1), :]
    t_ref[pl.ds(8, size1, stride=2), :] = e1
    t_ref[pl.ds(9, size1, stride=2), :] = e1
    for r, n in spans(8, 8 + size0, 16):
        copied = t_ref[pl.ds(r, n), :]
        for plane in range(2):
            w_ref[plane, pl.ds(r, n), :] = s0 * h_ref[plane, pl.ds(r, n), :] + copied
    for r, n in spans(8, 8 + size0, 16):
        lap_even, lap_odd, _, _ = five_point(w_ref, r, n)
        mask = mask0[pl.ds(r, n), :]
        g_ref[0, pl.ds(r, n), :] = mask * lap_even
        g_ref[1, pl.ds(r, n), :] = mask * lap_odd
    for r, n in spans(8, 8 + size0, 16):
        bi = five_point(g_ref, r, n)[:2]
        mask = mask0[pl.ds(r, n), :]
        for plane in range(2):
            here = w_ref[plane, pl.ds(r, n), :]
            out_ref[plane, pl.ds(r, n), :] = mask * (
                here + s0 * (h_ref[plane, pl.ds(r, n), :] - 4.0 * here - weight * bi[plane])
            )


def vcycle_scratch(depth, rows, slots):
    size0 = rows + 2 * depth
    one = lambda size: pltpu.VMEM((size + 16, LANES), F32)
    two = pltpu.VMEM((2, size0 + 16, LANES), F32)
    size1, size2 = size0 // 2, size0 // 4
    work = [two, two, one(size0), one(size1), one(size1), one(size1), one(size1), one(size2), one(size2)]
    positions = min(slots, 2)
    return work + [pltpu.VMEM((positions, size + 16, LANES), F32) for size in (size0, size1, size2)]


def prepare_vcycle(meta, depth, rows, masks, work):
    size0 = rows + 2 * depth
    sizes = (size0, size0 // 2, size0 // 4)
    for level, (mask, size) in enumerate(zip(masks, sizes)):
        for position in range(mask.shape[0]):
            for r, n in spans(0, size + 16, 64):
                mask[position, pl.ds(r, n), :] = mask_rows(
                    meta, position, r - 8 - (depth >> level), n, rows >> level
                )
    g_ref, w_ref, t_ref, h1, g1, w1, t1, h2, g2 = work
    for plane in range(2):
        zero_rows(w_ref, (plane,), ((0, 8), (size0 + 8, size0 + 16)))
    for ref, size in ((h1, sizes[1]), (g1, sizes[1]), (w1, sizes[1]), (h2, sizes[2]), (g2, sizes[2])):
        zero_rows(ref, (), ((0, 8), (size + 8, size + 16)))


def bilaplace_into(x_ref, x_base, g_ref, low, high, mask_of):
    for r, n in spans(low - 8, high + 8, 16):
        lap_even, lap_odd, _, _ = five_point(x_ref, r + x_base, n)
        mask = mask_of(r, n)
        g_ref[0, pl.ds(r - low + 8, n), :] = mask * lap_even
        g_ref[1, pl.ds(r - low + 8, n), :] = mask * lap_odd


def fold(values):
    total = values[0:8]
    for k in range(8, values.shape[0], 8):
        total = total + values[k : k + 8]
    return total


def order_inputs(start_ref, rhs_ref, reg_ref, xr_ref):
    rows = start_ref.shape[1]
    matrix = selection(
        (LANES, LANES), lambda s, t: s == 2 * (t & (HALF - 1)) + (t >= HALF).astype(jnp.int32)
    )
    xr_ref[pl.ds(0, rows), :] = exact_dot(start_ref[0], matrix)
    xr_ref[pl.ds(rows, rows), :] = exact_dot(rhs_ref[0], matrix)
    xr_ref[pl.ds(2 * rows, 8), :] = jnp.full((8, LANES), reg_ref[0], F32)


def order_valid(meta_ref, valid_ref, own_ref, a_ref, b_ref):
    meta = Meta(meta_ref)
    guides, rows = valid_ref.shape[:2]
    matrix = selection(
        (2 * LANES, 2 * LANES),
        lambda s, t: s
        == ((t >> 6) & 1) * LANES + 2 * (t & (HALF - 1)) + (t >= LANES).astype(jnp.int32),
    )
    for q in range((guides + 1) // 2):
        pair = [valid_ref[min(2 * q + k, guides - 1)].astype(F32).astype(BF16) for k in range(2)]
        planes = DOT(jnp.concatenate(pair, axis=1), matrix)
        for t in range(2):
            own_ref[q, t] = planes[:, t * LANES : (t + 1) * LANES]
            send_rows(
                meta, lambda r, n: own_ref[q, t, pl.ds(r, n), :], V_HALO, rows, a_ref, b_ref, (2 * q + t) * V_HALO
            )


def pair_inputs(slots, rows, meta_ref, *refs):
    meta = Meta(meta_ref)
    xr_refs, (x_ref, r_ref, reg_ref, a_ref, b_ref) = refs[:slots], refs[slots:]
    low = lane_iota() < HALF
    for slot in range(slots):
        reg_ref[pl.ds(8 * slot, 8), :] = xr_refs[slot][pl.ds(2 * rows, 8), :]
    for q in range((slots + 1) // 2):
        first, second = xr_refs[2 * q], xr_refs[min(2 * q + 1, slots - 1)]
        for out, at in ((x_ref, 0), (r_ref, rows)):
            for r, n in spans(0, rows, 32):
                one, two = first[pl.ds(at + r, n), :], second[pl.ds(at + r, n), :]
                out[q, 0, pl.ds(r, n), :] = jnp.where(low, one, roll(two, HALF))
                out[q, 1, pl.ds(r, n), :] = jnp.where(low, roll(one, HALF), two)
        for t in range(2):
            base = (2 * q + t) * (X_HALO + R_HALO)
            send_rows(meta, lambda r, n: x_ref[q, t, pl.ds(r, n), :], X_HALO, rows, a_ref, b_ref, base)
            send_rows(meta, lambda r, n: r_ref[q, t, pl.ds(r, n), :], R_HALO, rows, a_ref, b_ref, base + X_HALO)


def pair_rows(meta, own_ref, a_ref, b_ref, q, stride, at, skip, halo, rows, size=16):
    return rows_with_halo(
        meta,
        lambda t, r, n: own_ref[q, t, pl.ds(r, n), :],
        lambda t, r, n: a_ref[pl.ds((2 * q + t) * stride + at + r, n), :],
        lambda t, r, n: b_ref[pl.ds((2 * q + t) * stride + at + r, n), :],
        skip, halo, rows, size,
    )


def pack_columns(meta, mask, groups, out_a, out_b):
    base = 0
    for halo, groups_rows in groups:
        low = None
        for r, n, get in groups_rows:
            low = r if low is None else low
            a, b = send_columns(mask, get(0), get(1))
            out_a[pl.ds(base + r - low, n), :] = a
            out_b[pl.ds(base + r - low, n), :] = b
            end = base + r - low + n
        base = end


def pack_first(meta_ref, x_ref, r_ref, v_ref, xa, xb, va, vb, a_ref, b_ref, far_a, far_b):
    meta = Meta(meta_ref)
    mask = side_mask(meta)
    pairs, _, rows, _ = x_ref.shape
    stride = X_HALO + R_HALO
    groups = [(X_HALO, pair_rows(meta, x_ref, xa, xb, q, stride, 0, 0, X_HALO, rows)) for q in range(pairs)]
    groups += [(R_HALO, pair_rows(meta, r_ref, xa, xb, q, stride, X_HALO, 0, R_HALO, rows)) for q in range(pairs)]
    groups += [
        (V_NEAR, pair_rows(meta, v_ref, va, vb, q, V_HALO, 0, V_HALO - V_NEAR, V_NEAR, rows))
        for q in range(v_ref.shape[0])
    ]
    pack_columns(meta, mask, groups, a_ref, b_ref)
    far = V_HALO - V_NEAR
    for q in range(v_ref.shape[0]):
        for r, n, get in pair_rows(meta, v_ref, va, vb, q, V_HALO, 0, 0, V_HALO, rows, 8):
            at = r + V_HALO if r < -V_NEAR else r - rows - V_NEAR + far
            if r < -V_NEAR or r >= rows + V_NEAR:
                a, b = send_columns(mask, get(0), get(1))
                far_a[pl.ds(2 * far * q + at, n), :] = a
                far_b[pl.ds(2 * far * q + at, n), :] = b


def spread_valid(meta_ref, v_ref, va, vb, near_a, near_b, far_a, far_b, out_ref, halo=V_HALO, near_base=0):
    meta = Meta(meta_ref)
    mask = side_mask(meta)
    pairs, _, rows, _ = v_ref.shape
    far = V_HALO - V_NEAR
    for q in range(pairs):
        for r, n, get in pair_rows(meta, v_ref, va, vb, q, V_HALO, 0, V_HALO - halo, halo, rows, 8):
            if r < -V_NEAR:
                a, b, at = far_a, far_b, 2 * far * q + r + V_HALO
            elif r >= rows + V_NEAR:
                a, b, at = far_a, far_b, 2 * far * q + r - rows - V_NEAR + far
            else:
                a, b, at = near_a, near_b, near_base + (rows + 2 * V_NEAR) * q + r + V_NEAR
            fields = with_columns(meta, mask, get(0), get(1), a[pl.ds(at, n), :], b[pl.ds(at, n), :])
            for k, planes in enumerate(fields):
                if 2 * q + k < out_ref.shape[0]:
                    for t in range(2):
                        out_ref[2 * q + k, t, pl.ds(r + halo, n), :] = planes[t]


def load_fields(meta, mask, slots, q, rows_iter, a_ref, b_ref, base, shift, x_ref, x_base):
    for r, n, get in rows_iter:
        at = base + r + shift
        fields = with_columns(meta, mask, get(0), get(1), a_ref[pl.ds(at, n), :], b_ref[pl.ds(at, n), :])
        for k, planes in enumerate(fields):
            if 2 * q + k < slots:
                store_field(x_ref, 2 * q + k, r + x_base, n, *planes)


def stage_first(slots, meta_ref, shifts_ref, frac_ref, own_ref, r_ref, v_ref, reg_ref, xa, xb, va, vb, ga, gb, *refs):
    z_ref, out_a, out_b, res_ref, dot_ref = refs[:5]
    x_ref, valid_ref, m_ref, acc_ref, z_planes, *rest = refs[5:]
    work, masks = rest[:9], rest[9:12]
    meta = Meta(meta_ref)
    mask = side_mask(meta)
    pairs, _, rows, _ = own_ref.shape
    x_base, m_base, acc_base = X_HALO + 8, V_NEAR + 8, DEPTH1 + 8
    prepare_vcycle(meta, DEPTH1, rows, masks, work)
    total = rows + 2 * X_HALO
    total_r = rows + 2 * R_HALO
    stride = X_HALO + R_HALO
    for q in range(pairs):
        load_fields(
            meta, mask, slots, q, pair_rows(meta, own_ref, xa, xb, q, stride, 0, 0, X_HALO, rows),
            ga, gb, q * total, X_HALO, x_ref, x_base,
        )
    for k in range(slots):
        for plane in range(4):
            zero_rows(x_ref, (k, plane), ((0, 8), (total + 8, total + 16)))
        clear_planes(acc_ref, (k,))
    for plane in range(2):
        zero_rows(m_ref, (plane,), ((0, 8), (rows + 2 * V_NEAR + 8, rows + 2 * V_NEAR + 16)))
    spread_valid(
        meta_ref, v_ref, va, vb, ga, gb, None, None, valid_ref, V_NEAR, pairs * (total + total_r)
    )
    guide_loop(
        meta, shifts_ref, frac_ref, (x_ref, x_base), (valid_ref, V_NEAR), (m_ref, m_base), (acc_ref, acc_base),
        (-V_NEAR, rows + V_NEAR), (-DEPTH1, rows + DEPTH1), slots, slots,
    )
    g_ref = work[0]
    dot_ref[...] = jnp.zeros((8, LANES), F32)
    for q in range(pairs):
        base = pairs * total + q * total_r + R_HALO
        for r, n, get in pair_rows(meta, r_ref, xa, xb, q, stride, X_HALO, 0, R_HALO, rows):
            fields = with_columns(
                meta, mask, get(0), get(1), ga[pl.ds(base + r, n), :], gb[pl.ds(base + r, n), :]
            )
            at = r + DEPTH1 + 8
            for k, planes in enumerate(fields):
                if 2 * q + k < slots:
                    for t in range(2):
                        acc_ref[2 * q + k, t, pl.ds(at, n), :] = planes[t] - (
                            acc_ref[2 * q + k, t, pl.ds(at, n), :] + 0.1 * x_ref[2 * q + k, t, pl.ds(r + x_base, n), :]
                        )
    for k in range(slots):
        weight = reg_ref[pl.ds(8 * k, 1), :]
        own_masks = [m.at[k & 1] for m in masks]
        bilaplace_into(
            x_ref.at[k], x_base, g_ref, -DEPTH1, rows + DEPTH1,
            lambda r, n: own_masks[0][pl.ds(r + DEPTH1 + 8, n), :],
        )
        h_ref = acc_ref.at[k]
        for at, n in spans(8, rows + 2 * DEPTH1 + 8, 16):
            bi = five_point(g_ref, at, n)[:2]
            inside = own_masks[0][pl.ds(at, n), :]
            for t in range(2):
                h_ref[t, pl.ds(at, n), :] = inside * (h_ref[t, pl.ds(at, n), :] - weight * bi[t])
        for t in range(2):
            zero_rows(g_ref, (t,), ((0, 8), (rows + 2 * DEPTH1 + 8, rows + 2 * DEPTH1 + 16)))
        vcycle(h_ref, z_planes.at[k], weight, DEPTH1, rows, own_masks, work)
    for q in range(pairs):
        one, two = 2 * q, min(2 * q + 1, slots - 1)
        for r, n in spans(0, rows, 16):
            rows_at = pl.ds(r + DEPTH1 + 8, n)
            for t in range(2):
                z = merge(z_planes[one, t, rows_at, :], z_planes[two, t, rows_at, :])
                res = merge(acc_ref[one, t, rows_at, :], acc_ref[two, t, rows_at, :])
                z_ref[q, t, pl.ds(r, n), :] = z
                if q == 0:
                    res_ref[t, pl.ds(r, n), :] = res
                dot_ref[...] += fold(own_lanes(slots, q) * (z * res))
        for t in range(2):
            send_rows(
                meta, lambda r, n: z_ref[q, t, pl.ds(r, n), :], Z_HALO, rows, out_a, out_b, (2 * q + t) * Z_HALO
            )


def own_lanes(slots, q):
    return 1.0 if 2 * q + 1 < slots else (lane_iota() < HALF).astype(F32)


def pack_second(meta_ref, z_ref, za, zb, a_ref, b_ref):
    meta = Meta(meta_ref)
    pairs, _, rows, _ = z_ref.shape
    groups = [(Z_HALO, pair_rows(meta, z_ref, za, zb, q, Z_HALO, 0, 0, Z_HALO, rows)) for q in range(pairs)]
    pack_columns(meta, side_mask(meta), groups, a_ref, b_ref)


def stage_second(slots, meta_ref, shifts_ref, frac_ref, z_ref, reg_ref, valid_ref, za, zb, ga, gb, *refs):
    y_ref, out_a, out_b, image_ref, dot_zq, dot_yq = refs[:6]
    x_ref, m_ref, acc_ref, y_planes, *rest = refs[6:]
    work, masks = rest[:9], rest[9:12]
    meta = Meta(meta_ref)
    mask = side_mask(meta)
    pairs, _, rows, _ = z_ref.shape
    x_base, m_base, acc_base = Z_HALO, V_HALO + 8, DEPTH2 + 8
    prepare_vcycle(meta, DEPTH2, rows, masks, work)
    total = rows + 2 * Z_HALO
    for q in range(pairs):
        load_fields(
            meta, mask, slots, q, pair_rows(meta, z_ref, za, zb, q, Z_HALO, 0, 0, Z_HALO, rows),
            ga, gb, q * total, Z_HALO, x_ref, x_base,
        )
    for k in range(slots):
        for plane in range(4):
            zero_rows(x_ref, (k, plane), ((total, total + 8),))
        clear_planes(acc_ref, (k,))
    for plane in range(2):
        zero_rows(m_ref, (plane,), ((0, 8), (rows + 2 * V_HALO + 8, rows + 2 * V_HALO + 16)))
    guide_loop(
        meta, shifts_ref, frac_ref, (x_ref, x_base), (valid_ref, V_HALO), (m_ref, m_base), (acc_ref, acc_base),
        (-V_HALO, rows + V_HALO), (-DEPTH2, rows + DEPTH2), slots, slots,
    )
    g_ref = work[0]
    for k in range(slots):
        weight = reg_ref[pl.ds(8 * k, 1), :]
        own_masks = [m.at[k & 1] for m in masks]
        bilaplace_into(
            x_ref.at[k], x_base, g_ref, -DEPTH2, rows + DEPTH2,
            lambda r, n: own_masks[0][pl.ds(r + DEPTH2 + 8, n), :],
        )
        h_ref = acc_ref.at[k]
        for r, n in spans(-DEPTH2, rows + DEPTH2, 16):
            at = r + DEPTH2 + 8
            bi = five_point(g_ref, at, n)[:2]
            inside = own_masks[0][pl.ds(at, n), :]
            for t in range(2):
                h_ref[t, pl.ds(at, n), :] = inside * (
                    h_ref[t, pl.ds(at, n), :] + weight * bi[t] + 0.1 * x_ref[k, t, pl.ds(r + x_base, n), :]
                )
        for t in range(2):
            zero_rows(g_ref, (t,), ((0, 8), (rows + 2 * DEPTH2 + 8, rows + 2 * DEPTH2 + 16)))
        vcycle(h_ref, y_planes.at[k], weight, DEPTH2, rows, own_masks, work)
    dot_zq[...] = jnp.zeros((8, LANES), F32)
    dot_yq[...] = jnp.zeros((8, LANES), F32)
    total_y = rows + 2 * Y_HALO
    for q in range(pairs):
        one, two = 2 * q, min(2 * q + 1, slots - 1)
        for r, n in spans(-Y_HALO, rows + Y_HALO, 8):
            rows_at = pl.ds(r + DEPTH2 + 8, n)
            y = [merge(y_planes[one, t, rows_at, :], y_planes[two, t, rows_at, :]) for t in range(2)]
            at = pl.ds(q * total_y + r + Y_HALO, n)
            out_a[at, :], out_b[at, :] = send_columns(mask, *y)
            for t in range(2):
                y_ref[q, t, pl.ds(r + Y_HALO, n), :] = y[t]
                if 0 <= r < rows:
                    image = merge(acc_ref[one, t, rows_at, :], acc_ref[two, t, rows_at, :])
                    z = z_ref[q, t, pl.ds(r, n), :]
                    own = own_lanes(slots, q)
                    dot_zq[...] += fold(own * (z * image))
                    dot_yq[...] += fold(own * (y[t] * image))
                    if q == 0:
                        image_ref[t, pl.ds(r, n), :] = image


def stage_third(slots, meta_ref, shifts_ref, frac_ref, y_ref, reg_ref, valid_ref, dot_rz, dot_zq, dot_yq, ga, gb, *refs):
    image_ref, sums_ref, x_ref, m_ref, acc_ref, g_ref, square_ref, mask_ref = refs
    meta = Meta(meta_ref)
    mask = side_mask(meta)
    pairs, _, total, _ = y_ref.shape
    rows = total - 2 * Y_HALO
    x_base, m_base = Y_HALO, 24
    for q in range(pairs):
        load_fields(
            meta, mask, slots, q,
            [(r, n, lambda t, r=r, n=n: y_ref[q, t, pl.ds(r, n), :]) for r, n in spans(0, total, 16)],
            ga, gb, q * total, 0, x_ref, 0,
        )
    for k in range(slots):
        for plane in range(4):
            zero_rows(x_ref, (k, plane), ((total, total + 8),))
    clear_planes(acc_ref, (0,))
    square_ref[...] = jnp.zeros((8, LANES), F32)
    for position in range(mask_ref.shape[0]):
        for r, n in spans(-8, rows + 8, 48):
            mask_ref[position, pl.ds(r + 8, n), :] = mask_rows(meta, position, r, n, rows)
    guide_loop(
        meta, shifts_ref, frac_ref, (x_ref, x_base), (valid_ref, V_HALO), (m_ref, m_base), (acc_ref, 0),
        (-24, rows + 24), (0, rows), slots, 1, square_ref, rows,
    )
    for k in reversed(range(slots)):
        weight = reg_ref[pl.ds(8 * k, 1), :]
        bilaplace_into(
            x_ref.at[k], x_base, g_ref, 0, rows, lambda r, n: mask_ref[k & 1, pl.ds(r + 8, n), :]
        )
        own = (((lane_iota() - HALF * (k & 1)) & (LANES - 1)) < HALF).astype(F32)
        for r, n in spans(0, rows, 16):
            x = x_ref[k, 0, pl.ds(r + x_base, n), :], x_ref[k, 1, pl.ds(r + x_base, n), :]
            if k == 0:
                bi_even, bi_odd, g_even, g_odd = five_point(g_ref, r + 8, n)
                image_ref[0, pl.ds(r, n), :] = acc_ref[0, 0, pl.ds(r, n), :] + weight * bi_even + 0.1 * x[0]
                image_ref[1, pl.ds(r, n), :] = acc_ref[0, 1, pl.ds(r, n), :] + weight * bi_odd + 0.1 * x[1]
            else:
                g_even, g_odd = g_ref[0, pl.ds(r + 8, n), :], g_ref[1, pl.ds(r + 8, n), :]
            square_ref[...] += own * fold(
                weight * (g_even * g_even + g_odd * g_odd) + 0.1 * (x[0] * x[0] + x[1] * x[1])
            )
    row = lax.broadcasted_iota(jnp.int32, (8, LANES), 0)
    packed = jnp.zeros((8, LANES), F32)
    for at, part in enumerate((dot_rz[...], dot_zq[...], dot_yq[...], square_ref[...])):
        packed = jnp.where(row == at, jnp.sum(part, axis=0, keepdims=True), packed)
    for d in range(sums_ref.shape[0]):
        sums_ref[d] = packed


def finish(start_ref, z_ref, res_ref, q_ref, y_ref, p_ref, sums_ref, solution_ref, residual_ref):
    rows = start_ref.shape[1]
    total = sums_ref[0]
    for d in range(1, sums_ref.shape[0]):
        total = total + sums_ref[d]
    total = jnp.sum(total, axis=1, keepdims=True)
    rz, zq, yq, yp = (total[k : k + 1] for k in range(4))
    alpha = rz / zq
    rz_next = alpha * alpha * yq - rz
    grown = 1.0 + rz_next / rz
    alpha_next = rz_next / (grown * grown * zq - 2.0 * alpha * grown * yq + alpha * alpha * yp)
    matrix = selection(
        (2 * LANES, LANES), lambda s, t: s == (t >> 1) + LANES * (t & 1)
    )
    c_z = alpha + alpha_next * grown
    c_y = alpha_next * alpha
    step, rest = [], []
    for t in range(2):
        step.append(c_z * z_ref[0, t] - c_y * y_ref[0, t, pl.ds(Y_HALO, rows), :])
        rest.append(res_ref[t] - (c_z * q_ref[t] - c_y * p_ref[t]))
    solution_ref[0] = start_ref[0] + exact_dot(jnp.concatenate(step, axis=1), matrix)
    residual_ref[0] = exact_dot(jnp.concatenate(rest, axis=1), matrix)


def call(kernel, outs, *args, scratch=(), scalars=0, fetched=0):
    n_in, n_out = len(args), len(outs)
    spaces = [pltpu.SMEM] * scalars + [pltpu.VMEM] * (n_in - scalars - fetched) + [pl.ANY] * fetched
    landing = [pltpu.VMEM(a.shape, a.dtype) for a in args[n_in - fetched :]] if fetched else []

    def run(*refs):
        ins, outputs, rest = refs[:n_in], refs[n_in : n_in + n_out], refs[n_in + n_out :]
        if fetched:
            held, sems, rest = rest[:fetched], rest[fetched], rest[fetched + 1 :]
            copies = [
                pltpu.make_async_copy(src, dst, sems.at[k])
                for k, (src, dst) in enumerate(zip(ins[n_in - fetched :], held))
            ]
            for copy in copies:
                copy.start()
            for copy in copies:
                copy.wait()
            ins = ins[: n_in - fetched] + held
        kernel(*ins, *outputs, *rest)

    return pl.pallas_call(
        run,
        out_shape=[jax.ShapeDtypeStruct(shape, F32) for shape in outs],
        in_specs=[pl.BlockSpec(memory_space=space) for space in spaces],
        out_specs=[pl.BlockSpec(memory_space=pltpu.VMEM)] * n_out,
        scratch_shapes=[*landing, *([pltpu.SemaphoreType.DMA((fetched,))] if fetched else []), *scratch],
    )(*args)


def swap(a, b, axis, closed):
    n = lax.axis_size(axis)
    first = [(i, i ^ 1 if i ^ 1 < n else i) for i in range(n)]
    last = lambda i: i - 1 if i % 2 == 0 else i + 1
    if closed and n % 2 == 0:
        second = [(i, last(i) % n) for i in range(n)]
    else:
        second = [(i, last(i) if 0 <= last(i) < n else i) for i in range(n)]
    return lax.ppermute(a, axis, first), lax.ppermute(b, axis, second)


def shards(rhs, start, valid, reg, shifts, frac):
    rows = rhs.shape[1]
    guides = valid.shape[0]
    slots = lax.axis_size("layer")
    gx, gy = lax.axis_index("gx"), lax.axis_index("gy")
    n_gx, n_gy = lax.axis_size("gx"), lax.axis_size("gy")
    at = jnp.arange(8, dtype=jnp.int32)
    meta = jnp.zeros((8,), jnp.int32)
    for k, value in enumerate(
        (gx > 0, gx < n_gx - 1, gy > 0, gy < n_gy - 1, lax.axis_index("layer"), gx & 1, gy & 1)
    ):
        meta = jnp.where(at == k, value.astype(jnp.int32), meta)
    shifts, frac = shifts.reshape(-1), frac.reshape(-1)
    pairs, maps = (slots + 1) // 2, (guides + 1) // 2
    vmem = lambda *shape: pltpu.VMEM((*shape, LANES), F32)

    xr = pl.pallas_call(
        order_inputs,
        out_shape=jax.ShapeDtypeStruct((2 * rows + 8, LANES), F32),
        in_specs=[pl.BlockSpec(memory_space=pltpu.VMEM)] * 2 + [pl.BlockSpec(memory_space=pltpu.SMEM)],
        out_specs=pl.BlockSpec(memory_space=pltpu.VMEM),
    )(start, rhs, reg)
    strip = (maps * 2 * V_HALO, LANES)
    v_own, va, vb = call(order_valid, ((maps, 2, rows, LANES), strip, strip), meta, valid, scalars=1)
    va, vb = swap(va, vb, "gx", False)
    others = [lax.ppermute(xr, "layer", [(i, (i + k) % slots) for i in range(slots)]) for k in range(1, slots)]
    tile = (pairs, 2, rows, LANES)
    strip = (pairs * 2 * (X_HALO + R_HALO), LANES)
    x_own, r_own, weights, xa, xb = call(
        functools.partial(pair_inputs, slots, rows),
        (tile, tile, (8 * slots, LANES), strip, strip),
        meta, xr, *others,
        scalars=1, fetched=len(others),
    )
    xa, xb = swap(xa, xb, "gx", False)
    near = (pairs * (2 * rows + 2 * X_HALO + 2 * R_HALO) + maps * (rows + 2 * V_NEAR), LANES)
    far = (maps * 2 * (V_HALO - V_NEAR), LANES)
    ga, gb, fa, fb = call(
        pack_first, (near, near, far, far), meta, x_own, r_own, v_own, xa, xb, va, vb, scalars=1, fetched=4
    )
    ga, gb = swap(ga, gb, "gy", False)
    fa, fb = swap(fa, fb, "gy", False)

    size = rows + 2 * DEPTH1 + 16
    strip = (pairs * 2 * Z_HALO, LANES)
    z, za, zb, res, dot_rz = call(
        functools.partial(stage_first, slots),
        (tile, strip, strip, (2, rows, LANES), (8, LANES)),
        meta, shifts, frac, x_own, r_own, v_own, weights, xa, xb, va, vb, ga, gb,
        scalars=3, fetched=6,
        scratch=[
            vmem(slots, 4, rows + 2 * X_HALO + 16),
            vmem(guides, 2, rows + 2 * V_NEAR),
            vmem(2, rows + 2 * V_NEAR + 16),
            vmem(slots, 2, size),
            vmem(slots, 2, size),
            *vcycle_scratch(DEPTH1, rows, slots),
        ],
    )
    za, zb = swap(za, zb, "gx", False)
    (spread,) = call(
        functools.partial(spread_valid, near_base=pairs * (2 * rows + 2 * X_HALO + 2 * R_HALO)),
        ((guides, 2, rows + 2 * V_HALO, LANES),),
        meta, v_own, va, vb, ga, gb, fa, fb,
        scalars=1, fetched=6,
    )
    strip = (pairs * (rows + 2 * Z_HALO), LANES)
    ka, kb = call(pack_second, (strip, strip), meta, z, za, zb, scalars=1, fetched=2)
    ka, kb = swap(ka, kb, "gy", True)

    size = rows + 2 * DEPTH2 + 16
    strip = (pairs * (rows + 2 * Y_HALO), LANES)
    y, ya, yb, image, dot_zq, dot_yq = call(
        functools.partial(stage_second, slots),
        ((pairs, 2, rows + 2 * Y_HALO, LANES), strip, strip, (2, rows, LANES), (8, LANES), (8, LANES)),
        meta, shifts, frac, z, weights, spread, za, zb, ka, kb,
        scalars=3, fetched=4,
        scratch=[
            vmem(slots, 4, rows + 2 * Z_HALO + 8),
            vmem(2, rows + 2 * V_HALO + 16),
            vmem(slots, 2, size),
            vmem(slots, 2, size),
            *vcycle_scratch(DEPTH2, rows, slots),
        ],
    )
    ya, yb = swap(ya, yb, "gy", True)

    image_y, sums = call(
        functools.partial(stage_third, slots),
        ((2, rows, LANES), (n_gx * n_gy, 8, LANES)),
        meta, shifts, frac, y, weights, spread, dot_rz, dot_zq, dot_yq, ya, yb,
        scalars=3, fetched=2,
        scratch=[
            vmem(slots, 4, rows + 2 * Y_HALO + 8),
            vmem(2, rows + 48),
            vmem(1, 2, rows),
            vmem(2, rows + 16),
            vmem(8),
            vmem(min(slots, 2), rows + 16),
        ],
    )
    sums = lax.all_to_all(sums, ("gx", "gy"), 0, 0)
    return call(finish, ((1, rows, LANES), (1, rows, LANES)), start, z, res, image, y, image_y, sums)


def solution(mesh):
    in_specs = (
        P("layer", "gx", "gy"),
        P("layer", "gx", "gy"),
        P(None, "gx", "gy"),
        P("layer"),
        P(),
        P(),
    )
    out_specs = (P("layer", "gx", "gy"), P("layer", "gx", "gy"))

    def run(*args):
        return tuple(jax.shard_map(shards, mesh=mesh, in_specs=in_specs, out_specs=out_specs, check_vma=False)(*args))

    return run
```

```python
import functools

import jax
import jax.numpy as jnp
from jax import lax
from jax.experimental import pallas as pl
from jax.experimental.pallas import tpu as pltpu
from jax.sharding import PartitionSpec as P

GUIDES = 8
SHIFT_MAX = 16
LANES = 128
HALF = LANES // 2
QUART = LANES // 4
F32 = jnp.float32
BF16 = jnp.bfloat16
DOT = functools.partial(jnp.dot, preferred_element_type=F32)

X_HALO, R_HALO, V_HALO, V_NEAR, Z_HALO, Y_HALO = 56, 24, 72, 40, 88, 40
DEPTH1, DEPTH2 = 24, 56
VMEM_LIMIT = 16 << 20
V_CLOSED = True


def lane_iota(shape=(1, LANES)):
    return lax.broadcasted_iota(jnp.int32, shape, len(shape) - 1)


def roll(x, amount):
    amount = amount % LANES if isinstance(amount, int) else amount & (LANES - 1)
    if isinstance(amount, int) and amount == 0:
        return x
    return pltpu.roll(x, amount, x.ndim - 1)


def spans(low, high, size):
    return [(r, min(size, high - r)) for r in range(low, high, size)]


class Meta:
    def __init__(self, ref):
        self.top_ok, self.bottom_ok, self.left_ok, self.right_ok = (ref[k].astype(F32) for k in range(4))
        self.layer, self.gx_odd, self.gy_odd = ref[4], ref[5], ref[6]


def exact_dot(values, matrix):
    high = values.astype(BF16)
    rest = values - high.astype(F32)
    mid = rest.astype(BF16)
    low = (rest - mid.astype(F32)).astype(BF16)
    return DOT(high, matrix) + (DOT(mid, matrix) + DOT(low, matrix))


def selection(shape, wanted_of):
    source = lax.broadcasted_iota(jnp.int32, shape, 0)
    target = lax.broadcasted_iota(jnp.int32, shape, 1)
    return wanted_of(source, target).astype(F32).astype(BF16)


def send_rows(meta, own_of, halo, rows, out_a, out_b, base):
    for r, n in spans(0, halo, 32):
        up, down = own_of(r, n), own_of(rows - halo + r, n)
        odd = meta.gx_odd == 1
        out_a[pl.ds(base + r, n), :] = jnp.where(odd, up, down)
        out_b[pl.ds(base + r, n), :] = jnp.where(odd, down, up)


def rows_with_halo(meta, own_of, a_of, b_of, skip, halo, rows, size=16):
    odd = meta.gx_odd == 1
    for r, n in spans(0, halo, size):
        yield r - halo, n, lambda t, r=r, n=n: jnp.where(odd, a_of(t, skip + r, n), b_of(t, skip + r, n)) * meta.top_ok
    for r, n in spans(0, rows, size):
        yield r, n, lambda t, r=r, n=n: own_of(t, r, n)
    for r, n in spans(0, halo, size):
        yield rows + r, n, lambda t, r=r, n=n: jnp.where(odd, b_of(t, r, n), a_of(t, r, n)) * meta.bottom_ok


def side_mask(meta):
    return ((lane_iota() >> 5) & 1) == meta.gy_odd


def send_columns(mask, even, odd):
    moved = roll(odd, -QUART)
    return jnp.where(mask, moved, even), jnp.where(mask, even, moved)


def with_columns(meta, mask, even, odd, from_a, from_b):
    lane = lane_iota()
    near = ((lane >> 5) & 1) == 0
    side_even = jnp.where(mask, from_a, from_b) * jnp.where(near, meta.right_ok, meta.left_ok)
    side_odd = jnp.where(mask, from_b, from_a) * jnp.where(near, meta.left_ok, meta.right_ok)
    side_even, side_odd = roll(side_even, HALF), roll(side_odd, -QUART)
    low = lane < HALF
    return (
        (jnp.where(low, even, side_even), jnp.where(low, odd, side_odd)),
        (jnp.where(low, side_even, even), jnp.where(low, side_odd, odd)),
    )


def merge(first, second):
    return jnp.where(lane_iota() < HALF, first, second)


def rows_of(ref, start):
    return lambda r, n: ref[pl.ds(start + r, n), :]


def five_point(ref, at, n):
    even, odd = ref[0, pl.ds(at, n), :], ref[1, pl.ds(at, n), :]
    sum_even = ref[0, pl.ds(at - 1, n), :] + ref[0, pl.ds(at + 1, n), :] + (odd + roll(odd, 1))
    sum_odd = ref[1, pl.ds(at - 1, n), :] + ref[1, pl.ds(at + 1, n), :] + (even + roll(even, -1))
    return sum_even - 4.0 * even, sum_odd - 4.0 * odd, even, odd


def five_coarse(ref, at, n, step):
    here = ref[pl.ds(at, n), :]
    sides = roll(here, step) + roll(here, -step)
    return ref[pl.ds(at - 1, n), :] + ref[pl.ds(at + 1, n), :] + sides - 4.0 * here, here


def mask_rows(meta, position, row_at, n, rows):
    row = row_at + lax.broadcasted_iota(jnp.int32, (n, LANES), 0)
    lane = (lane_iota((n, LANES)) - HALF * position) & (LANES - 1)
    by_row = jnp.where(row < 0, meta.top_ok, jnp.where(row >= rows, meta.bottom_ok, 1.0))
    return by_row * jnp.where(lane < HALF, 1.0, jnp.where(lane < 3 * QUART, meta.right_ok, meta.left_ok))


def guide_loop(meta, table_ref, guides, slots, x=None, valid=None, m=None, acc=None, p_rows=None, outs=None, out_slots=None, footprints=None, square_ref=None, rows=None):
    def coefficients(g, slot):
        layer = lax.rem(meta.layer - slot + slots, slots)
        at = (g * slots + layer) * 2
        there = guides * slots * 2
        return (
            table_ref[at],
            table_ref[at + 1],
            table_ref[there + at].astype(F32) * (1.0 / 256.0),
            table_ref[there + at + 1].astype(F32) * (1.0 / 256.0),
        )

    def between(ref, index, at, step, n, u):
        here = ref[index + (pl.ds(at, n), slice(None))]
        return here + u * (ref[index + (pl.ds(at + step, n), slice(None))] - here)

    def forward(g):
        home = HALF * (g & 1)
        x_ref, x_base = x
        fixed = []
        for slot in range(slots):
            a, b, u, v = coefficients(g, slot)
            amount = home - HALF * (slot & 1) - lax.shift_right_arithmetic(b, 1)
            fixed.append((a, u, v, b & 1, amount & (LANES - 1)))
        squares = []
        for r, n in spans(*p_rows, 16):
            even = odd = None
            for slot in range(slots):
                a, u, v, parity, amount = fixed[slot]
                c0, c1, c2 = (between(x_ref, (slot, parity + k), r + x_base + a, 1, n, u) for k in range(3))
                this_even = roll(c0 + v * (c1 - c0), amount)
                this_odd = roll(c1 + v * (c2 - c1), amount)
                even = this_even if even is None else even + this_even
                odd = this_odd if odd is None else odd + this_odd
            if footprints is not None:
                out_ref, out_base = footprints
                out_ref[g, 0, pl.ds(r + out_base, n), :] = even
                out_ref[g, 1, pl.ds(r + out_base, n), :] = odd
                continue
            (valid_ref, v_base), (m_ref, m_base) = valid, m
            m_even = even * valid_ref[g, 0, pl.ds(r + v_base, n), :]
            m_odd = odd * valid_ref[g, 1, pl.ds(r + v_base, n), :]
            m_ref[0, pl.ds(r + m_base, n), :] = m_even
            m_ref[1, pl.ds(r + m_base, n), :] = m_odd
            if square_ref is not None:
                for k in range(0, n, 8):
                    if 0 <= r + k < rows:
                        sl = slice(k, k + 8)
                        squares.append(m_even[sl] * even[sl] + m_odd[sl] * odd[sl])
        if squares:
            own = (((lane_iota() - home) & (LANES - 1)) < HALF).astype(F32)
            square_ref[...] += own * total_of(squares)

    def backward(g):
        home = HALF * (g & 1)
        (m_ref, m_base), (acc_ref, acc_base) = m, acc
        lead = () if x is not None else (g,)
        for slot in range(out_slots):
            a, b, u, v = coefficients(g, slot)
            back = -b - 1
            parity = back & 1
            amount = HALF * (slot & 1) - home - lax.shift_right_arithmetic(back, 1)
            for r, n in spans(*outs, 16):
                at = r + m_base - a
                plane_a = between(m_ref, (*lead, parity), at, -1, n, u)
                plane_b = between(m_ref, (*lead, 1 - parity), at, -1, n, u)
                q0, q1, q2 = roll(plane_a, amount), roll(plane_b, amount - parity), roll(plane_a, amount - 1)
                acc_ref[slot, 0, pl.ds(r + acc_base, n), :] += q1 + v * (q0 - q1)
                acc_ref[slot, 1, pl.ds(r + acc_base, n), :] += q2 + v * (q1 - q2)

    def body(g, carry):
        if x is not None:
            forward(g)
        if acc is not None:
            backward(g)
        return carry

    lax.fori_loop(0, guides, body, 0)


def store_field(x_ref, slot, at, n, even, odd):
    for plane, value in enumerate((even, odd, roll(even, -1), roll(odd, -1))):
        x_ref[slot, plane, pl.ds(at, n), :] = value


def zero_rows(ref, index, ranges):
    for low, high in ranges:
        if high > low:
            ref[index + (pl.ds(low, high - low), slice(None))] = jnp.zeros((high - low, LANES), F32)


def clear_planes(ref, index):
    for plane in range(2):
        for r, n in spans(0, ref.shape[-2], 64):
            ref[index + (plane, pl.ds(r, n), slice(None))] = jnp.zeros((n, LANES), F32)


def vcycle(h_ref, out_ref, weight, depth, rows, masks, work):
    g_ref, w_ref, t_ref, h1, g1, w1, t1, h2, g2 = work
    mask0, mask1, mask2 = masks
    size0 = rows + 2 * depth
    size1, size2 = size0 // 2, size0 // 4
    lane = lane_iota()
    s0 = 0.5 / (4.0 + 20.0 * weight)
    weight1, weight2 = weight * (1.0 / 16.0), weight * (1.0 / 256.0)
    s1 = 0.5 / (4.0 + 20.0 * weight1)
    s2 = 0.5 / (4.0 + 20.0 * weight2)

    for r, n in spans(8, 8 + size0, 16):
        lap_even, lap_odd, _, _ = five_point(h_ref, r, n)
        mask = mask0[pl.ds(r, n), :]
        g_ref[0, pl.ds(r, n), :] = mask * lap_even
        g_ref[1, pl.ds(r, n), :] = mask * lap_odd
    yield
    for r, n in spans(8, 8 + size0, 16):
        bi_even, bi_odd, _, _ = five_point(g_ref, r, n)
        h_both = h_ref[0, pl.ds(r, n), :] + h_ref[1, pl.ds(r, n), :]
        t_ref[pl.ds(r, n), :] = mask0[pl.ds(r, n), :] * (
            h_both - s0 * (4.0 * h_both + weight * (bi_even + bi_odd))
        )
    h1[pl.ds(8, size1), :] = 0.25 * (t_ref[pl.ds(8, size1, stride=2), :] + t_ref[pl.ds(9, size1, stride=2), :])
    yield
    for r, n in spans(8, 8 + size1, 32):
        lap, _ = five_coarse(h1, r, n, 1)
        g1[pl.ds(r, n), :] = mask1[pl.ds(r, n), :] * lap
    yield
    for r, n in spans(8, 8 + size1, 32):
        bi, _ = five_coarse(g1, r, n, 1)
        here = h1[pl.ds(r, n), :]
        t1[pl.ds(r, n), :] = mask1[pl.ds(r, n), :] * (here - s1 * (4.0 * here + weight1 * bi))
    both = t1[pl.ds(8, size2, stride=2), :] + t1[pl.ds(9, size2, stride=2), :]
    h2[pl.ds(8, size2), :] = 0.25 * (both + jnp.where((lane & 1) == 0, roll(both, -1), roll(both, 1)))
    yield
    lap, _ = five_coarse(h2, 8, size2, 2)
    g2[pl.ds(8, size2), :] = mask2[pl.ds(8, size2), :] * lap
    yield
    bi, _ = five_coarse(g2, 8, size2, 2)
    here = h2[pl.ds(8, size2), :]
    e2 = mask2[pl.ds(8, size2), :] * (s2 * (2.0 * here - s2 * (4.0 * here + weight2 * bi)))
    yield
    t1[pl.ds(8, size2, stride=2), :] = e2
    t1[pl.ds(9, size2, stride=2), :] = e2
    yield
    for r, n in spans(8, 8 + size1, 32):
        w1[pl.ds(r, n), :] = s1 * h1[pl.ds(r, n), :] + t1[pl.ds(r, n), :]
    yield
    for r, n in spans(8, 8 + size1, 32):
        lap, _ = five_coarse(w1, r, n, 1)
        g1[pl.ds(r, n), :] = mask1[pl.ds(r, n), :] * lap
    yield
    for r, n in spans(8, 8 + size1, 32):
        bi, _ = five_coarse(g1, r, n, 1)
        here = w1[pl.ds(r, n), :]
        t1[pl.ds(r, n), :] = mask1[pl.ds(r, n), :] * (
            here + s1 * (h1[pl.ds(r, n), :] - 4.0 * here - weight1 * bi)
        )
    e1 = t1[pl.ds(8, size1), :]
    yield
    t_ref[pl.ds(8, size1, stride=2), :] = e1
    t_ref[pl.ds(9, size1, stride=2), :] = e1
    yield
    for r, n in spans(8, 8 + size0, 16):
        copied = t_ref[pl.ds(r, n), :]
        for plane in range(2):
            w_ref[plane, pl.ds(r, n), :] = s0 * h_ref[plane, pl.ds(r, n), :] + copied
    yield
    for r, n in spans(8, 8 + size0, 16):
        lap_even, lap_odd, _, _ = five_point(w_ref, r, n)
        mask = mask0[pl.ds(r, n), :]
        g_ref[0, pl.ds(r, n), :] = mask * lap_even
        g_ref[1, pl.ds(r, n), :] = mask * lap_odd
    yield
    for r, n in spans(8, 8 + size0, 16):
        bi = five_point(g_ref, r, n)[:2]
        mask = mask0[pl.ds(r, n), :]
        for plane in range(2):
            here = w_ref[plane, pl.ds(r, n), :]
            out_ref[plane, pl.ds(r, n), :] = mask * (
                here + s0 * (h_ref[plane, pl.ds(r, n), :] - 4.0 * here - weight * bi[plane])
            )


def in_step(runs):
    runs = list(runs)
    while runs:
        runs = [run for run in runs if next(run, runs) is not runs]


def vcycle_scratch(depth, rows, slots):
    size0 = rows + 2 * depth
    one = lambda size: pltpu.VMEM((size + 16, LANES), F32)
    two = pltpu.VMEM((2, size0 + 16, LANES), F32)
    size1, size2 = size0 // 2, size0 // 4
    work = [two, two, one(size0), one(size1), one(size1), one(size1), one(size1), one(size2), one(size2)]
    positions = min(slots, 2)
    return work * positions + [pltpu.VMEM((positions, size + 16, LANES), F32) for size in (size0, size1, size2)]


def prepare_vcycle(meta, depth, rows, masks, work):
    size0 = rows + 2 * depth
    sizes = (size0, size0 // 2, size0 // 4)
    for level, (mask, size) in enumerate(zip(masks, sizes)):
        for position in range(mask.shape[0]):
            for r, n in spans(0, size + 16, 64):
                mask[position, pl.ds(r, n), :] = mask_rows(
                    meta, position, r - 8 - (depth >> level), n, rows >> level
                )
    for k in range(0, len(work), 9):
        g_ref, w_ref, t_ref, h1, g1, w1, t1, h2, g2 = work[k : k + 9]
        for plane in range(2):
            zero_rows(w_ref, (plane,), ((0, 8), (size0 + 8, size0 + 16)))
        for ref, size in ((h1, sizes[1]), (g1, sizes[1]), (w1, sizes[1]), (h2, sizes[2]), (g2, sizes[2])):
            zero_rows(ref, (), ((0, 8), (size + 8, size + 16)))


def bilaplace_into(x_ref, x_base, g_ref, low, high, mask_of):
    for r, n in spans(low - 8, high + 8, 16):
        lap_even, lap_odd, _, _ = five_point(x_ref, r + x_base, n)
        mask = mask_of(r, n)
        g_ref[0, pl.ds(r - low + 8, n), :] = mask * lap_even
        g_ref[1, pl.ds(r - low + 8, n), :] = mask * lap_odd


def total_of(parts):
    while len(parts) > 1:
        parts = [sum(parts[k : k + 2][1:], parts[k]) for k in range(0, len(parts), 2)]
    return parts[0]


def fold(values):
    return total_of([values[k : k + 8] for k in range(0, values.shape[0], 8)])


def order_inputs(meta_ref, reg_ref, start_ref, rhs_ref, xr_ref, a_ref, b_ref):
    meta = Meta(meta_ref)
    rows = start_ref.shape[1]
    matrix = selection(
        (LANES, LANES), lambda s, t: s == 2 * (t & (HALF - 1)) + (t >= HALF).astype(jnp.int32)
    )
    xr_ref[pl.ds(0, rows), :] = exact_dot(start_ref[0], matrix)
    xr_ref[pl.ds(rows, rows), :] = exact_dot(rhs_ref[0], matrix)
    xr_ref[pl.ds(2 * rows, 8), :] = jnp.full((8, LANES), reg_ref[0], F32)
    send_rows(meta, lambda r, n: xr_ref[pl.ds(r, n), :], X_HALO, rows, a_ref, b_ref, 0)
    send_rows(meta, lambda r, n: xr_ref[pl.ds(rows + r, n), :], R_HALO, rows, a_ref, b_ref, X_HALO)


def order_valid(meta_ref, valid_ref, _, __, own_ref, a_ref, b_ref):
    meta = Meta(meta_ref)
    guides, rows = valid_ref.shape[:2]
    matrix = selection(
        (2 * LANES, 2 * LANES),
        lambda s, t: s
        == ((t >> 6) & 1) * LANES + 2 * (t & (HALF - 1)) + (t >= LANES).astype(jnp.int32),
    )
    for q in range((guides + 1) // 2):
        pair = [valid_ref[min(2 * q + k, guides - 1)].astype(F32).astype(BF16) for k in range(2)]
        planes = DOT(jnp.concatenate(pair, axis=1), matrix)
        for t in range(2):
            own_ref[q, t] = planes[:, t * LANES : (t + 1) * LANES]
            own = lambda r, n: own_ref[q, t, pl.ds(r, n), :]
            send_rows(meta, own, V_NEAR, rows, a_ref, b_ref, (2 * q + t) * V_NEAR)


def input_rows(meta, slots, xrs, a_refs, b_refs, q, own_at, at, halo, rows):
    one, two = 2 * q, min(2 * q + 1, slots - 1)

    def of(refs, start):
        def get(t, r, n):
            first, second = refs[one][pl.ds(start + r, n), :], refs[two][pl.ds(start + r, n), :]
            return merge(first, roll(second, HALF)) if t == 0 else merge(roll(first, HALF), second)

        return get

    return rows_with_halo(meta, of(xrs, own_at), of(a_refs, at), of(b_refs, at), 0, halo, rows)


def pair_rows(meta, own_ref, a_ref, b_ref, q, stride, at, skip, halo, rows, size=16):
    return rows_with_halo(
        meta,
        lambda t, r, n: own_ref[q, t, pl.ds(r, n), :],
        lambda t, r, n: a_ref[pl.ds((2 * q + t) * stride + at + r, n), :],
        lambda t, r, n: b_ref[pl.ds((2 * q + t) * stride + at + r, n), :],
        skip, halo, rows, size,
    )


def pack_columns(meta, mask, groups, out_a, out_b):
    base = 0
    for halo, groups_rows in groups:
        low = None
        for r, n, get in groups_rows:
            low = r if low is None else low
            a, b = send_columns(mask, get(0), get(1))
            out_a[pl.ds(base + r - low, n), :] = a
            out_b[pl.ds(base + r - low, n), :] = b
            end = base + r - low + n
        base = end


def pack_inputs(slots, meta_ref, *refs):
    xrs, xa, xb = refs[:slots], refs[slots : 2 * slots], refs[2 * slots : 3 * slots]
    _, _, out_a, out_b = refs[3 * slots :]
    meta = Meta(meta_ref)
    mask = side_mask(meta)
    rows = (xrs[0].shape[0] - 8) // 2
    pairs = range((slots + 1) // 2)
    groups = [(X_HALO, input_rows(meta, slots, xrs, xa, xb, q, 0, 0, X_HALO, rows)) for q in pairs]
    groups += [(R_HALO, input_rows(meta, slots, xrs, xa, xb, q, rows, X_HALO, R_HALO, rows)) for q in pairs]
    pack_columns(meta, mask, groups, out_a, out_b)


def pack_valid(meta_ref, v_ref, va, vb, _, __, v_a, v_b, far_a, far_b):
    meta = Meta(meta_ref)
    mask = side_mask(meta)
    maps, _, rows, _ = v_ref.shape
    pack_columns(
        meta, mask,
        [(V_NEAR, pair_rows(meta, v_ref, va, vb, q, V_NEAR, 0, 0, V_NEAR, rows)) for q in range(maps)],
        v_a, v_b,
    )
    gap = V_HALO - V_NEAR
    odd = meta.gx_odd == 1
    for q in range(maps):
        for t in range(2):
            for r, n in spans(0, gap, 32):
                up = v_ref[q, t, pl.ds(V_NEAR + r, n), :]
                down = v_ref[q, t, pl.ds(rows - V_HALO + r, n), :]
                far_a[pl.ds((2 * q + t) * gap + r, n), :] = jnp.where(odd, up, down)
                far_b[pl.ds((2 * q + t) * gap + r, n), :] = jnp.where(odd, down, up)


def far_rows(meta, fa, fb, q):
    gap = V_HALO - V_NEAR
    odd = meta.gx_odd == 1
    for below in range(2):
        scale = meta.bottom_ok if below else meta.top_ok
        for r, n in spans(0, gap, 16):

            def get(t, r=r, n=n):
                rows_at = pl.ds((2 * q + t) * gap + r, n)
                first, second = (fa, fb) if below == 0 else (fb, fa)
                return jnp.where(odd, first[rows_at, :], second[rows_at, :]) * scale

            yield below * gap + r, n, get


def pack_far(meta_ref, fa, fb, _, __, out_a, out_b):
    meta = Meta(meta_ref)
    mask = side_mask(meta)
    gap = V_HALO - V_NEAR
    for q in range(out_a.shape[0] // (2 * gap)):
        for at, n, get in far_rows(meta, fa, fb, q):
            a, b = send_columns(mask, get(0), get(1))
            out_a[pl.ds(2 * gap * q + at, n), :] = a
            out_b[pl.ds(2 * gap * q + at, n), :] = b


def spread_valid(meta, mask, v_ref, va, vb, near_a, near_b, guides, halo, put):
    maps, _, rows, _ = v_ref.shape
    for q in range(maps):
        for r, n, get in pair_rows(meta, v_ref, va, vb, q, V_NEAR, 0, 0, V_NEAR, rows):
            at = pl.ds((rows + 2 * V_NEAR) * q + r + V_NEAR, n)
            fields = with_columns(meta, mask, get(0), get(1), near_a[at, :], near_b[at, :])
            for k, planes in enumerate(fields[: guides - 2 * q]):
                for t in range(2):
                    put(2 * q + k, t, r + halo, n, planes[t])


def spread_all(meta_ref, v_ref, va, vb, near_a, near_b, fa, fb, far_a, far_b, out_ref):
    meta = Meta(meta_ref)
    mask = side_mask(meta)
    guides = out_ref.shape[0]

    def put(g, t, at, n, value):
        out_ref[g, t, pl.ds(at, n), :] = value

    spread_valid(meta, mask, v_ref, va, vb, near_a, near_b, guides, V_HALO, put)
    maps, _, rows, _ = v_ref.shape
    gap = V_HALO - V_NEAR
    for q in range(maps):
        for at, n, get in far_rows(meta, fa, fb, q):
            rows_at = pl.ds(2 * gap * q + at, n)
            where = at if at < gap else at - gap + V_HALO + rows + V_NEAR
            fields = with_columns(meta, mask, get(0), get(1), far_a[rows_at, :], far_b[rows_at, :])
            for k, planes in enumerate(fields[: guides - 2 * q]):
                for t in range(2):
                    put(2 * q + k, t, where, n, planes[t])


def load_fields(meta, mask, slots, q, rows_iter, a_ref, b_ref, base, shift, x_ref, x_base):
    for r, n, get in rows_iter:
        at = base + r + shift
        fields = with_columns(meta, mask, get(0), get(1), a_ref[pl.ds(at, n), :], b_ref[pl.ds(at, n), :])
        for k, planes in enumerate(fields):
            if 2 * q + k < slots:
                store_field(x_ref, 2 * q + k, r + x_base, n, *planes)


def stage_inputs(slots, meta_ref, table_ref, ga, gb, *refs):
    xrs, xa, xb = refs[:slots], refs[slots : 2 * slots], refs[2 * slots : 3 * slots]
    foot_ref, part_ref, reg_ref, x_ref, g_all, mask_ref = refs[3 * slots :]
    meta = Meta(meta_ref)
    mask = side_mask(meta)
    rows = (xrs[0].shape[0] - 8) // 2
    pairs = (slots + 1) // 2
    x_base = X_HALO + 8
    total = rows + 2 * X_HALO
    total_r = rows + 2 * R_HALO
    for k in range(slots):
        reg_ref[pl.ds(8 * k, 8), :] = xrs[k][pl.ds(2 * rows, 8), :]
        for plane in range(4):
            zero_rows(x_ref, (k, plane), ((0, 8), (total + 8, total + 16)))
    for q in range(pairs):
        load_fields(
            meta, mask, slots, q, input_rows(meta, slots, xrs, xa, xb, q, 0, 0, X_HALO, rows),
            ga, gb, q * total, X_HALO, x_ref, x_base,
        )
    for position in range(mask_ref.shape[0]):
        for r, n in spans(0, rows + 2 * DEPTH1 + 16, 32):
            mask_ref[position, pl.ds(r, n), :] = mask_rows(meta, position, r - DEPTH1 - 8, n, rows)
    guide_loop(
        meta, table_ref, foot_ref.shape[0], slots, (x_ref, x_base),
        p_rows=(-V_NEAR, rows + V_NEAR), footprints=(foot_ref, V_NEAR),
    )
    for k in range(slots):
        bilaplace_into(
            x_ref.at[k], x_base, g_all.at[k], -DEPTH1, rows + DEPTH1,
            lambda r, n: mask_ref[k & 1, pl.ds(r + DEPTH1 + 8, n), :],
        )
    for q in range(pairs):
        base = pairs * total + q * total_r + R_HALO
        for r, n, get in input_rows(meta, slots, xrs, xa, xb, q, rows, X_HALO, R_HALO, rows):
            fields = with_columns(
                meta, mask, get(0), get(1), ga[pl.ds(base + r, n), :], gb[pl.ds(base + r, n), :]
            )
            at = r + DEPTH1 + 8
            for k, planes in enumerate(fields[: slots - 2 * q]):
                slot = 2 * q + k
                weight = reg_ref[pl.ds(8 * slot, 1), :]
                bi = five_point(g_all.at[slot], at, n)[:2]
                for t in range(2):
                    part_ref[slot, t, pl.ds(r + DEPTH1, n), :] = (
                        planes[t] - weight * bi[t] - 0.1 * x_ref[slot, t, pl.ds(r + x_base, n), :]
                    )


def stage_first(slots, meta_ref, table_ref, v_ref, va, vb, na, nb, foot_ref, part_ref, reg_ref, _, *refs):
    z_ref, out_a, out_b, res_ref, dot_ref = refs[:5]
    m_ref, acc_ref, z_planes, *rest = refs[5:]
    work, masks = rest[:-3], rest[-3:]
    meta = Meta(meta_ref)
    mask = side_mask(meta)
    maps, _, rows, _ = v_ref.shape
    guides = foot_ref.shape[0]
    pairs = (slots + 1) // 2
    m_base, acc_base = V_NEAR + 8, DEPTH1 + 8
    prepare_vcycle(meta, DEPTH1, rows, masks, work)
    for k in range(slots):
        clear_planes(acc_ref, (k,))
    for g in range(guides):
        for plane in range(2):
            zero_rows(m_ref, (g, plane), ((0, 8), (rows + 2 * V_NEAR + 8, rows + 2 * V_NEAR + 16)))

    def put(g, t, at, n, value):
        m_ref[g, t, pl.ds(at + 8, n), :] = value * foot_ref[g, t, pl.ds(at, n), :]

    spread_valid(meta, mask, v_ref, va, vb, na, nb, guides, V_NEAR, put)
    guide_loop(
        meta, table_ref, guides, slots, m=(m_ref, m_base), acc=(acc_ref, acc_base),
        outs=(-DEPTH1, rows + DEPTH1), out_slots=slots,
    )

    def finish_slot(k):
        weight = reg_ref[pl.ds(8 * k, 1), :]
        own_masks = [m.at[k & 1] for m in masks]
        own_work = work[9 * (k & 1) :][:9]
        h_ref = acc_ref.at[k]
        for at, n in spans(8, rows + 2 * DEPTH1 + 8, 16):
            inside = own_masks[0][pl.ds(at, n), :]
            for t in range(2):
                h_ref[t, pl.ds(at, n), :] = inside * (
                    part_ref[k, t, pl.ds(at - 8, n), :] - h_ref[t, pl.ds(at, n), :]
                )
        for t in range(2):
            zero_rows(own_work[0], (t,), ((0, 8), (rows + 2 * DEPTH1 + 8, rows + 2 * DEPTH1 + 16)))
        yield
        yield from vcycle(h_ref, z_planes.at[k], weight, DEPTH1, rows, own_masks, own_work)

    for q in range(pairs):
        in_step(finish_slot(k) for k in range(2 * q, min(2 * q + 2, slots)))
    dots = []
    for q in range(pairs):
        one, two = 2 * q, min(2 * q + 1, slots - 1)
        for r, n in spans(0, rows, 16):
            rows_at = pl.ds(r + DEPTH1 + 8, n)
            for t in range(2):
                z = merge(z_planes[one, t, rows_at, :], z_planes[two, t, rows_at, :])
                res = merge(acc_ref[one, t, rows_at, :], acc_ref[two, t, rows_at, :])
                z_ref[q, t, pl.ds(r, n), :] = z
                if q == 0:
                    res_ref[t, pl.ds(r, n), :] = res
                dots.append(fold(own_lanes(slots, q) * (z * res)))
        for t in range(2):
            send_rows(
                meta, lambda r, n: z_ref[q, t, pl.ds(r, n), :], Z_HALO, rows, out_a, out_b, (2 * q + t) * Z_HALO
            )
    dot_ref[...] = total_of(dots)


def own_lanes(slots, q):
    return 1.0 if 2 * q + 1 < slots else (lane_iota() < HALF).astype(F32)


def pack_second(meta_ref, z_ref, za, zb, _, __, a_ref, b_ref):
    meta = Meta(meta_ref)
    pairs, _, rows, _ = z_ref.shape
    groups = [(Z_HALO, pair_rows(meta, z_ref, za, zb, q, Z_HALO, 0, 0, Z_HALO, rows)) for q in range(pairs)]
    pack_columns(meta, side_mask(meta), groups, a_ref, b_ref)


def stage_second(slots, meta_ref, table_ref, z_ref, reg_ref, valid_ref, za, zb, ga, gb, *refs):
    y_ref, out_a, out_b, image_ref, dot_zq, dot_yq = refs[:6]
    x_ref, m_ref, acc_ref, y_planes, *rest = refs[6:]
    work, masks = rest[:-3], rest[-3:]
    meta = Meta(meta_ref)
    mask = side_mask(meta)
    pairs, _, rows, _ = z_ref.shape
    x_base, m_base, acc_base = Z_HALO, V_HALO + 8, DEPTH2 + 8
    prepare_vcycle(meta, DEPTH2, rows, masks, work)
    total = rows + 2 * Z_HALO
    for q in range(pairs):
        load_fields(
            meta, mask, slots, q, pair_rows(meta, z_ref, za, zb, q, Z_HALO, 0, 0, Z_HALO, rows),
            ga, gb, q * total, Z_HALO, x_ref, x_base,
        )
    for k in range(slots):
        for plane in range(4):
            zero_rows(x_ref, (k, plane), ((total, total + 8),))
        clear_planes(acc_ref, (k,))
    for plane in range(2):
        zero_rows(m_ref, (plane,), ((0, 8), (rows + 2 * V_HALO + 8, rows + 2 * V_HALO + 16)))
    guide_loop(
        meta, table_ref, valid_ref.shape[0], slots,
        (x_ref, x_base), (valid_ref, V_HALO), (m_ref, m_base), (acc_ref, acc_base),
        (-V_HALO, rows + V_HALO), (-DEPTH2, rows + DEPTH2), slots,
    )

    def finish_slot(k):
        weight = reg_ref[pl.ds(8 * k, 1), :]
        own_masks = [m.at[k & 1] for m in masks]
        own_work = work[9 * (k & 1) :][:9]
        g_ref = own_work[0]
        bilaplace_into(
            x_ref.at[k], x_base, g_ref, -DEPTH2, rows + DEPTH2,
            lambda r, n: own_masks[0][pl.ds(r + DEPTH2 + 8, n), :],
        )
        yield
        h_ref = acc_ref.at[k]
        for r, n in spans(-DEPTH2, rows + DEPTH2, 16):
            at = r + DEPTH2 + 8
            bi = five_point(g_ref, at, n)[:2]
            inside = own_masks[0][pl.ds(at, n), :]
            for t in range(2):
                h_ref[t, pl.ds(at, n), :] = inside * (
                    h_ref[t, pl.ds(at, n), :] + weight * bi[t] + 0.1 * x_ref[k, t, pl.ds(r + x_base, n), :]
                )
        for t in range(2):
            zero_rows(g_ref, (t,), ((0, 8), (rows + 2 * DEPTH2 + 8, rows + 2 * DEPTH2 + 16)))
        yield
        yield from vcycle(h_ref, y_planes.at[k], weight, DEPTH2, rows, own_masks, own_work)

    for q in range(pairs):
        in_step(finish_slot(k) for k in range(2 * q, min(2 * q + 2, slots)))
    zq, yq = [], []
    total_y = rows + 2 * Y_HALO
    for q in range(pairs):
        one, two = 2 * q, min(2 * q + 1, slots - 1)
        for r, n in spans(-Y_HALO, rows + Y_HALO, 8):
            rows_at = pl.ds(r + DEPTH2 + 8, n)
            y = [merge(y_planes[one, t, rows_at, :], y_planes[two, t, rows_at, :]) for t in range(2)]
            at = pl.ds(q * total_y + r + Y_HALO, n)
            out_a[at, :], out_b[at, :] = send_columns(mask, *y)
            for t in range(2):
                y_ref[q, t, pl.ds(r + Y_HALO, n), :] = y[t]
                if 0 <= r < rows:
                    image = merge(acc_ref[one, t, rows_at, :], acc_ref[two, t, rows_at, :])
                    z = z_ref[q, t, pl.ds(r, n), :]
                    own = own_lanes(slots, q)
                    zq.append(own * (z * image))
                    yq.append(own * (y[t] * image))
                    if q == 0:
                        image_ref[t, pl.ds(r, n), :] = image
    dot_zq[...], dot_yq[...] = total_of(zq), total_of(yq)


def stage_third(slots, meta_ref, table_ref, y_ref, reg_ref, valid_ref, dot_rz, dot_zq, dot_yq, ga, gb, *refs):
    image_ref, sums_ref, x_ref, m_ref, acc_ref, g_ref, square_ref, mask_ref = refs
    meta = Meta(meta_ref)
    mask = side_mask(meta)
    pairs, _, total, _ = y_ref.shape
    rows = total - 2 * Y_HALO
    x_base, m_base = Y_HALO, 24
    for q in range(pairs):
        load_fields(
            meta, mask, slots, q,
            [(r, n, lambda t, r=r, n=n: y_ref[q, t, pl.ds(r, n), :]) for r, n in spans(0, total, 16)],
            ga, gb, q * total, 0, x_ref, 0,
        )
    for k in range(slots):
        for plane in range(4):
            zero_rows(x_ref, (k, plane), ((total, total + 8),))
    clear_planes(acc_ref, (0,))
    square_ref[...] = jnp.zeros((8, LANES), F32)
    for position in range(mask_ref.shape[0]):
        for r, n in spans(-8, rows + 8, 48):
            mask_ref[position, pl.ds(r + 8, n), :] = mask_rows(meta, position, r, n, rows)
    guide_loop(
        meta, table_ref, valid_ref.shape[0], slots,
        (x_ref, x_base), (valid_ref, V_HALO), (m_ref, m_base), (acc_ref, 0),
        (-24, rows + 24), (0, rows), 1, square_ref=square_ref, rows=rows,
    )
    squares = []
    for k in reversed(range(slots)):
        weight = reg_ref[pl.ds(8 * k, 1), :]
        bilaplace_into(
            x_ref.at[k], x_base, g_ref, 0, rows, lambda r, n: mask_ref[k & 1, pl.ds(r + 8, n), :]
        )
        own = (((lane_iota() - HALF * (k & 1)) & (LANES - 1)) < HALF).astype(F32)
        for r, n in spans(0, rows, 16):
            x = x_ref[k, 0, pl.ds(r + x_base, n), :], x_ref[k, 1, pl.ds(r + x_base, n), :]
            if k == 0:
                bi_even, bi_odd, g_even, g_odd = five_point(g_ref, r + 8, n)
                image_ref[0, pl.ds(r, n), :] = acc_ref[0, 0, pl.ds(r, n), :] + weight * bi_even + 0.1 * x[0]
                image_ref[1, pl.ds(r, n), :] = acc_ref[0, 1, pl.ds(r, n), :] + weight * bi_odd + 0.1 * x[1]
            else:
                g_even, g_odd = g_ref[0, pl.ds(r + 8, n), :], g_ref[1, pl.ds(r + 8, n), :]
            squares.append(
                own * fold(weight * (g_even * g_even + g_odd * g_odd) + 0.1 * (x[0] * x[0] + x[1] * x[1]))
            )
    square_ref[...] += total_of(squares)
    row = lax.broadcasted_iota(jnp.int32, (8, LANES), 0)
    packed = jnp.zeros((8, LANES), F32)
    for at, part in enumerate((dot_rz[...], dot_zq[...], dot_yq[...], square_ref[...])):
        packed = jnp.where(row == at, jnp.sum(part, axis=0, keepdims=True), packed)
    for d in range(sums_ref.shape[0]):
        sums_ref[d] = packed


def finish(start_ref, z_ref, res_ref, q_ref, y_ref, p_ref, sums_ref, solution_ref, residual_ref):
    rows = start_ref.shape[1]
    total = sums_ref[0]
    for d in range(1, sums_ref.shape[0]):
        total = total + sums_ref[d]
    total = jnp.sum(total, axis=1, keepdims=True)
    rz, zq, yq, yp = (total[k : k + 1] for k in range(4))
    alpha = rz / zq
    rz_next = alpha * alpha * yq - rz
    grown = 1.0 + rz_next / rz
    alpha_next = rz_next / (grown * grown * zq - 2.0 * alpha * grown * yq + alpha * alpha * yp)
    matrix = selection(
        (2 * LANES, LANES), lambda s, t: s == (t >> 1) + LANES * (t & 1)
    )
    c_z = alpha + alpha_next * grown
    c_y = alpha_next * alpha
    step, rest = [], []
    for t in range(2):
        step.append(c_z * z_ref[0, t] - c_y * y_ref[0, t, pl.ds(Y_HALO, rows), :])
        rest.append(res_ref[t] - (c_z * q_ref[t] - c_y * p_ref[t]))
    solution_ref[0] = start_ref[0] + exact_dot(jnp.concatenate(step, axis=1), matrix)
    residual_ref[0] = exact_dot(jnp.concatenate(rest, axis=1), matrix)


def call(kernel, outs, *args, scratch=(), scalars=0, unread=0):
    n_in, n_out = len(args), len(outs)
    spaces = [pltpu.SMEM] * scalars + [pltpu.VMEM] * (n_in - scalars - unread) + [pl.ANY] * unread
    return pl.pallas_call(
        kernel,
        out_shape=[jax.ShapeDtypeStruct(shape, F32) for shape in outs],
        in_specs=[pl.BlockSpec(memory_space=space) for space in spaces],
        out_specs=[pl.BlockSpec(memory_space=pltpu.VMEM)] * n_out,
        scratch_shapes=list(scratch),
        compiler_params=pltpu.CompilerParams(vmem_limit_bytes=VMEM_LIMIT),
    )(*args)


def swap(a, b, axis, closed):
    n = lax.axis_size(axis)
    first = [(i, i ^ 1 if i ^ 1 < n else i) for i in range(n)]
    last = lambda i: i - 1 if i % 2 == 0 else i + 1
    if closed and n % 2 == 0:
        second = [(i, last(i) % n) for i in range(n)]
    else:
        second = [(i, last(i) if 0 <= last(i) < n else i) for i in range(n)]
    return lax.ppermute(a, axis, first), lax.ppermute(b, axis, second)


def shards(rhs, start, valid, reg, shifts, frac):
    rows = rhs.shape[1]
    guides = valid.shape[0]
    slots = lax.axis_size("layer")
    gx, gy = lax.axis_index("gx"), lax.axis_index("gy")
    n_gx, n_gy = lax.axis_size("gx"), lax.axis_size("gy")
    at = jnp.arange(8, dtype=jnp.int32)
    meta = jnp.zeros((8,), jnp.int32)
    for k, value in enumerate(
        (gx > 0, gx < n_gx - 1, gy > 0, gy < n_gy - 1, lax.axis_index("layer"), gx & 1, gy & 1)
    ):
        meta = jnp.where(at == k, value.astype(jnp.int32), meta)
    table = jnp.concatenate([shifts.reshape(-1), frac.reshape(-1)])
    pairs, maps = (slots + 1) // 2, (guides + 1) // 2
    vmem = lambda *shape: pltpu.VMEM((*shape, LANES), F32)

    strip = (X_HALO + R_HALO, LANES)
    xr, xa, xb = call(order_inputs, ((2 * rows + 8, LANES), strip, strip), meta, reg, start, rhs, scalars=2)
    round_layers = lambda x: [x] + [
        lax.ppermute(x, "layer", [(i, (i + k) % slots) for i in range(slots)]) for k in range(1, slots)
    ]
    xa, xb = swap(xa, xb, "gx", True)
    xrs = round_layers(xr)
    near, far = (maps * 2 * V_NEAR, LANES), (maps * 2 * (V_HALO - V_NEAR), LANES)
    v_own, va, vb = call(
        order_valid, ((maps, 2, rows, LANES), near, near), meta, valid, xa, xb, scalars=1, unread=2
    )
    va, vb = swap(va, vb, "gx", True)
    xas, xbs = round_layers(xa), round_layers(xb)
    strip = (2 * pairs * (rows + X_HALO + R_HALO), LANES)
    v_strip = (maps * (rows + 2 * V_NEAR), LANES)
    ga, gb = call(
        functools.partial(pack_inputs, slots), (strip, strip),
        meta, *xrs, *xas, *xbs, table, v_own,
        scalars=1, unread=2,
    )
    ga, gb = swap(ga, gb, "gy", True)
    na, nb, fa, fb = call(
        pack_valid, (v_strip, v_strip, far, far), meta, v_own, va, vb, ga, gb, scalars=1, unread=2
    )
    na, nb = swap(na, nb, "gy", V_CLOSED)
    fa, fb = swap(fa, fb, "gx", True)

    tile = (pairs, 2, rows, LANES)
    size = rows + 2 * DEPTH1 + 16
    positions = min(slots, 2)
    footprints, part, weights = call(
        functools.partial(stage_inputs, slots),
        ((guides, 2, rows + 2 * V_NEAR, LANES), (slots, 2, rows + 2 * DEPTH1, LANES), (8 * slots, LANES)),
        meta, table, ga, gb, *xrs, *xas, *xbs,
        scalars=2,
        scratch=[vmem(slots, 4, rows + 2 * X_HALO + 16), vmem(slots, 2, size), vmem(positions, size)],
    )
    ha, hb = call(pack_far, (far, far), meta, fa, fb, na, weights, scalars=1, unread=2)
    packed_far = ha
    ha, hb = swap(ha, hb, "gy", True)
    strip = (pairs * 2 * Z_HALO, LANES)
    z, za, zb, res, dot_rz = call(
        functools.partial(stage_first, slots),
        (tile, strip, strip, (2, rows, LANES), (8, LANES)),
        meta, table, v_own, va, vb, na, nb, footprints, part, weights, packed_far,
        scalars=2, unread=1,
        scratch=[
            vmem(guides, 2, rows + 2 * V_NEAR + 16),
            vmem(slots, 2, size),
            vmem(slots, 2, size),
            *vcycle_scratch(DEPTH1, rows, slots),
        ],
    )
    za, zb = swap(za, zb, "gx", True)
    (spread,) = call(
        spread_all,
        ((guides, 2, rows + 2 * V_HALO, LANES),),
        meta, v_own, va, vb, na, nb, fa, fb, ha, hb,
        scalars=1,
    )
    strip = (pairs * (rows + 2 * Z_HALO), LANES)
    ka, kb = call(pack_second, (strip, strip), meta, z, za, zb, ha, hb, scalars=1, unread=2)
    ka, kb = swap(ka, kb, "gy", True)

    size = rows + 2 * DEPTH2 + 16
    strip = (pairs * (rows + 2 * Y_HALO), LANES)
    y, ya, yb, image, dot_zq, dot_yq = call(
        functools.partial(stage_second, slots),
        ((pairs, 2, rows + 2 * Y_HALO, LANES), strip, strip, (2, rows, LANES), (8, LANES), (8, LANES)),
        meta, table, z, weights, spread, za, zb, ka, kb,
        scalars=2,
        scratch=[
            vmem(slots, 4, rows + 2 * Z_HALO + 8),
            vmem(2, rows + 2 * V_HALO + 16),
            vmem(slots, 2, size),
            vmem(slots, 2, size),
            *vcycle_scratch(DEPTH2, rows, slots),
        ],
    )
    ya, yb = swap(ya, yb, "gy", True)

    image_y, sums = call(
        functools.partial(stage_third, slots),
        ((2, rows, LANES), (n_gx * n_gy, 8, LANES)),
        meta, table, y, weights, spread, dot_rz, dot_zq, dot_yq, ya, yb,
        scalars=2,
        scratch=[
            vmem(slots, 4, rows + 2 * Y_HALO + 8),
            vmem(2, rows + 48),
            vmem(1, 2, rows),
            vmem(2, rows + 16),
            vmem(8),
            vmem(min(slots, 2), rows + 16),
        ],
    )
    sums = lax.all_to_all(sums, ("gx", "gy"), 0, 0)
    return call(finish, ((1, rows, LANES), (1, rows, LANES)), start, z, res, image, y, image_y, sums)


def solution(mesh):
    in_specs = (
        P("layer", "gx", "gy"),
        P("layer", "gx", "gy"),
        P(None, "gx", "gy"),
        P("layer"),
        P(),
        P(),
    )
    out_specs = (P("layer", "gx", "gy"), P("layer", "gx", "gy"))

    def run(*args):
        return tuple(jax.shard_map(shards, mesh=mesh, in_specs=in_specs, out_specs=out_specs, check_vma=False)(*args))

    return run
```

```python
import functools

import jax
import jax.numpy as jnp
import numpy as np
from jax import lax
from jax.experimental import pallas as pl
from jax.experimental.pallas import tpu as pltpu
from jax.sharding import PartitionSpec as P

GUIDES = 8
SHIFT_MAX = 16
LANES = 128
HALF = LANES // 2
QUART = LANES // 4
F32 = jnp.float32
BF16 = jnp.bfloat16
DOT = functools.partial(jnp.dot, preferred_element_type=F32)

X_HALO, R_HALO, V_HALO, V_NEAR, Z_HALO, Y_HALO = 56, 24, 72, 40, 88, 40
DEPTH1, DEPTH2 = 24, 56
VMEM_LIMIT = 16 << 20


def lane_iota(shape=(1, LANES)):
    return lax.broadcasted_iota(jnp.int32, shape, len(shape) - 1)


def roll(x, amount):
    amount = amount % LANES if isinstance(amount, int) else amount & (LANES - 1)
    if isinstance(amount, int) and amount == 0:
        return x
    return pltpu.roll(x, amount, x.ndim - 1)


def spans(low, high, size):
    return [(r, min(size, high - r)) for r in range(low, high, size)]


class Meta:
    def __init__(self, ref):
        self.top_ok, self.bottom_ok, self.left_ok, self.right_ok = (ref[k].astype(F32) for k in range(4))
        self.layer, self.gx_odd, self.gy_odd = ref[4], ref[5], ref[6]


def exact_dot(values, matrix):
    high = values.astype(BF16)
    rest = values - high.astype(F32)
    mid = rest.astype(BF16)
    low = (rest - mid.astype(F32)).astype(BF16)
    return DOT(high, matrix) + (DOT(mid, matrix) + DOT(low, matrix))


def selection(shape, wanted_of):
    source = lax.broadcasted_iota(jnp.int32, shape, 0)
    target = lax.broadcasted_iota(jnp.int32, shape, 1)
    return wanted_of(source, target).astype(F32).astype(BF16)


def send_rows(meta, own_of, halo, rows, out_a, out_b, base):
    for r, n in spans(0, halo, 32):
        up, down = own_of(r, n), own_of(rows - halo + r, n)
        odd = meta.gx_odd == 1
        out_a[pl.ds(base + r, n), :] = jnp.where(odd, up, down)
        out_b[pl.ds(base + r, n), :] = jnp.where(odd, down, up)


def rows_with_halo(meta, own_of, a_of, b_of, skip, halo, rows, size=16):
    odd = meta.gx_odd == 1
    for r, n in spans(0, halo, size):
        yield r - halo, n, lambda t, r=r, n=n: jnp.where(odd, a_of(t, skip + r, n), b_of(t, skip + r, n)) * meta.top_ok
    for r, n in spans(0, rows, size):
        yield r, n, lambda t, r=r, n=n: own_of(t, r, n)
    for r, n in spans(0, halo, size):
        yield rows + r, n, lambda t, r=r, n=n: jnp.where(odd, b_of(t, r, n), a_of(t, r, n)) * meta.bottom_ok


def side_mask(meta):
    return ((lane_iota() >> 5) & 1) == meta.gy_odd


def send_columns(mask, even, odd):
    moved = roll(odd, -QUART)
    return jnp.where(mask, moved, even), jnp.where(mask, even, moved)


def with_columns(meta, mask, even, odd, from_a, from_b):
    lane = lane_iota()
    near = ((lane >> 5) & 1) == 0
    side_even = jnp.where(mask, from_a, from_b) * jnp.where(near, meta.right_ok, meta.left_ok)
    side_odd = jnp.where(mask, from_b, from_a) * jnp.where(near, meta.left_ok, meta.right_ok)
    side_even, side_odd = roll(side_even, HALF), roll(side_odd, -QUART)
    low = lane < HALF
    return (
        (jnp.where(low, even, side_even), jnp.where(low, odd, side_odd)),
        (jnp.where(low, side_even, even), jnp.where(low, side_odd, odd)),
    )


def merge(first, second):
    return jnp.where(lane_iota() < HALF, first, second)


def rows_of(ref, start):
    return lambda r, n: ref[pl.ds(start + r, n), :]


def five_point(ref, at, n):
    even, odd = ref[0, pl.ds(at, n), :], ref[1, pl.ds(at, n), :]
    sum_even = ref[0, pl.ds(at - 1, n), :] + ref[0, pl.ds(at + 1, n), :] + (odd + roll(odd, 1))
    sum_odd = ref[1, pl.ds(at - 1, n), :] + ref[1, pl.ds(at + 1, n), :] + (even + roll(even, -1))
    return sum_even - 4.0 * even, sum_odd - 4.0 * odd, even, odd


def five_coarse(ref, at, n, step):
    here = ref[pl.ds(at, n), :]
    sides = roll(here, step) + roll(here, -step)
    return ref[pl.ds(at - 1, n), :] + ref[pl.ds(at + 1, n), :] + sides - 4.0 * here, here


def mask_rows(meta, position, row_at, n, rows):
    row = row_at + lax.broadcasted_iota(jnp.int32, (n, LANES), 0)
    lane = (lane_iota((n, LANES)) - HALF * position) & (LANES - 1)
    by_row = jnp.where(row < 0, meta.top_ok, jnp.where(row >= rows, meta.bottom_ok, 1.0))
    return by_row * jnp.where(lane < HALF, 1.0, jnp.where(lane < 3 * QUART, meta.right_ok, meta.left_ok))


def guide_loop(meta, table_ref, guides, slots, x=None, valid=None, m=None, acc=None, p_rows=None, outs=None, out_slots=None, footprints=None, square_ref=None, rows=None):
    def coefficients(g, slot):
        layer = lax.rem(meta.layer - slot + slots, slots)
        at = (g * slots + layer) * 2
        there = guides * slots * 2
        return (
            table_ref[at],
            table_ref[at + 1],
            table_ref[there + at].astype(F32) * (1.0 / 256.0),
            table_ref[there + at + 1].astype(F32) * (1.0 / 256.0),
        )

    def between(ref, index, at, step, n, u):
        here = ref[index + (pl.ds(at, n), slice(None))]
        return here + u * (ref[index + (pl.ds(at + step, n), slice(None))] - here)

    def forward(g):
        home = HALF * (g & 1)
        x_ref, x_base = x
        fixed = []
        for slot in range(slots):
            a, b, u, v = coefficients(g, slot)
            amount = home - HALF * (slot & 1) - lax.shift_right_arithmetic(b, 1)
            fixed.append((a, u, v, b & 1, amount & (LANES - 1)))
        squares = []
        for r, n in spans(*p_rows, 16):
            even = odd = None
            for slot in range(slots):
                a, u, v, parity, amount = fixed[slot]
                c0, c1, c2 = (between(x_ref, (slot, parity + k), r + x_base + a, 1, n, u) for k in range(3))
                this_even = roll(c0 + v * (c1 - c0), amount)
                this_odd = roll(c1 + v * (c2 - c1), amount)
                even = this_even if even is None else even + this_even
                odd = this_odd if odd is None else odd + this_odd
            if footprints is not None:
                out_ref, out_base = footprints
                out_ref[g, 0, pl.ds(r + out_base, n), :] = even
                out_ref[g, 1, pl.ds(r + out_base, n), :] = odd
                continue
            (valid_ref, v_base), (m_ref, m_base) = valid, m
            m_even = even * valid_ref[g, 0, pl.ds(r + v_base, n), :]
            m_odd = odd * valid_ref[g, 1, pl.ds(r + v_base, n), :]
            m_ref[0, pl.ds(r + m_base, n), :] = m_even
            m_ref[1, pl.ds(r + m_base, n), :] = m_odd
            if square_ref is not None:
                for k in range(0, n, 8):
                    if 0 <= r + k < rows:
                        sl = slice(k, k + 8)
                        squares.append(m_even[sl] * even[sl] + m_odd[sl] * odd[sl])
        if squares:
            own = (((lane_iota() - home) & (LANES - 1)) < HALF).astype(F32)
            square_ref[...] += own * total_of(squares)

    def backward(g):
        home = HALF * (g & 1)
        (m_ref, m_base), (acc_ref, acc_base) = m, acc
        lead = () if x is not None else (g,)
        for slot in range(out_slots):
            a, b, u, v = coefficients(g, slot)
            back = -b - 1
            parity = back & 1
            amount = HALF * (slot & 1) - home - lax.shift_right_arithmetic(back, 1)
            for r, n in spans(*outs, 16):
                at = r + m_base - a
                plane_a = between(m_ref, (*lead, parity), at, -1, n, u)
                plane_b = between(m_ref, (*lead, 1 - parity), at, -1, n, u)
                q0, q1, q2 = roll(plane_a, amount), roll(plane_b, amount - parity), roll(plane_a, amount - 1)
                acc_ref[slot, 0, pl.ds(r + acc_base, n), :] += q1 + v * (q0 - q1)
                acc_ref[slot, 1, pl.ds(r + acc_base, n), :] += q2 + v * (q1 - q2)

    def body(g, carry):
        if x is not None:
            forward(g)
        if acc is not None:
            backward(g)
        return carry

    lax.fori_loop(0, guides, body, 0)


def store_field(x_ref, slot, at, n, even, odd):
    for plane, value in enumerate((even, odd, roll(even, -1), roll(odd, -1))):
        x_ref[slot, plane, pl.ds(at, n), :] = value


def zero_rows(ref, index, ranges):
    for low, high in ranges:
        if high > low:
            ref[index + (pl.ds(low, high - low), slice(None))] = jnp.zeros((high - low, LANES), F32)


def clear_planes(ref, index):
    for plane in range(2):
        for r, n in spans(0, ref.shape[-2], 64):
            ref[index + (plane, pl.ds(r, n), slice(None))] = jnp.zeros((n, LANES), F32)


def vcycle(h_ref, out_ref, weight, depth, rows, masks, work):
    g_ref, w_ref, t_ref, h1, g1, w1, t1, h2, g2 = work
    mask0, mask1, mask2 = masks
    size0 = rows + 2 * depth
    size1, size2 = size0 // 2, size0 // 4
    lane = lane_iota()
    s0 = 0.5 / (4.0 + 20.0 * weight)
    weight1, weight2 = weight * (1.0 / 16.0), weight * (1.0 / 256.0)
    s1 = 0.5 / (4.0 + 20.0 * weight1)
    s2 = 0.5 / (4.0 + 20.0 * weight2)

    for r, n in spans(8, 8 + size0, 16):
        lap_even, lap_odd, _, _ = five_point(h_ref, r, n)
        mask = mask0[pl.ds(r, n), :]
        g_ref[0, pl.ds(r, n), :] = mask * lap_even
        g_ref[1, pl.ds(r, n), :] = mask * lap_odd
    yield
    for r, n in spans(8, 8 + size0, 16):
        bi_even, bi_odd, _, _ = five_point(g_ref, r, n)
        h_both = h_ref[0, pl.ds(r, n), :] + h_ref[1, pl.ds(r, n), :]
        t_ref[pl.ds(r, n), :] = mask0[pl.ds(r, n), :] * (
            h_both - s0 * (4.0 * h_both + weight * (bi_even + bi_odd))
        )
    h1[pl.ds(8, size1), :] = 0.25 * (t_ref[pl.ds(8, size1, stride=2), :] + t_ref[pl.ds(9, size1, stride=2), :])
    yield
    for r, n in spans(8, 8 + size1, 32):
        lap, _ = five_coarse(h1, r, n, 1)
        g1[pl.ds(r, n), :] = mask1[pl.ds(r, n), :] * lap
    yield
    for r, n in spans(8, 8 + size1, 32):
        bi, _ = five_coarse(g1, r, n, 1)
        here = h1[pl.ds(r, n), :]
        t1[pl.ds(r, n), :] = mask1[pl.ds(r, n), :] * (here - s1 * (4.0 * here + weight1 * bi))
    both = t1[pl.ds(8, size2, stride=2), :] + t1[pl.ds(9, size2, stride=2), :]
    h2[pl.ds(8, size2), :] = 0.25 * (both + jnp.where((lane & 1) == 0, roll(both, -1), roll(both, 1)))
    yield
    lap, _ = five_coarse(h2, 8, size2, 2)
    g2[pl.ds(8, size2), :] = mask2[pl.ds(8, size2), :] * lap
    yield
    bi, _ = five_coarse(g2, 8, size2, 2)
    here = h2[pl.ds(8, size2), :]
    e2 = mask2[pl.ds(8, size2), :] * (s2 * (2.0 * here - s2 * (4.0 * here + weight2 * bi)))
    yield
    t1[pl.ds(8, size2, stride=2), :] = e2
    t1[pl.ds(9, size2, stride=2), :] = e2
    yield
    for r, n in spans(8, 8 + size1, 32):
        w1[pl.ds(r, n), :] = s1 * h1[pl.ds(r, n), :] + t1[pl.ds(r, n), :]
    yield
    for r, n in spans(8, 8 + size1, 32):
        lap, _ = five_coarse(w1, r, n, 1)
        g1[pl.ds(r, n), :] = mask1[pl.ds(r, n), :] * lap
    yield
    for r, n in spans(8, 8 + size1, 32):
        bi, _ = five_coarse(g1, r, n, 1)
        here = w1[pl.ds(r, n), :]
        t1[pl.ds(r, n), :] = mask1[pl.ds(r, n), :] * (
            here + s1 * (h1[pl.ds(r, n), :] - 4.0 * here - weight1 * bi)
        )
    e1 = t1[pl.ds(8, size1), :]
    yield
    t_ref[pl.ds(8, size1, stride=2), :] = e1
    t_ref[pl.ds(9, size1, stride=2), :] = e1
    yield
    for r, n in spans(8, 8 + size0, 16):
        copied = t_ref[pl.ds(r, n), :]
        for plane in range(2):
            w_ref[plane, pl.ds(r, n), :] = s0 * h_ref[plane, pl.ds(r, n), :] + copied
    yield
    for r, n in spans(8, 8 + size0, 16):
        lap_even, lap_odd, _, _ = five_point(w_ref, r, n)
        mask = mask0[pl.ds(r, n), :]
        g_ref[0, pl.ds(r, n), :] = mask * lap_even
        g_ref[1, pl.ds(r, n), :] = mask * lap_odd
    yield
    for r, n in spans(8, 8 + size0, 16):
        bi = five_point(g_ref, r, n)[:2]
        mask = mask0[pl.ds(r, n), :]
        for plane in range(2):
            here = w_ref[plane, pl.ds(r, n), :]
            out_ref[plane, pl.ds(r, n), :] = mask * (
                here + s0 * (h_ref[plane, pl.ds(r, n), :] - 4.0 * here - weight * bi[plane])
            )


def in_step(runs):
    runs = list(runs)
    while runs:
        runs = [run for run in runs if next(run, runs) is not runs]


def vcycle_scratch(depth, rows, slots):
    size0 = rows + 2 * depth
    one = lambda size: pltpu.VMEM((size + 16, LANES), F32)
    two = pltpu.VMEM((2, size0 + 16, LANES), F32)
    size1, size2 = size0 // 2, size0 // 4
    work = [two, two, one(size0), one(size1), one(size1), one(size1), one(size1), one(size2), one(size2)]
    positions = min(slots, 2)
    return work * positions + [pltpu.VMEM((positions, size + 16, LANES), F32) for size in (size0, size1, size2)]


def prepare_vcycle(meta, depth, rows, masks, work):
    size0 = rows + 2 * depth
    sizes = (size0, size0 // 2, size0 // 4)
    for level, (mask, size) in enumerate(zip(masks, sizes)):
        for position in range(mask.shape[0]):
            for r, n in spans(0, size + 16, 64):
                mask[position, pl.ds(r, n), :] = mask_rows(
                    meta, position, r - 8 - (depth >> level), n, rows >> level
                )
    for k in range(0, len(work), 9):
        g_ref, w_ref, t_ref, h1, g1, w1, t1, h2, g2 = work[k : k + 9]
        for plane in range(2):
            zero_rows(w_ref, (plane,), ((0, 8), (size0 + 8, size0 + 16)))
        for ref, size in ((h1, sizes[1]), (g1, sizes[1]), (w1, sizes[1]), (h2, sizes[2]), (g2, sizes[2])):
            zero_rows(ref, (), ((0, 8), (size + 8, size + 16)))


def bilaplace_into(x_ref, x_base, g_ref, low, high, mask_of):
    for r, n in spans(low - 8, high + 8, 16):
        lap_even, lap_odd, _, _ = five_point(x_ref, r + x_base, n)
        mask = mask_of(r, n)
        g_ref[0, pl.ds(r - low + 8, n), :] = mask * lap_even
        g_ref[1, pl.ds(r - low + 8, n), :] = mask * lap_odd


def total_of(parts):
    while len(parts) > 1:
        parts = [sum(parts[k : k + 2][1:], parts[k]) for k in range(0, len(parts), 2)]
    return parts[0]


def fold(values):
    return total_of([values[k : k + 8] for k in range(0, values.shape[0], 8)])


def order_inputs(meta_ref, reg_ref, start_ref, rhs_ref, xr_ref, a_ref, b_ref):
    meta = Meta(meta_ref)
    rows = start_ref.shape[1]
    matrix = selection(
        (LANES, LANES), lambda s, t: s == 2 * (t & (HALF - 1)) + (t >= HALF).astype(jnp.int32)
    )
    xr_ref[pl.ds(0, rows), :] = exact_dot(start_ref[0], matrix)
    xr_ref[pl.ds(rows, rows), :] = exact_dot(rhs_ref[0], matrix)
    xr_ref[pl.ds(2 * rows, 8), :] = jnp.full((8, LANES), reg_ref[0], F32)
    send_rows(meta, lambda r, n: xr_ref[pl.ds(r, n), :], X_HALO, rows, a_ref, b_ref, 0)
    send_rows(meta, lambda r, n: xr_ref[pl.ds(rows + r, n), :], R_HALO, rows, a_ref, b_ref, X_HALO)


def order_valid(meta_ref, valid_ref, _, __, own_ref, a_ref, b_ref):
    meta = Meta(meta_ref)
    guides, rows = valid_ref.shape[:2]
    matrix = selection(
        (2 * LANES, 2 * LANES),
        lambda s, t: s
        == ((t >> 6) & 1) * LANES + 2 * (t & (HALF - 1)) + (t >= LANES).astype(jnp.int32),
    )
    for q in range((guides + 1) // 2):
        pair = [valid_ref[min(2 * q + k, guides - 1)].astype(F32).astype(BF16) for k in range(2)]
        planes = DOT(jnp.concatenate(pair, axis=1), matrix)
        for t in range(2):
            own_ref[q, t] = planes[:, t * LANES : (t + 1) * LANES]
            own = lambda r, n: own_ref[q, t, pl.ds(r, n), :]
            send_rows(meta, own, V_NEAR, rows, a_ref, b_ref, (2 * q + t) * V_NEAR)


def input_rows(meta, slots, xrs, a_refs, b_refs, q, own_at, at, halo, rows):
    one, two = 2 * q, min(2 * q + 1, slots - 1)

    def of(refs, start):
        def get(t, r, n):
            first, second = refs[one][pl.ds(start + r, n), :], refs[two][pl.ds(start + r, n), :]
            return merge(first, roll(second, HALF)) if t == 0 else merge(roll(first, HALF), second)

        return get

    return rows_with_halo(meta, of(xrs, own_at), of(a_refs, at), of(b_refs, at), 0, halo, rows)


def pair_rows(meta, own_ref, a_ref, b_ref, q, stride, at, skip, halo, rows, size=16):
    return rows_with_halo(
        meta,
        lambda t, r, n: own_ref[q, t, pl.ds(r, n), :],
        lambda t, r, n: a_ref[pl.ds((2 * q + t) * stride + at + r, n), :],
        lambda t, r, n: b_ref[pl.ds((2 * q + t) * stride + at + r, n), :],
        skip, halo, rows, size,
    )


def pack_columns(meta, mask, groups, out_a, out_b):
    base = 0
    for halo, groups_rows in groups:
        low = None
        for r, n, get in groups_rows:
            low = r if low is None else low
            a, b = send_columns(mask, get(0), get(1))
            out_a[pl.ds(base + r - low, n), :] = a
            out_b[pl.ds(base + r - low, n), :] = b
            end = base + r - low + n
        base = end


def pack_inputs(slots, meta_ref, *refs):
    xrs, xa, xb = refs[:slots], refs[slots : 2 * slots], refs[2 * slots : 3 * slots]
    _, _, out_a, out_b = refs[3 * slots :]
    meta = Meta(meta_ref)
    mask = side_mask(meta)
    rows = (xrs[0].shape[0] - 8) // 2
    pairs = range((slots + 1) // 2)
    groups = [(X_HALO, input_rows(meta, slots, xrs, xa, xb, q, 0, 0, X_HALO, rows)) for q in pairs]
    groups += [(R_HALO, input_rows(meta, slots, xrs, xa, xb, q, rows, X_HALO, R_HALO, rows)) for q in pairs]
    pack_columns(meta, mask, groups, out_a, out_b)


def pack_valid(meta_ref, v_ref, va, vb, _, __, v_a, v_b, far_a, far_b):
    meta = Meta(meta_ref)
    mask = side_mask(meta)
    maps, _, rows, _ = v_ref.shape
    pack_columns(
        meta, mask,
        [(V_NEAR, pair_rows(meta, v_ref, va, vb, q, V_NEAR, 0, 0, V_NEAR, rows)) for q in range(maps)],
        v_a, v_b,
    )
    gap = V_HALO - V_NEAR
    odd = meta.gx_odd == 1
    for q in range(maps):
        for t in range(2):
            for r, n in spans(0, gap, 32):
                up = v_ref[q, t, pl.ds(V_NEAR + r, n), :]
                down = v_ref[q, t, pl.ds(rows - V_HALO + r, n), :]
                far_a[pl.ds((2 * q + t) * gap + r, n), :] = jnp.where(odd, up, down)
                far_b[pl.ds((2 * q + t) * gap + r, n), :] = jnp.where(odd, down, up)


def far_rows(meta, fa, fb, q):
    gap = V_HALO - V_NEAR
    odd = meta.gx_odd == 1
    for below in range(2):
        scale = meta.bottom_ok if below else meta.top_ok
        for r, n in spans(0, gap, 16):

            def get(t, r=r, n=n):
                rows_at = pl.ds((2 * q + t) * gap + r, n)
                first, second = (fa, fb) if below == 0 else (fb, fa)
                return jnp.where(odd, first[rows_at, :], second[rows_at, :]) * scale

            yield below * gap + r, n, get


def pack_far(meta_ref, fa, fb, _, __, out_a, out_b):
    meta = Meta(meta_ref)
    mask = side_mask(meta)
    gap = V_HALO - V_NEAR
    for q in range(out_a.shape[0] // (2 * gap)):
        for at, n, get in far_rows(meta, fa, fb, q):
            a, b = send_columns(mask, get(0), get(1))
            out_a[pl.ds(2 * gap * q + at, n), :] = a
            out_b[pl.ds(2 * gap * q + at, n), :] = b


def spread_valid(meta, mask, v_ref, va, vb, near_a, near_b, guides, halo, put):
    maps, _, rows, _ = v_ref.shape
    for q in range(maps):
        for r, n, get in pair_rows(meta, v_ref, va, vb, q, V_NEAR, 0, 0, V_NEAR, rows):
            at = pl.ds((rows + 2 * V_NEAR) * q + r + V_NEAR, n)
            fields = with_columns(meta, mask, get(0), get(1), near_a[at, :], near_b[at, :])
            for k, planes in enumerate(fields[: guides - 2 * q]):
                for t in range(2):
                    put(2 * q + k, t, r + halo, n, planes[t])


def spread_all(meta_ref, v_ref, va, vb, near_a, near_b, fa, fb, far_a, far_b, out_ref):
    meta = Meta(meta_ref)
    mask = side_mask(meta)
    guides = out_ref.shape[0]

    def put(g, t, at, n, value):
        out_ref[g, t, pl.ds(at, n), :] = value

    spread_valid(meta, mask, v_ref, va, vb, near_a, near_b, guides, V_HALO, put)
    maps, _, rows, _ = v_ref.shape
    gap = V_HALO - V_NEAR
    for q in range(maps):
        for at, n, get in far_rows(meta, fa, fb, q):
            rows_at = pl.ds(2 * gap * q + at, n)
            where = at if at < gap else at - gap + V_HALO + rows + V_NEAR
            fields = with_columns(meta, mask, get(0), get(1), far_a[rows_at, :], far_b[rows_at, :])
            for k, planes in enumerate(fields[: guides - 2 * q]):
                for t in range(2):
                    put(2 * q + k, t, where, n, planes[t])


def load_fields(meta, mask, slots, q, rows_iter, a_ref, b_ref, base, shift, x_ref, x_base):
    for r, n, get in rows_iter:
        at = base + r + shift
        fields = with_columns(meta, mask, get(0), get(1), a_ref[pl.ds(at, n), :], b_ref[pl.ds(at, n), :])
        for k, planes in enumerate(fields):
            if 2 * q + k < slots:
                store_field(x_ref, 2 * q + k, r + x_base, n, *planes)


def stage_inputs(slots, meta_ref, table_ref, ga, gb, *refs):
    xrs, xa, xb = refs[:slots], refs[slots : 2 * slots], refs[2 * slots : 3 * slots]
    foot_ref, part_ref, reg_ref, x_ref, g_all, mask_ref = refs[3 * slots :]
    meta = Meta(meta_ref)
    mask = side_mask(meta)
    rows = (xrs[0].shape[0] - 8) // 2
    pairs = (slots + 1) // 2
    x_base = X_HALO + 8
    total = rows + 2 * X_HALO
    total_r = rows + 2 * R_HALO
    for k in range(slots):
        reg_ref[pl.ds(8 * k, 8), :] = xrs[k][pl.ds(2 * rows, 8), :]
        for plane in range(4):
            zero_rows(x_ref, (k, plane), ((0, 8), (total + 8, total + 16)))
    for q in range(pairs):
        load_fields(
            meta, mask, slots, q, input_rows(meta, slots, xrs, xa, xb, q, 0, 0, X_HALO, rows),
            ga, gb, q * total, X_HALO, x_ref, x_base,
        )
    for position in range(mask_ref.shape[0]):
        for r, n in spans(0, rows + 2 * DEPTH1 + 16, 32):
            mask_ref[position, pl.ds(r, n), :] = mask_rows(meta, position, r - DEPTH1 - 8, n, rows)
    guide_loop(
        meta, table_ref, foot_ref.shape[0], slots, (x_ref, x_base),
        p_rows=(-V_NEAR, rows + V_NEAR), footprints=(foot_ref, V_NEAR),
    )
    for k in range(slots):
        bilaplace_into(
            x_ref.at[k], x_base, g_all.at[k], -DEPTH1, rows + DEPTH1,
            lambda r, n: mask_ref[k & 1, pl.ds(r + DEPTH1 + 8, n), :],
        )
    for q in range(pairs):
        base = pairs * total + q * total_r + R_HALO
        for r, n, get in input_rows(meta, slots, xrs, xa, xb, q, rows, X_HALO, R_HALO, rows):
            fields = with_columns(
                meta, mask, get(0), get(1), ga[pl.ds(base + r, n), :], gb[pl.ds(base + r, n), :]
            )
            at = r + DEPTH1 + 8
            for k, planes in enumerate(fields[: slots - 2 * q]):
                slot = 2 * q + k
                weight = reg_ref[pl.ds(8 * slot, 1), :]
                bi = five_point(g_all.at[slot], at, n)[:2]
                for t in range(2):
                    part_ref[slot, t, pl.ds(r + DEPTH1, n), :] = (
                        planes[t] - weight * bi[t] - 0.1 * x_ref[slot, t, pl.ds(r + x_base, n), :]
                    )


def stage_first(slots, meta_ref, table_ref, v_ref, va, vb, na, nb, foot_ref, part_ref, reg_ref, *refs):
    z_ref, out_a, out_b, res_ref, dot_ref = refs[:5]
    m_ref, acc_ref, z_planes, *rest = refs[5:]
    work, masks = rest[:-3], rest[-3:]
    meta = Meta(meta_ref)
    mask = side_mask(meta)
    maps, _, rows, _ = v_ref.shape
    guides = foot_ref.shape[0]
    pairs = (slots + 1) // 2
    m_base, acc_base = V_NEAR + 8, DEPTH1 + 8
    prepare_vcycle(meta, DEPTH1, rows, masks, work)
    for k in range(slots):
        clear_planes(acc_ref, (k,))
    for g in range(guides):
        for plane in range(2):
            zero_rows(m_ref, (g, plane), ((0, 8), (rows + 2 * V_NEAR + 8, rows + 2 * V_NEAR + 16)))

    def put(g, t, at, n, value):
        m_ref[g, t, pl.ds(at + 8, n), :] = value * foot_ref[g, t, pl.ds(at, n), :]

    spread_valid(meta, mask, v_ref, va, vb, na, nb, guides, V_NEAR, put)
    guide_loop(
        meta, table_ref, guides, slots, m=(m_ref, m_base), acc=(acc_ref, acc_base),
        outs=(-DEPTH1, rows + DEPTH1), out_slots=slots,
    )

    def finish_slot(k):
        weight = reg_ref[pl.ds(8 * k, 1), :]
        own_masks = [m.at[k & 1] for m in masks]
        own_work = work[9 * (k & 1) :][:9]
        h_ref = acc_ref.at[k]
        for at, n in spans(8, rows + 2 * DEPTH1 + 8, 16):
            inside = own_masks[0][pl.ds(at, n), :]
            for t in range(2):
                h_ref[t, pl.ds(at, n), :] = inside * (
                    part_ref[k, t, pl.ds(at - 8, n), :] - h_ref[t, pl.ds(at, n), :]
                )
        for t in range(2):
            zero_rows(own_work[0], (t,), ((0, 8), (rows + 2 * DEPTH1 + 8, rows + 2 * DEPTH1 + 16)))
        yield
        yield from vcycle(h_ref, z_planes.at[k], weight, DEPTH1, rows, own_masks, own_work)

    for q in range(pairs):
        in_step(finish_slot(k) for k in range(2 * q, min(2 * q + 2, slots)))
    dots = []
    for q in range(pairs):
        one, two = 2 * q, min(2 * q + 1, slots - 1)
        for r, n in spans(0, rows, 16):
            rows_at = pl.ds(r + DEPTH1 + 8, n)
            for t in range(2):
                z = merge(z_planes[one, t, rows_at, :], z_planes[two, t, rows_at, :])
                res = merge(acc_ref[one, t, rows_at, :], acc_ref[two, t, rows_at, :])
                z_ref[q, t, pl.ds(r, n), :] = z
                if q == 0:
                    res_ref[t, pl.ds(r, n), :] = res
                dots.append(fold(own_lanes(slots, q) * (z * res)))
        for t in range(2):
            send_rows(
                meta, lambda r, n: z_ref[q, t, pl.ds(r, n), :], Z_HALO, rows, out_a, out_b, (2 * q + t) * Z_HALO
            )
    dot_ref[...] = total_of(dots)


def own_lanes(slots, q):
    return 1.0 if 2 * q + 1 < slots else (lane_iota() < HALF).astype(F32)


def pack_second(meta_ref, z_ref, za, zb, _, __, a_ref, b_ref):
    meta = Meta(meta_ref)
    pairs, _, rows, _ = z_ref.shape
    groups = [(Z_HALO, pair_rows(meta, z_ref, za, zb, q, Z_HALO, 0, 0, Z_HALO, rows)) for q in range(pairs)]
    pack_columns(meta, side_mask(meta), groups, a_ref, b_ref)


def stage_second(slots, meta_ref, table_ref, z_ref, reg_ref, valid_ref, za, zb, ga, gb, *refs):
    y_ref, out_a, out_b, image_ref, dot_zq, dot_yq = refs[:6]
    x_ref, m_ref, acc_ref, y_planes, *rest = refs[6:]
    work, masks = rest[:-3], rest[-3:]
    meta = Meta(meta_ref)
    mask = side_mask(meta)
    pairs, _, rows, _ = z_ref.shape
    x_base, m_base, acc_base = Z_HALO, V_HALO + 8, DEPTH2 + 8
    prepare_vcycle(meta, DEPTH2, rows, masks, work)
    total = rows + 2 * Z_HALO
    for q in range(pairs):
        load_fields(
            meta, mask, slots, q, pair_rows(meta, z_ref, za, zb, q, Z_HALO, 0, 0, Z_HALO, rows),
            ga, gb, q * total, Z_HALO, x_ref, x_base,
        )
    for k in range(slots):
        for plane in range(4):
            zero_rows(x_ref, (k, plane), ((total, total + 8),))
        clear_planes(acc_ref, (k,))
    for plane in range(2):
        zero_rows(m_ref, (plane,), ((0, 8), (rows + 2 * V_HALO + 8, rows + 2 * V_HALO + 16)))
    guide_loop(
        meta, table_ref, valid_ref.shape[0], slots,
        (x_ref, x_base), (valid_ref, V_HALO), (m_ref, m_base), (acc_ref, acc_base),
        (-V_HALO, rows + V_HALO), (-DEPTH2, rows + DEPTH2), slots,
    )

    def finish_slot(k):
        weight = reg_ref[pl.ds(8 * k, 1), :]
        own_masks = [m.at[k & 1] for m in masks]
        own_work = work[9 * (k & 1) :][:9]
        g_ref = own_work[0]
        bilaplace_into(
            x_ref.at[k], x_base, g_ref, -DEPTH2, rows + DEPTH2,
            lambda r, n: own_masks[0][pl.ds(r + DEPTH2 + 8, n), :],
        )
        yield
        h_ref = acc_ref.at[k]
        for r, n in spans(-DEPTH2, rows + DEPTH2, 16):
            at = r + DEPTH2 + 8
            bi = five_point(g_ref, at, n)[:2]
            inside = own_masks[0][pl.ds(at, n), :]
            for t in range(2):
                h_ref[t, pl.ds(at, n), :] = inside * (
                    h_ref[t, pl.ds(at, n), :] + weight * bi[t] + 0.1 * x_ref[k, t, pl.ds(r + x_base, n), :]
                )
        for t in range(2):
            zero_rows(g_ref, (t,), ((0, 8), (rows + 2 * DEPTH2 + 8, rows + 2 * DEPTH2 + 16)))
        yield
        yield from vcycle(h_ref, y_planes.at[k], weight, DEPTH2, rows, own_masks, own_work)

    for q in range(pairs):
        in_step(finish_slot(k) for k in range(2 * q, min(2 * q + 2, slots)))
    zq, yq = [], []
    total_y = rows + 2 * Y_HALO
    for q in range(pairs):
        one, two = 2 * q, min(2 * q + 1, slots - 1)
        for r, n in spans(-Y_HALO, rows + Y_HALO, 8):
            rows_at = pl.ds(r + DEPTH2 + 8, n)
            y = [merge(y_planes[one, t, rows_at, :], y_planes[two, t, rows_at, :]) for t in range(2)]
            at = pl.ds(q * total_y + r + Y_HALO, n)
            out_a[at, :], out_b[at, :] = send_columns(mask, *y)
            for t in range(2):
                y_ref[q, t, pl.ds(r + Y_HALO, n), :] = y[t]
                if 0 <= r < rows:
                    image = merge(acc_ref[one, t, rows_at, :], acc_ref[two, t, rows_at, :])
                    z = z_ref[q, t, pl.ds(r, n), :]
                    own = own_lanes(slots, q)
                    zq.append(own * (z * image))
                    yq.append(own * (y[t] * image))
                    if q == 0:
                        image_ref[t, pl.ds(r, n), :] = image
    dot_zq[...], dot_yq[...] = total_of(zq), total_of(yq)


def stage_third(slots, meta_ref, table_ref, y_ref, reg_ref, valid_ref, dot_rz, dot_zq, dot_yq, ga, gb, *refs):
    image_ref, sums_ref, x_ref, m_ref, acc_ref, g_ref, square_ref, mask_ref = refs
    meta = Meta(meta_ref)
    mask = side_mask(meta)
    pairs, _, total, _ = y_ref.shape
    rows = total - 2 * Y_HALO
    x_base, m_base = Y_HALO, 24
    for q in range(pairs):
        load_fields(
            meta, mask, slots, q,
            [(r, n, lambda t, r=r, n=n: y_ref[q, t, pl.ds(r, n), :]) for r, n in spans(0, total, 16)],
            ga, gb, q * total, 0, x_ref, 0,
        )
    for k in range(slots):
        for plane in range(4):
            zero_rows(x_ref, (k, plane), ((total, total + 8),))
    clear_planes(acc_ref, (0,))
    square_ref[...] = jnp.zeros((8, LANES), F32)
    for position in range(mask_ref.shape[0]):
        for r, n in spans(-8, rows + 8, 48):
            mask_ref[position, pl.ds(r + 8, n), :] = mask_rows(meta, position, r, n, rows)
    guide_loop(
        meta, table_ref, valid_ref.shape[0], slots,
        (x_ref, x_base), (valid_ref, V_HALO), (m_ref, m_base), (acc_ref, 0),
        (-24, rows + 24), (0, rows), 1, square_ref=square_ref, rows=rows,
    )
    squares = []
    for k in reversed(range(slots)):
        weight = reg_ref[pl.ds(8 * k, 1), :]
        bilaplace_into(
            x_ref.at[k], x_base, g_ref, 0, rows, lambda r, n: mask_ref[k & 1, pl.ds(r + 8, n), :]
        )
        own = (((lane_iota() - HALF * (k & 1)) & (LANES - 1)) < HALF).astype(F32)
        for r, n in spans(0, rows, 16):
            x = x_ref[k, 0, pl.ds(r + x_base, n), :], x_ref[k, 1, pl.ds(r + x_base, n), :]
            if k == 0:
                bi_even, bi_odd, g_even, g_odd = five_point(g_ref, r + 8, n)
                image_ref[0, pl.ds(r, n), :] = acc_ref[0, 0, pl.ds(r, n), :] + weight * bi_even + 0.1 * x[0]
                image_ref[1, pl.ds(r, n), :] = acc_ref[0, 1, pl.ds(r, n), :] + weight * bi_odd + 0.1 * x[1]
            else:
                g_even, g_odd = g_ref[0, pl.ds(r + 8, n), :], g_ref[1, pl.ds(r + 8, n), :]
            squares.append(
                own * fold(weight * (g_even * g_even + g_odd * g_odd) + 0.1 * (x[0] * x[0] + x[1] * x[1]))
            )
    square_ref[...] += total_of(squares)
    row = lax.broadcasted_iota(jnp.int32, (8, LANES), 0)
    packed = jnp.zeros((8, LANES), F32)
    for at, part in enumerate((dot_rz[...], dot_zq[...], dot_yq[...], square_ref[...])):
        packed = jnp.where(row == at, jnp.sum(part, axis=0, keepdims=True), packed)
    for d in range(sums_ref.shape[0]):
        sums_ref[d] = packed


def finish(start_ref, z_ref, res_ref, q_ref, y_ref, p_ref, sums_ref, solution_ref, residual_ref):
    rows = start_ref.shape[1]
    total = sums_ref[0]
    for d in range(1, sums_ref.shape[0]):
        total = total + sums_ref[d]
    total = jnp.sum(total, axis=1, keepdims=True)
    rz, zq, yq, yp = (total[k : k + 1] for k in range(4))
    alpha = rz / zq
    rz_next = alpha * alpha * yq - rz
    grown = 1.0 + rz_next / rz
    alpha_next = rz_next / (grown * grown * zq - 2.0 * alpha * grown * yq + alpha * alpha * yp)
    matrix = selection(
        (2 * LANES, LANES), lambda s, t: s == (t >> 1) + LANES * (t & 1)
    )
    c_z = alpha + alpha_next * grown
    c_y = alpha_next * alpha
    step, rest = [], []
    for t in range(2):
        step.append(c_z * z_ref[0, t] - c_y * y_ref[0, t, pl.ds(Y_HALO, rows), :])
        rest.append(res_ref[t] - (c_z * q_ref[t] - c_y * p_ref[t]))
    solution_ref[0] = start_ref[0] + exact_dot(jnp.concatenate(step, axis=1), matrix)
    residual_ref[0] = exact_dot(jnp.concatenate(rest, axis=1), matrix)


def call(kernel, outs, *args, scratch=(), scalars=0, unread=0):
    n_in, n_out = len(args), len(outs)
    spaces = [pltpu.SMEM] * scalars + [pltpu.VMEM] * (n_in - scalars - unread) + [pl.ANY] * unread
    return pl.pallas_call(
        kernel,
        out_shape=[jax.ShapeDtypeStruct(shape, F32) for shape in outs],
        in_specs=[pl.BlockSpec(memory_space=space) for space in spaces],
        out_specs=[pl.BlockSpec(memory_space=pltpu.VMEM)] * n_out,
        scratch_shapes=list(scratch),
        compiler_params=pltpu.CompilerParams(vmem_limit_bytes=VMEM_LIMIT),
    )(*args)


def swap(a, b, axis):
    axes = ("layer", "gx", "gy")
    sizes = [lax.axis_size(name) for name in axes]
    moved = axes.index(axis)
    n = sizes[moved]

    def pairs(partner):
        found = []
        for source in np.ndindex(*sizes):
            target = list(source)
            other = partner(source[moved])
            if 0 <= other < n:
                target[moved] = other
            elif source[0] ^ 1 < sizes[0]:
                target[0] ^= 1
            found.append(tuple(int(np.ravel_multi_index(place, sizes)) for place in (source, tuple(target))))
        return found

    return (
        lax.ppermute(a, axes, pairs(lambda i: i ^ 1)),
        lax.ppermute(b, axes, pairs(lambda i: i - 1 if i % 2 == 0 else i + 1)),
    )


def shards(rhs, start, valid, reg, shifts, frac):
    rows = rhs.shape[1]
    guides = valid.shape[0]
    slots = lax.axis_size("layer")
    gx, gy = lax.axis_index("gx"), lax.axis_index("gy")
    n_gx, n_gy = lax.axis_size("gx"), lax.axis_size("gy")
    at = jnp.arange(8, dtype=jnp.int32)
    meta = jnp.zeros((8,), jnp.int32)
    for k, value in enumerate(
        (gx > 0, gx < n_gx - 1, gy > 0, gy < n_gy - 1, lax.axis_index("layer"), gx & 1, gy & 1)
    ):
        meta = jnp.where(at == k, value.astype(jnp.int32), meta)
    table = jnp.concatenate([shifts.reshape(-1), frac.reshape(-1)])
    pairs, maps = (slots + 1) // 2, (guides + 1) // 2
    vmem = lambda *shape: pltpu.VMEM((*shape, LANES), F32)

    strip = (X_HALO + R_HALO, LANES)
    xr, xa, xb = call(order_inputs, ((2 * rows + 8, LANES), strip, strip), meta, reg, start, rhs, scalars=2)
    round_layers = lambda x: [x] + [
        lax.ppermute(x, "layer", [(i, (i + k) % slots) for i in range(slots)]) for k in range(1, slots)
    ]
    xa, xb = swap(xa, xb, "gx")
    xrs = round_layers(xr)
    near, far = (maps * 2 * V_NEAR, LANES), (maps * 2 * (V_HALO - V_NEAR), LANES)
    v_own, va, vb = call(
        order_valid, ((maps, 2, rows, LANES), near, near), meta, valid, xa, xb, scalars=1, unread=2
    )
    va, vb = swap(va, vb, "gx")
    xas, xbs = round_layers(xa), round_layers(xb)
    strip = (2 * pairs * (rows + X_HALO + R_HALO), LANES)
    v_strip = (maps * (rows + 2 * V_NEAR), LANES)
    ga, gb = call(
        functools.partial(pack_inputs, slots), (strip, strip),
        meta, *xrs, *xas, *xbs, table, v_own,
        scalars=1, unread=2,
    )
    ga, gb = swap(ga, gb, "gy")
    na, nb, fa, fb = call(
        pack_valid, (v_strip, v_strip, far, far), meta, v_own, va, vb, ga, gb, scalars=1, unread=2
    )
    na, nb = swap(na, nb, "gy")
    fa, fb = swap(fa, fb, "gx")

    tile = (pairs, 2, rows, LANES)
    size = rows + 2 * DEPTH1 + 16
    positions = min(slots, 2)
    footprints, part, weights = call(
        functools.partial(stage_inputs, slots),
        ((guides, 2, rows + 2 * V_NEAR, LANES), (slots, 2, rows + 2 * DEPTH1, LANES), (8 * slots, LANES)),
        meta, table, ga, gb, *xrs, *xas, *xbs,
        scalars=2,
        scratch=[vmem(slots, 4, rows + 2 * X_HALO + 16), vmem(slots, 2, size), vmem(positions, size)],
    )
    strip = (pairs * 2 * Z_HALO, LANES)
    z, za, zb, res, dot_rz = call(
        functools.partial(stage_first, slots),
        (tile, strip, strip, (2, rows, LANES), (8, LANES)),
        meta, table, v_own, va, vb, na, nb, footprints, part, weights,
        scalars=2,
        scratch=[
            vmem(guides, 2, rows + 2 * V_NEAR + 16),
            vmem(slots, 2, size),
            vmem(slots, 2, size),
            *vcycle_scratch(DEPTH1, rows, slots),
        ],
    )
    ha, hb = call(pack_far, (far, far), meta, fa, fb, z, weights, scalars=1, unread=2)
    za, zb = swap(za, zb, "gx")
    ha, hb = swap(ha, hb, "gy")
    (spread,) = call(
        spread_all,
        ((guides, 2, rows + 2 * V_HALO, LANES),),
        meta, v_own, va, vb, na, nb, fa, fb, ha, hb,
        scalars=1,
    )
    strip = (pairs * (rows + 2 * Z_HALO), LANES)
    ka, kb = call(pack_second, (strip, strip), meta, z, za, zb, ha, hb, scalars=1, unread=2)
    ka, kb = swap(ka, kb, "gy")

    size = rows + 2 * DEPTH2 + 16
    strip = (pairs * (rows + 2 * Y_HALO), LANES)
    y, ya, yb, image, dot_zq, dot_yq = call(
        functools.partial(stage_second, slots),
        ((pairs, 2, rows + 2 * Y_HALO, LANES), strip, strip, (2, rows, LANES), (8, LANES), (8, LANES)),
        meta, table, z, weights, spread, za, zb, ka, kb,
        scalars=2,
        scratch=[
            vmem(slots, 4, rows + 2 * Z_HALO + 8),
            vmem(2, rows + 2 * V_HALO + 16),
            vmem(slots, 2, size),
            vmem(slots, 2, size),
            *vcycle_scratch(DEPTH2, rows, slots),
        ],
    )
    ya, yb = swap(ya, yb, "gy")

    image_y, sums = call(
        functools.partial(stage_third, slots),
        ((2, rows, LANES), (n_gx * n_gy, 8, LANES)),
        meta, table, y, weights, spread, dot_rz, dot_zq, dot_yq, ya, yb,
        scalars=2,
        scratch=[
            vmem(slots, 4, rows + 2 * Y_HALO + 8),
            vmem(2, rows + 48),
            vmem(1, 2, rows),
            vmem(2, rows + 16),
            vmem(8),
            vmem(min(slots, 2), rows + 16),
        ],
    )
    sums = lax.all_to_all(sums, ("gx", "gy"), 0, 0)
    return call(finish, ((1, rows, LANES), (1, rows, LANES)), start, z, res, image, y, image_y, sums)


def solution(mesh):
    in_specs = (
        P("layer", "gx", "gy"),
        P("layer", "gx", "gy"),
        P(None, "gx", "gy"),
        P("layer"),
        P(),
        P(),
    )
    out_specs = (P("layer", "gx", "gy"), P("layer", "gx", "gy"))

    def run(*args):
        return tuple(jax.shard_map(shards, mesh=mesh, in_specs=in_specs, out_specs=out_specs, check_vma=False)(*args))

    return run
```

```python
import functools

import jax
import jax.numpy as jnp
import numpy as np
from jax import lax
from jax.experimental import pallas as pl
from jax.experimental.pallas import tpu as pltpu
from jax.sharding import PartitionSpec as P

GUIDES = 8
SHIFT_MAX = 16
LANES = 128
HALF = LANES // 2
QUART = LANES // 4
F32 = jnp.float32
BF16 = jnp.bfloat16
DOT = functools.partial(jnp.dot, preferred_element_type=F32)

X_HALO, R_HALO, V_HALO, V_NEAR, Z_HALO, Y_HALO = 56, 24, 72, 40, 88, 40
DEPTH1, DEPTH2 = 24, 56
VMEM_LIMIT = 16 << 20


def lane_iota(shape=(1, LANES)):
    return lax.broadcasted_iota(jnp.int32, shape, len(shape) - 1)


def roll(x, amount):
    amount = amount % LANES if isinstance(amount, int) else amount & (LANES - 1)
    if isinstance(amount, int) and amount == 0:
        return x
    return pltpu.roll(x, amount, x.ndim - 1)


def spans(low, high, size):
    return [(r, min(size, high - r)) for r in range(low, high, size)]


class Meta:
    def __init__(self, ref):
        self.top_ok, self.bottom_ok, self.left_ok, self.right_ok = (ref[k].astype(F32) for k in range(4))
        self.layer, self.gx_odd, self.gy_odd = ref[4], ref[5], ref[6]


def exact_dot(values, matrix):
    high = values.astype(BF16)
    rest = values - high.astype(F32)
    mid = rest.astype(BF16)
    low = (rest - mid.astype(F32)).astype(BF16)
    return DOT(high, matrix) + (DOT(mid, matrix) + DOT(low, matrix))


def selection(shape, wanted_of):
    source = lax.broadcasted_iota(jnp.int32, shape, 0)
    target = lax.broadcasted_iota(jnp.int32, shape, 1)
    return wanted_of(source, target).astype(F32).astype(BF16)


def send_rows(meta, own_of, halo, rows, out_a, out_b, base):
    for r, n in spans(0, halo, 32):
        up, down = own_of(r, n), own_of(rows - halo + r, n)
        odd = meta.gx_odd == 1
        out_a[pl.ds(base + r, n), :] = jnp.where(odd, up, down)
        out_b[pl.ds(base + r, n), :] = jnp.where(odd, down, up)


def rows_with_halo(meta, own_of, a_of, b_of, skip, halo, rows, size=16):
    odd = meta.gx_odd == 1
    for r, n in spans(0, halo, size):
        yield r - halo, n, lambda t, r=r, n=n: jnp.where(odd, a_of(t, skip + r, n), b_of(t, skip + r, n)) * meta.top_ok
    for r, n in spans(0, rows, size):
        yield r, n, lambda t, r=r, n=n: own_of(t, r, n)
    for r, n in spans(0, halo, size):
        yield rows + r, n, lambda t, r=r, n=n: jnp.where(odd, b_of(t, r, n), a_of(t, r, n)) * meta.bottom_ok


def side_mask(meta):
    return ((lane_iota() >> 5) & 1) == meta.gy_odd


def send_columns(mask, even, odd):
    moved = roll(odd, -QUART)
    return jnp.where(mask, moved, even), jnp.where(mask, even, moved)


def with_columns(meta, mask, even, odd, from_a, from_b):
    lane = lane_iota()
    near = ((lane >> 5) & 1) == 0
    side_even = jnp.where(mask, from_a, from_b) * jnp.where(near, meta.right_ok, meta.left_ok)
    side_odd = jnp.where(mask, from_b, from_a) * jnp.where(near, meta.left_ok, meta.right_ok)
    side_even, side_odd = roll(side_even, HALF), roll(side_odd, -QUART)
    low = lane < HALF
    return (
        (jnp.where(low, even, side_even), jnp.where(low, odd, side_odd)),
        (jnp.where(low, side_even, even), jnp.where(low, side_odd, odd)),
    )


def merge(first, second):
    return jnp.where(lane_iota() < HALF, first, second)


def rows_of(ref, start):
    return lambda r, n: ref[pl.ds(start + r, n), :]


def five_point(ref, at, n):
    even, odd = ref[0, pl.ds(at, n), :], ref[1, pl.ds(at, n), :]
    sum_even = ref[0, pl.ds(at - 1, n), :] + ref[0, pl.ds(at + 1, n), :] + (odd + roll(odd, 1))
    sum_odd = ref[1, pl.ds(at - 1, n), :] + ref[1, pl.ds(at + 1, n), :] + (even + roll(even, -1))
    return sum_even - 4.0 * even, sum_odd - 4.0 * odd, even, odd


def five_coarse(ref, at, n, step):
    here = ref[pl.ds(at, n), :]
    sides = roll(here, step) + roll(here, -step)
    return ref[pl.ds(at - 1, n), :] + ref[pl.ds(at + 1, n), :] + sides - 4.0 * here, here


def mask_rows(meta, position, row_at, n, rows):
    row = row_at + lax.broadcasted_iota(jnp.int32, (n, LANES), 0)
    lane = (lane_iota((n, LANES)) - HALF * position) & (LANES - 1)
    by_row = jnp.where(row < 0, meta.top_ok, jnp.where(row >= rows, meta.bottom_ok, 1.0))
    return by_row * jnp.where(lane < HALF, 1.0, jnp.where(lane < 3 * QUART, meta.right_ok, meta.left_ok))


def guide_loop(meta, table_ref, guides, slots, x=None, valid=None, m=None, acc=None, p_rows=None, outs=None, out_slots=None, footprints=None, square_ref=None, rows=None):
    def coefficients(g, slot):
        layer = lax.rem(meta.layer - slot + slots, slots)
        at = (g * slots + layer) * 2
        there = guides * slots * 2
        return (
            table_ref[at],
            table_ref[at + 1],
            table_ref[there + at].astype(F32) * (1.0 / 256.0),
            table_ref[there + at + 1].astype(F32) * (1.0 / 256.0),
        )

    def between(ref, index, at, step, n, u):
        here = ref[index + (pl.ds(at, n), slice(None))]
        return here + u * (ref[index + (pl.ds(at + step, n), slice(None))] - here)

    def forward(g):
        home = HALF * (g & 1)
        x_ref, x_base = x
        fixed = []
        for slot in range(slots):
            a, b, u, v = coefficients(g, slot)
            amount = home - HALF * (slot & 1) - lax.shift_right_arithmetic(b, 1)
            fixed.append((a, u, v, b & 1, amount & (LANES - 1)))
        squares = []
        for r, n in spans(*p_rows, 16):
            even = odd = None
            for slot in range(slots):
                a, u, v, parity, amount = fixed[slot]
                c0, c1, c2 = (between(x_ref, (slot, parity + k), r + x_base + a, 1, n, u) for k in range(3))
                this_even = roll(c0 + v * (c1 - c0), amount)
                this_odd = roll(c1 + v * (c2 - c1), amount)
                even = this_even if even is None else even + this_even
                odd = this_odd if odd is None else odd + this_odd
            if footprints is not None:
                out_ref, out_base = footprints
                out_ref[g, 0, pl.ds(r + out_base, n), :] = even
                out_ref[g, 1, pl.ds(r + out_base, n), :] = odd
                continue
            (valid_ref, v_base), (m_ref, m_base) = valid, m
            m_even = even * valid_ref[g, 0, pl.ds(r + v_base, n), :]
            m_odd = odd * valid_ref[g, 1, pl.ds(r + v_base, n), :]
            m_ref[0, pl.ds(r + m_base, n), :] = m_even
            m_ref[1, pl.ds(r + m_base, n), :] = m_odd
            if square_ref is not None:
                for k in range(0, n, 8):
                    if 0 <= r + k < rows:
                        sl = slice(k, k + 8)
                        squares.append(m_even[sl] * even[sl] + m_odd[sl] * odd[sl])
        if squares:
            own = (((lane_iota() - home) & (LANES - 1)) < HALF).astype(F32)
            square_ref[...] += own * total_of(squares)

    def backward(g):
        home = HALF * (g & 1)
        (m_ref, m_base), (acc_ref, acc_base) = m, acc
        lead = () if x is not None else (g,)
        for slot in range(out_slots):
            a, b, u, v = coefficients(g, slot)
            back = -b - 1
            parity = back & 1
            amount = HALF * (slot & 1) - home - lax.shift_right_arithmetic(back, 1)
            for r, n in spans(*outs, 16):
                at = r + m_base - a
                plane_a = between(m_ref, (*lead, parity), at, -1, n, u)
                plane_b = between(m_ref, (*lead, 1 - parity), at, -1, n, u)
                q0, q1, q2 = roll(plane_a, amount), roll(plane_b, amount - parity), roll(plane_a, amount - 1)
                acc_ref[slot, 0, pl.ds(r + acc_base, n), :] += q1 + v * (q0 - q1)
                acc_ref[slot, 1, pl.ds(r + acc_base, n), :] += q2 + v * (q1 - q2)

    def body(g, carry):
        if x is not None:
            forward(g)
        if acc is not None:
            backward(g)
        return carry

    lax.fori_loop(0, guides, body, 0, unroll=4 if x is None or acc is None else 2)


def store_field(x_ref, slot, at, n, even, odd):
    for plane, value in enumerate((even, odd, roll(even, -1), roll(odd, -1))):
        x_ref[slot, plane, pl.ds(at, n), :] = value


def zero_rows(ref, index, ranges):
    for low, high in ranges:
        if high > low:
            ref[index + (pl.ds(low, high - low), slice(None))] = jnp.zeros((high - low, LANES), F32)


def clear_planes(ref, index):
    for plane in range(2):
        for r, n in spans(0, ref.shape[-2], 64):
            ref[index + (plane, pl.ds(r, n), slice(None))] = jnp.zeros((n, LANES), F32)


def vcycle(h_ref, out_ref, weight, depth, rows, masks, work):
    g_ref, w_ref, t_ref, h1, g1, w1, t1, h2, g2 = work
    mask0, mask1, mask2 = masks
    size0 = rows + 2 * depth
    size1, size2 = size0 // 2, size0 // 4
    lane = lane_iota()
    s0 = 0.5 / (4.0 + 20.0 * weight)
    weight1, weight2 = weight * (1.0 / 16.0), weight * (1.0 / 256.0)
    s1 = 0.5 / (4.0 + 20.0 * weight1)
    s2 = 0.5 / (4.0 + 20.0 * weight2)

    for r, n in spans(8, 8 + size0, 16):
        lap_even, lap_odd, _, _ = five_point(h_ref, r, n)
        mask = mask0[pl.ds(r, n), :]
        g_ref[0, pl.ds(r, n), :] = mask * lap_even
        g_ref[1, pl.ds(r, n), :] = mask * lap_odd
    yield
    for r, n in spans(8, 8 + size0, 16):
        bi_even, bi_odd, _, _ = five_point(g_ref, r, n)
        h_both = h_ref[0, pl.ds(r, n), :] + h_ref[1, pl.ds(r, n), :]
        t_ref[pl.ds(r, n), :] = mask0[pl.ds(r, n), :] * (
            h_both - s0 * (4.0 * h_both + weight * (bi_even + bi_odd))
        )
    h1[pl.ds(8, size1), :] = 0.25 * (t_ref[pl.ds(8, size1, stride=2), :] + t_ref[pl.ds(9, size1, stride=2), :])
    yield
    for r, n in spans(8, 8 + size1, 32):
        lap, _ = five_coarse(h1, r, n, 1)
        g1[pl.ds(r, n), :] = mask1[pl.ds(r, n), :] * lap
    yield
    for r, n in spans(8, 8 + size1, 32):
        bi, _ = five_coarse(g1, r, n, 1)
        here = h1[pl.ds(r, n), :]
        t1[pl.ds(r, n), :] = mask1[pl.ds(r, n), :] * (here - s1 * (4.0 * here + weight1 * bi))
    both = t1[pl.ds(8, size2, stride=2), :] + t1[pl.ds(9, size2, stride=2), :]
    h2[pl.ds(8, size2), :] = 0.25 * (both + jnp.where((lane & 1) == 0, roll(both, -1), roll(both, 1)))
    yield
    lap, _ = five_coarse(h2, 8, size2, 2)
    g2[pl.ds(8, size2), :] = mask2[pl.ds(8, size2), :] * lap
    yield
    bi, _ = five_coarse(g2, 8, size2, 2)
    here = h2[pl.ds(8, size2), :]
    e2 = mask2[pl.ds(8, size2), :] * (s2 * (2.0 * here - s2 * (4.0 * here + weight2 * bi)))
    yield
    t1[pl.ds(8, size2, stride=2), :] = e2
    t1[pl.ds(9, size2, stride=2), :] = e2
    yield
    for r, n in spans(8, 8 + size1, 32):
        w1[pl.ds(r, n), :] = s1 * h1[pl.ds(r, n), :] + t1[pl.ds(r, n), :]
    yield
    for r, n in spans(8, 8 + size1, 32):
        lap, _ = five_coarse(w1, r, n, 1)
        g1[pl.ds(r, n), :] = mask1[pl.ds(r, n), :] * lap
    yield
    for r, n in spans(8, 8 + size1, 32):
        bi, _ = five_coarse(g1, r, n, 1)
        here = w1[pl.ds(r, n), :]
        t1[pl.ds(r, n), :] = mask1[pl.ds(r, n), :] * (
            here + s1 * (h1[pl.ds(r, n), :] - 4.0 * here - weight1 * bi)
        )
    e1 = t1[pl.ds(8, size1), :]
    yield
    t_ref[pl.ds(8, size1, stride=2), :] = e1
    t_ref[pl.ds(9, size1, stride=2), :] = e1
    yield
    for r, n in spans(8, 8 + size0, 16):
        copied = t_ref[pl.ds(r, n), :]
        for plane in range(2):
            w_ref[plane, pl.ds(r, n), :] = s0 * h_ref[plane, pl.ds(r, n), :] + copied
    yield
    for r, n in spans(8, 8 + size0, 16):
        lap_even, lap_odd, _, _ = five_point(w_ref, r, n)
        mask = mask0[pl.ds(r, n), :]
        g_ref[0, pl.ds(r, n), :] = mask * lap_even
        g_ref[1, pl.ds(r, n), :] = mask * lap_odd
    yield
    for r, n in spans(8, 8 + size0, 16):
        bi = five_point(g_ref, r, n)[:2]
        mask = mask0[pl.ds(r, n), :]
        for plane in range(2):
            here = w_ref[plane, pl.ds(r, n), :]
            out_ref[plane, pl.ds(r, n), :] = mask * (
                here + s0 * (h_ref[plane, pl.ds(r, n), :] - 4.0 * here - weight * bi[plane])
            )


def in_step(runs):
    runs = list(runs)
    while runs:
        runs = [run for run in runs if next(run, runs) is not runs]


def vcycle_scratch(depth, rows, slots):
    size0 = rows + 2 * depth
    one = lambda size: pltpu.VMEM((size + 16, LANES), F32)
    two = pltpu.VMEM((2, size0 + 16, LANES), F32)
    size1, size2 = size0 // 2, size0 // 4
    work = [two, two, one(size0), one(size1), one(size1), one(size1), one(size1), one(size2), one(size2)]
    positions = min(slots, 2)
    return work * positions + [pltpu.VMEM((positions, size + 16, LANES), F32) for size in (size0, size1, size2)]


def prepare_vcycle(meta, depth, rows, masks, work):
    size0 = rows + 2 * depth
    sizes = (size0, size0 // 2, size0 // 4)
    for level, (mask, size) in enumerate(zip(masks, sizes)):
        for position in range(mask.shape[0]):
            for r, n in spans(0, size + 16, 64):
                mask[position, pl.ds(r, n), :] = mask_rows(
                    meta, position, r - 8 - (depth >> level), n, rows >> level
                )
    for k in range(0, len(work), 9):
        g_ref, w_ref, t_ref, h1, g1, w1, t1, h2, g2 = work[k : k + 9]
        for plane in range(2):
            zero_rows(w_ref, (plane,), ((0, 8), (size0 + 8, size0 + 16)))
        for ref, size in ((h1, sizes[1]), (g1, sizes[1]), (w1, sizes[1]), (h2, sizes[2]), (g2, sizes[2])):
            zero_rows(ref, (), ((0, 8), (size + 8, size + 16)))


def bilaplace_into(x_ref, x_base, g_ref, low, high, mask_of):
    for r, n in spans(low - 8, high + 8, 16):
        lap_even, lap_odd, _, _ = five_point(x_ref, r + x_base, n)
        mask = mask_of(r, n)
        g_ref[0, pl.ds(r - low + 8, n), :] = mask * lap_even
        g_ref[1, pl.ds(r - low + 8, n), :] = mask * lap_odd


def total_of(parts):
    while len(parts) > 1:
        parts = [sum(parts[k : k + 2][1:], parts[k]) for k in range(0, len(parts), 2)]
    return parts[0]


def fold(values):
    return total_of([values[k : k + 8] for k in range(0, values.shape[0], 8)])


def order_inputs(meta_ref, reg_ref, start_ref, rhs_ref, xr_ref, a_ref, b_ref):
    meta = Meta(meta_ref)
    rows = start_ref.shape[1]
    matrix = selection(
        (LANES, LANES), lambda s, t: s == 2 * (t & (HALF - 1)) + (t >= HALF).astype(jnp.int32)
    )
    xr_ref[pl.ds(0, rows), :] = exact_dot(start_ref[0], matrix)
    xr_ref[pl.ds(rows, rows), :] = exact_dot(rhs_ref[0], matrix)
    xr_ref[pl.ds(2 * rows, 8), :] = jnp.full((8, LANES), reg_ref[0], F32)
    send_rows(meta, lambda r, n: xr_ref[pl.ds(r, n), :], X_HALO, rows, a_ref, b_ref, 0)
    send_rows(meta, lambda r, n: xr_ref[pl.ds(rows + r, n), :], R_HALO, rows, a_ref, b_ref, X_HALO)


def order_valid(meta_ref, valid_ref, _, __, own_ref, a_ref, b_ref):
    meta = Meta(meta_ref)
    guides, rows = valid_ref.shape[:2]
    matrix = selection(
        (2 * LANES, 2 * LANES),
        lambda s, t: s
        == ((t >> 6) & 1) * LANES + 2 * (t & (HALF - 1)) + (t >= LANES).astype(jnp.int32),
    )
    for q in range((guides + 1) // 2):
        pair = [valid_ref[min(2 * q + k, guides - 1)].astype(F32).astype(BF16) for k in range(2)]
        planes = DOT(jnp.concatenate(pair, axis=1), matrix)
        for t in range(2):
            own_ref[q, t] = planes[:, t * LANES : (t + 1) * LANES]
            own = lambda r, n: own_ref[q, t, pl.ds(r, n), :]
            send_rows(meta, own, V_NEAR, rows, a_ref, b_ref, (2 * q + t) * V_NEAR)


def input_rows(meta, slots, xrs, a_refs, b_refs, q, own_at, at, halo, rows):
    one, two = 2 * q, min(2 * q + 1, slots - 1)

    def of(refs, start):
        def get(t, r, n):
            first, second = refs[one][pl.ds(start + r, n), :], refs[two][pl.ds(start + r, n), :]
            return merge(first, roll(second, HALF)) if t == 0 else merge(roll(first, HALF), second)

        return get

    return rows_with_halo(meta, of(xrs, own_at), of(a_refs, at), of(b_refs, at), 0, halo, rows)


def pair_rows(meta, own_ref, a_ref, b_ref, q, stride, at, skip, halo, rows, size=16):
    return rows_with_halo(
        meta,
        lambda t, r, n: own_ref[q, t, pl.ds(r, n), :],
        lambda t, r, n: a_ref[pl.ds((2 * q + t) * stride + at + r, n), :],
        lambda t, r, n: b_ref[pl.ds((2 * q + t) * stride + at + r, n), :],
        skip, halo, rows, size,
    )


def pack_columns(meta, mask, groups, out_a, out_b):
    base = 0
    for halo, groups_rows in groups:
        low = None
        for r, n, get in groups_rows:
            low = r if low is None else low
            a, b = send_columns(mask, get(0), get(1))
            out_a[pl.ds(base + r - low, n), :] = a
            out_b[pl.ds(base + r - low, n), :] = b
            end = base + r - low + n
        base = end


def pack_inputs(slots, meta_ref, *refs):
    xrs, xa, xb = refs[:slots], refs[slots : 2 * slots], refs[2 * slots : 3 * slots]
    _, _, out_a, out_b = refs[3 * slots :]
    meta = Meta(meta_ref)
    mask = side_mask(meta)
    rows = (xrs[0].shape[0] - 8) // 2
    pairs = range((slots + 1) // 2)
    groups = [(X_HALO, input_rows(meta, slots, xrs, xa, xb, q, 0, 0, X_HALO, rows)) for q in pairs]
    groups += [(R_HALO, input_rows(meta, slots, xrs, xa, xb, q, rows, X_HALO, R_HALO, rows)) for q in pairs]
    pack_columns(meta, mask, groups, out_a, out_b)


def pack_valid(meta_ref, v_ref, va, vb, _, __, v_a, v_b, far_a, far_b):
    meta = Meta(meta_ref)
    mask = side_mask(meta)
    maps, _, rows, _ = v_ref.shape
    pack_columns(
        meta, mask,
        [(V_NEAR, pair_rows(meta, v_ref, va, vb, q, V_NEAR, 0, 0, V_NEAR, rows)) for q in range(maps)],
        v_a, v_b,
    )
    gap = V_HALO - V_NEAR
    odd = meta.gx_odd == 1
    for q in range(maps):
        for t in range(2):
            for r, n in spans(0, gap, 32):
                up = v_ref[q, t, pl.ds(V_NEAR + r, n), :]
                down = v_ref[q, t, pl.ds(rows - V_HALO + r, n), :]
                far_a[pl.ds((2 * q + t) * gap + r, n), :] = jnp.where(odd, up, down)
                far_b[pl.ds((2 * q + t) * gap + r, n), :] = jnp.where(odd, down, up)


def far_rows(meta, fa, fb, q):
    gap = V_HALO - V_NEAR
    odd = meta.gx_odd == 1
    for below in range(2):
        scale = meta.bottom_ok if below else meta.top_ok
        for r, n in spans(0, gap, 16):

            def get(t, r=r, n=n):
                rows_at = pl.ds((2 * q + t) * gap + r, n)
                first, second = (fa, fb) if below == 0 else (fb, fa)
                return jnp.where(odd, first[rows_at, :], second[rows_at, :]) * scale

            yield below * gap + r, n, get


def pack_far(meta_ref, fa, fb, _, __, out_a, out_b):
    meta = Meta(meta_ref)
    mask = side_mask(meta)
    gap = V_HALO - V_NEAR
    for q in range(out_a.shape[0] // (2 * gap)):
        for at, n, get in far_rows(meta, fa, fb, q):
            a, b = send_columns(mask, get(0), get(1))
            out_a[pl.ds(2 * gap * q + at, n), :] = a
            out_b[pl.ds(2 * gap * q + at, n), :] = b


def spread_valid(meta, mask, v_ref, va, vb, near_a, near_b, guides, halo, put):
    maps, _, rows, _ = v_ref.shape
    for q in range(maps):
        for r, n, get in pair_rows(meta, v_ref, va, vb, q, V_NEAR, 0, 0, V_NEAR, rows):
            at = pl.ds((rows + 2 * V_NEAR) * q + r + V_NEAR, n)
            fields = with_columns(meta, mask, get(0), get(1), near_a[at, :], near_b[at, :])
            for k, planes in enumerate(fields[: guides - 2 * q]):
                for t in range(2):
                    put(2 * q + k, t, r + halo, n, planes[t])


def spread_all(meta_ref, v_ref, va, vb, near_a, near_b, fa, fb, far_a, far_b, out_ref):
    meta = Meta(meta_ref)
    mask = side_mask(meta)
    guides = out_ref.shape[0]

    def put(g, t, at, n, value):
        out_ref[g, t, pl.ds(at, n), :] = value

    spread_valid(meta, mask, v_ref, va, vb, near_a, near_b, guides, V_HALO, put)
    maps, _, rows, _ = v_ref.shape
    gap = V_HALO - V_NEAR
    for q in range(maps):
        for at, n, get in far_rows(meta, fa, fb, q):
            rows_at = pl.ds(2 * gap * q + at, n)
            where = at if at < gap else at - gap + V_HALO + rows + V_NEAR
            fields = with_columns(meta, mask, get(0), get(1), far_a[rows_at, :], far_b[rows_at, :])
            for k, planes in enumerate(fields[: guides - 2 * q]):
                for t in range(2):
                    put(2 * q + k, t, where, n, planes[t])


def load_fields(meta, mask, slots, q, rows_iter, a_ref, b_ref, base, shift, x_ref, x_base):
    for r, n, get in rows_iter:
        at = base + r + shift
        fields = with_columns(meta, mask, get(0), get(1), a_ref[pl.ds(at, n), :], b_ref[pl.ds(at, n), :])
        for k, planes in enumerate(fields):
            if 2 * q + k < slots:
                store_field(x_ref, 2 * q + k, r + x_base, n, *planes)


def stage_inputs(slots, meta_ref, table_ref, ga, gb, *refs):
    xrs, xa, xb = refs[:slots], refs[slots : 2 * slots], refs[2 * slots : 3 * slots]
    foot_ref, part_ref, reg_ref, x_ref, g_all, mask_ref = refs[3 * slots :]
    meta = Meta(meta_ref)
    mask = side_mask(meta)
    rows = (xrs[0].shape[0] - 8) // 2
    pairs = (slots + 1) // 2
    x_base = X_HALO + 8
    total = rows + 2 * X_HALO
    total_r = rows + 2 * R_HALO
    for k in range(slots):
        reg_ref[pl.ds(8 * k, 8), :] = xrs[k][pl.ds(2 * rows, 8), :]
        for plane in range(4):
            zero_rows(x_ref, (k, plane), ((0, 8), (total + 8, total + 16)))
    for q in range(pairs):
        load_fields(
            meta, mask, slots, q, input_rows(meta, slots, xrs, xa, xb, q, 0, 0, X_HALO, rows),
            ga, gb, q * total, X_HALO, x_ref, x_base,
        )
    for position in range(mask_ref.shape[0]):
        for r, n in spans(0, rows + 2 * DEPTH1 + 16, 32):
            mask_ref[position, pl.ds(r, n), :] = mask_rows(meta, position, r - DEPTH1 - 8, n, rows)
    guide_loop(
        meta, table_ref, foot_ref.shape[0], slots, (x_ref, x_base),
        p_rows=(-V_NEAR, rows + V_NEAR), footprints=(foot_ref, V_NEAR),
    )
    for k in range(slots):
        bilaplace_into(
            x_ref.at[k], x_base, g_all.at[k], -DEPTH1, rows + DEPTH1,
            lambda r, n: mask_ref[k & 1, pl.ds(r + DEPTH1 + 8, n), :],
        )
    for q in range(pairs):
        base = pairs * total + q * total_r + R_HALO
        for r, n, get in input_rows(meta, slots, xrs, xa, xb, q, rows, X_HALO, R_HALO, rows):
            fields = with_columns(
                meta, mask, get(0), get(1), ga[pl.ds(base + r, n), :], gb[pl.ds(base + r, n), :]
            )
            at = r + DEPTH1 + 8
            for k, planes in enumerate(fields[: slots - 2 * q]):
                slot = 2 * q + k
                weight = reg_ref[pl.ds(8 * slot, 1), :]
                bi = five_point(g_all.at[slot], at, n)[:2]
                for t in range(2):
                    part_ref[slot, t, pl.ds(r + DEPTH1, n), :] = (
                        planes[t] - weight * bi[t] - 0.1 * x_ref[slot, t, pl.ds(r + x_base, n), :]
                    )


def stage_first(slots, meta_ref, table_ref, v_ref, va, vb, na, nb, foot_ref, part_ref, reg_ref, *refs):
    z_ref, out_a, out_b, res_ref, dot_ref = refs[:5]
    m_ref, acc_ref, z_planes, *rest = refs[5:]
    work, masks = rest[:-3], rest[-3:]
    meta = Meta(meta_ref)
    mask = side_mask(meta)
    maps, _, rows, _ = v_ref.shape
    guides = foot_ref.shape[0]
    pairs = (slots + 1) // 2
    m_base, acc_base = V_NEAR + 8, DEPTH1 + 8
    prepare_vcycle(meta, DEPTH1, rows, masks, work)
    for k in range(slots):
        clear_planes(acc_ref, (k,))
    for g in range(guides):
        for plane in range(2):
            zero_rows(m_ref, (g, plane), ((0, 8), (rows + 2 * V_NEAR + 8, rows + 2 * V_NEAR + 16)))

    def put(g, t, at, n, value):
        m_ref[g, t, pl.ds(at + 8, n), :] = value * foot_ref[g, t, pl.ds(at, n), :]

    spread_valid(meta, mask, v_ref, va, vb, na, nb, guides, V_NEAR, put)
    guide_loop(
        meta, table_ref, guides, slots, m=(m_ref, m_base), acc=(acc_ref, acc_base),
        outs=(-DEPTH1, rows + DEPTH1), out_slots=slots,
    )

    def finish_slot(k):
        weight = reg_ref[pl.ds(8 * k, 1), :]
        own_masks = [m.at[k & 1] for m in masks]
        own_work = work[9 * (k & 1) :][:9]
        h_ref = acc_ref.at[k]
        for at, n in spans(8, rows + 2 * DEPTH1 + 8, 16):
            inside = own_masks[0][pl.ds(at, n), :]
            for t in range(2):
                h_ref[t, pl.ds(at, n), :] = inside * (
                    part_ref[k, t, pl.ds(at - 8, n), :] - h_ref[t, pl.ds(at, n), :]
                )
        for t in range(2):
            zero_rows(own_work[0], (t,), ((0, 8), (rows + 2 * DEPTH1 + 8, rows + 2 * DEPTH1 + 16)))
        yield
        yield from vcycle(h_ref, z_planes.at[k], weight, DEPTH1, rows, own_masks, own_work)

    for q in range(pairs):
        in_step(finish_slot(k) for k in range(2 * q, min(2 * q + 2, slots)))
    dots = []
    for q in range(pairs):
        one, two = 2 * q, min(2 * q + 1, slots - 1)
        for r, n in spans(0, rows, 16):
            rows_at = pl.ds(r + DEPTH1 + 8, n)
            for t in range(2):
                z = merge(z_planes[one, t, rows_at, :], z_planes[two, t, rows_at, :])
                res = merge(acc_ref[one, t, rows_at, :], acc_ref[two, t, rows_at, :])
                z_ref[q, t, pl.ds(r, n), :] = z
                if q == 0:
                    res_ref[t, pl.ds(r, n), :] = res
                dots.append(fold(own_lanes(slots, q) * (z * res)))
        for t in range(2):
            send_rows(
                meta, lambda r, n: z_ref[q, t, pl.ds(r, n), :], Z_HALO, rows, out_a, out_b, (2 * q + t) * Z_HALO
            )
    dot_ref[...] = total_of(dots)


def own_lanes(slots, q):
    return 1.0 if 2 * q + 1 < slots else (lane_iota() < HALF).astype(F32)


def pack_second(meta_ref, z_ref, za, zb, _, __, a_ref, b_ref):
    meta = Meta(meta_ref)
    pairs, _, rows, _ = z_ref.shape
    groups = [(Z_HALO, pair_rows(meta, z_ref, za, zb, q, Z_HALO, 0, 0, Z_HALO, rows)) for q in range(pairs)]
    pack_columns(meta, side_mask(meta), groups, a_ref, b_ref)


def stage_second(slots, meta_ref, table_ref, z_ref, reg_ref, valid_ref, za, zb, ga, gb, *refs):
    y_ref, out_a, out_b, image_ref, dot_zq, dot_yq = refs[:6]
    x_ref, m_ref, acc_ref, y_planes, *rest = refs[6:]
    work, masks = rest[:-3], rest[-3:]
    meta = Meta(meta_ref)
    mask = side_mask(meta)
    pairs, _, rows, _ = z_ref.shape
    x_base, m_base, acc_base = Z_HALO, V_HALO + 8, DEPTH2 + 8
    prepare_vcycle(meta, DEPTH2, rows, masks, work)
    total = rows + 2 * Z_HALO
    for q in range(pairs):
        load_fields(
            meta, mask, slots, q, pair_rows(meta, z_ref, za, zb, q, Z_HALO, 0, 0, Z_HALO, rows),
            ga, gb, q * total, Z_HALO, x_ref, x_base,
        )
    for k in range(slots):
        for plane in range(4):
            zero_rows(x_ref, (k, plane), ((total, total + 8),))
        clear_planes(acc_ref, (k,))
    for plane in range(2):
        zero_rows(m_ref, (plane,), ((0, 8), (rows + 2 * V_HALO + 8, rows + 2 * V_HALO + 16)))
    guide_loop(
        meta, table_ref, valid_ref.shape[0], slots,
        (x_ref, x_base), (valid_ref, V_HALO), (m_ref, m_base), (acc_ref, acc_base),
        (-V_HALO, rows + V_HALO), (-DEPTH2, rows + DEPTH2), slots,
    )

    def finish_slot(k):
        weight = reg_ref[pl.ds(8 * k, 1), :]
        own_masks = [m.at[k & 1] for m in masks]
        own_work = work[9 * (k & 1) :][:9]
        g_ref = own_work[0]
        bilaplace_into(
            x_ref.at[k], x_base, g_ref, -DEPTH2, rows + DEPTH2,
            lambda r, n: own_masks[0][pl.ds(r + DEPTH2 + 8, n), :],
        )
        yield
        h_ref = acc_ref.at[k]
        for r, n in spans(-DEPTH2, rows + DEPTH2, 16):
            at = r + DEPTH2 + 8
            bi = five_point(g_ref, at, n)[:2]
            inside = own_masks[0][pl.ds(at, n), :]
            for t in range(2):
                h_ref[t, pl.ds(at, n), :] = inside * (
                    h_ref[t, pl.ds(at, n), :] + weight * bi[t] + 0.1 * x_ref[k, t, pl.ds(r + x_base, n), :]
                )
        for t in range(2):
            zero_rows(g_ref, (t,), ((0, 8), (rows + 2 * DEPTH2 + 8, rows + 2 * DEPTH2 + 16)))
        yield
        yield from vcycle(h_ref, y_planes.at[k], weight, DEPTH2, rows, own_masks, own_work)

    for q in range(pairs):
        in_step(finish_slot(k) for k in range(2 * q, min(2 * q + 2, slots)))
    zq, yq = [], []
    total_y = rows + 2 * Y_HALO
    for q in range(pairs):
        one, two = 2 * q, min(2 * q + 1, slots - 1)
        for r, n in spans(-Y_HALO, rows + Y_HALO, 8):
            rows_at = pl.ds(r + DEPTH2 + 8, n)
            y = [merge(y_planes[one, t, rows_at, :], y_planes[two, t, rows_at, :]) for t in range(2)]
            at = pl.ds(q * total_y + r + Y_HALO, n)
            out_a[at, :], out_b[at, :] = send_columns(mask, *y)
            for t in range(2):
                y_ref[q, t, pl.ds(r + Y_HALO, n), :] = y[t]
                if 0 <= r < rows:
                    image = merge(acc_ref[one, t, rows_at, :], acc_ref[two, t, rows_at, :])
                    z = z_ref[q, t, pl.ds(r, n), :]
                    own = own_lanes(slots, q)
                    zq.append(own * (z * image))
                    yq.append(own * (y[t] * image))
                    if q == 0:
                        image_ref[t, pl.ds(r, n), :] = image
    dot_zq[...], dot_yq[...] = total_of(zq), total_of(yq)


def stage_third(slots, meta_ref, table_ref, y_ref, reg_ref, valid_ref, dot_rz, dot_zq, dot_yq, ga, gb, *refs):
    image_ref, sums_ref, x_ref, m_ref, acc_ref, g_ref, square_ref, mask_ref = refs
    meta = Meta(meta_ref)
    mask = side_mask(meta)
    pairs, _, total, _ = y_ref.shape
    rows = total - 2 * Y_HALO
    x_base, m_base = Y_HALO, 24
    for q in range(pairs):
        load_fields(
            meta, mask, slots, q,
            [(r, n, lambda t, r=r, n=n: y_ref[q, t, pl.ds(r, n), :]) for r, n in spans(0, total, 16)],
            ga, gb, q * total, 0, x_ref, 0,
        )
    for k in range(slots):
        for plane in range(4):
            zero_rows(x_ref, (k, plane), ((total, total + 8),))
    clear_planes(acc_ref, (0,))
    square_ref[...] = jnp.zeros((8, LANES), F32)
    for position in range(mask_ref.shape[0]):
        for r, n in spans(-8, rows + 8, 48):
            mask_ref[position, pl.ds(r + 8, n), :] = mask_rows(meta, position, r, n, rows)
    guide_loop(
        meta, table_ref, valid_ref.shape[0], slots,
        (x_ref, x_base), (valid_ref, V_HALO), (m_ref, m_base), (acc_ref, 0),
        (-24, rows + 24), (0, rows), 1, square_ref=square_ref, rows=rows,
    )
    squares = []
    for k in reversed(range(slots)):
        weight = reg_ref[pl.ds(8 * k, 1), :]
        bilaplace_into(
            x_ref.at[k], x_base, g_ref, 0, rows, lambda r, n: mask_ref[k & 1, pl.ds(r + 8, n), :]
        )
        own = (((lane_iota() - HALF * (k & 1)) & (LANES - 1)) < HALF).astype(F32)
        for r, n in spans(0, rows, 16):
            x = x_ref[k, 0, pl.ds(r + x_base, n), :], x_ref[k, 1, pl.ds(r + x_base, n), :]
            if k == 0:
                bi_even, bi_odd, g_even, g_odd = five_point(g_ref, r + 8, n)
                image_ref[0, pl.ds(r, n), :] = acc_ref[0, 0, pl.ds(r, n), :] + weight * bi_even + 0.1 * x[0]
                image_ref[1, pl.ds(r, n), :] = acc_ref[0, 1, pl.ds(r, n), :] + weight * bi_odd + 0.1 * x[1]
            else:
                g_even, g_odd = g_ref[0, pl.ds(r + 8, n), :], g_ref[1, pl.ds(r + 8, n), :]
            squares.append(
                own * fold(weight * (g_even * g_even + g_odd * g_odd) + 0.1 * (x[0] * x[0] + x[1] * x[1]))
            )
    square_ref[...] += total_of(squares)
    row = lax.broadcasted_iota(jnp.int32, (8, LANES), 0)
    packed = jnp.zeros((8, LANES), F32)
    for at, part in enumerate((dot_rz[...], dot_zq[...], dot_yq[...], square_ref[...])):
        packed = jnp.where(row == at, jnp.sum(part, axis=0, keepdims=True), packed)
    for d in range(sums_ref.shape[0]):
        sums_ref[d] = packed


def finish(start_ref, z_ref, res_ref, q_ref, y_ref, p_ref, sums_ref, solution_ref, residual_ref):
    rows = start_ref.shape[1]
    total = sums_ref[0]
    for d in range(1, sums_ref.shape[0]):
        total = total + sums_ref[d]
    total = jnp.sum(total, axis=1, keepdims=True)
    rz, zq, yq, yp = (total[k : k + 1] for k in range(4))
    alpha = rz / zq
    rz_next = alpha * alpha * yq - rz
    grown = 1.0 + rz_next / rz
    alpha_next = rz_next / (grown * grown * zq - 2.0 * alpha * grown * yq + alpha * alpha * yp)
    matrix = selection(
        (2 * LANES, LANES), lambda s, t: s == (t >> 1) + LANES * (t & 1)
    )
    c_z = alpha + alpha_next * grown
    c_y = alpha_next * alpha
    step, rest = [], []
    for t in range(2):
        step.append(c_z * z_ref[0, t] - c_y * y_ref[0, t, pl.ds(Y_HALO, rows), :])
        rest.append(res_ref[t] - (c_z * q_ref[t] - c_y * p_ref[t]))
    solution_ref[0] = start_ref[0] + exact_dot(jnp.concatenate(step, axis=1), matrix)
    residual_ref[0] = exact_dot(jnp.concatenate(rest, axis=1), matrix)


def call(kernel, outs, *args, scratch=(), scalars=0, unread=0):
    n_in, n_out = len(args), len(outs)
    spaces = [pltpu.SMEM] * scalars + [pltpu.VMEM] * (n_in - scalars - unread) + [pl.ANY] * unread
    return pl.pallas_call(
        kernel,
        out_shape=[jax.ShapeDtypeStruct(shape, F32) for shape in outs],
        in_specs=[pl.BlockSpec(memory_space=space) for space in spaces],
        out_specs=[pl.BlockSpec(memory_space=pltpu.VMEM)] * n_out,
        scratch_shapes=list(scratch),
        compiler_params=pltpu.CompilerParams(vmem_limit_bytes=VMEM_LIMIT),
    )(*args)


def swap(a, b, axis):
    axes = ("layer", "gx", "gy")
    sizes = [lax.axis_size(name) for name in axes]
    moved = axes.index(axis)
    n = sizes[moved]

    def pairs(partner):
        found = []
        for source in np.ndindex(*sizes):
            target = list(source)
            other = partner(source[moved])
            if 0 <= other < n:
                target[moved] = other
            elif source[0] ^ 1 < sizes[0]:
                target[0] ^= 1
            found.append(tuple(int(np.ravel_multi_index(place, sizes)) for place in (source, tuple(target))))
        return found

    return (
        lax.ppermute(a, axes, pairs(lambda i: i ^ 1)),
        lax.ppermute(b, axes, pairs(lambda i: i - 1 if i % 2 == 0 else i + 1)),
    )


def shards(rhs, start, valid, reg, shifts, frac):
    rows = rhs.shape[1]
    guides = valid.shape[0]
    slots = lax.axis_size("layer")
    gx, gy = lax.axis_index("gx"), lax.axis_index("gy")
    n_gx, n_gy = lax.axis_size("gx"), lax.axis_size("gy")
    at = jnp.arange(8, dtype=jnp.int32)
    meta = jnp.zeros((8,), jnp.int32)
    for k, value in enumerate(
        (gx > 0, gx < n_gx - 1, gy > 0, gy < n_gy - 1, lax.axis_index("layer"), gx & 1, gy & 1)
    ):
        meta = jnp.where(at == k, value.astype(jnp.int32), meta)
    table = jnp.concatenate([shifts.reshape(-1), frac.reshape(-1)])
    pairs, maps = (slots + 1) // 2, (guides + 1) // 2
    vmem = lambda *shape: pltpu.VMEM((*shape, LANES), F32)

    strip = (X_HALO + R_HALO, LANES)
    xr, xa, xb = call(order_inputs, ((2 * rows + 8, LANES), strip, strip), meta, reg, start, rhs, scalars=2)
    round_layers = lambda x: [x] + [
        lax.ppermute(x, "layer", [(i, (i + k) % slots) for i in range(slots)]) for k in range(1, slots)
    ]
    xa, xb = swap(xa, xb, "gx")
    xrs = round_layers(xr)
    near, far = (maps * 2 * V_NEAR, LANES), (maps * 2 * (V_HALO - V_NEAR), LANES)
    v_own, va, vb = call(
        order_valid, ((maps, 2, rows, LANES), near, near), meta, valid, xa, xb, scalars=1, unread=2
    )
    va, vb = swap(va, vb, "gx")
    xas, xbs = round_layers(xa), round_layers(xb)
    strip = (2 * pairs * (rows + X_HALO + R_HALO), LANES)
    v_strip = (maps * (rows + 2 * V_NEAR), LANES)
    ga, gb = call(
        functools.partial(pack_inputs, slots), (strip, strip),
        meta, *xrs, *xas, *xbs, table, v_own,
        scalars=1, unread=2,
    )
    ga, gb = swap(ga, gb, "gy")
    na, nb, fa, fb = call(
        pack_valid, (v_strip, v_strip, far, far), meta, v_own, va, vb, ga, gb, scalars=1, unread=2
    )
    na, nb = swap(na, nb, "gy")
    fa, fb = swap(fa, fb, "gx")

    tile = (pairs, 2, rows, LANES)
    size = rows + 2 * DEPTH1 + 16
    positions = min(slots, 2)
    footprints, part, weights = call(
        functools.partial(stage_inputs, slots),
        ((guides, 2, rows + 2 * V_NEAR, LANES), (slots, 2, rows + 2 * DEPTH1, LANES), (8 * slots, LANES)),
        meta, table, ga, gb, *xrs, *xas, *xbs,
        scalars=2,
        scratch=[vmem(slots, 4, rows + 2 * X_HALO + 16), vmem(slots, 2, size), vmem(positions, size)],
    )
    strip = (pairs * 2 * Z_HALO, LANES)
    z, za, zb, res, dot_rz = call(
        functools.partial(stage_first, slots),
        (tile, strip, strip, (2, rows, LANES), (8, LANES)),
        meta, table, v_own, va, vb, na, nb, footprints, part, weights,
        scalars=2,
        scratch=[
            vmem(guides, 2, rows + 2 * V_NEAR + 16),
            vmem(slots, 2, size),
            vmem(slots, 2, size),
            *vcycle_scratch(DEPTH1, rows, slots),
        ],
    )
    ha, hb = call(pack_far, (far, far), meta, fa, fb, z, weights, scalars=1, unread=2)
    za, zb = swap(za, zb, "gx")
    ha, hb = swap(ha, hb, "gy")
    (spread,) = call(
        spread_all,
        ((guides, 2, rows + 2 * V_HALO, LANES),),
        meta, v_own, va, vb, na, nb, fa, fb, ha, hb,
        scalars=1,
    )
    strip = (pairs * (rows + 2 * Z_HALO), LANES)
    ka, kb = call(pack_second, (strip, strip), meta, z, za, zb, ha, hb, scalars=1, unread=2)
    ka, kb = swap(ka, kb, "gy")

    size = rows + 2 * DEPTH2 + 16
    strip = (pairs * (rows + 2 * Y_HALO), LANES)
    y, ya, yb, image, dot_zq, dot_yq = call(
        functools.partial(stage_second, slots),
        ((pairs, 2, rows + 2 * Y_HALO, LANES), strip, strip, (2, rows, LANES), (8, LANES), (8, LANES)),
        meta, table, z, weights, spread, za, zb, ka, kb,
        scalars=2,
        scratch=[
            vmem(slots, 4, rows + 2 * Z_HALO + 8),
            vmem(2, rows + 2 * V_HALO + 16),
            vmem(slots, 2, size),
            vmem(slots, 2, size),
            *vcycle_scratch(DEPTH2, rows, slots),
        ],
    )
    ya, yb = swap(ya, yb, "gy")

    image_y, sums = call(
        functools.partial(stage_third, slots),
        ((2, rows, LANES), (n_gx * n_gy, 8, LANES)),
        meta, table, y, weights, spread, dot_rz, dot_zq, dot_yq, ya, yb,
        scalars=2,
        scratch=[
            vmem(slots, 4, rows + 2 * Y_HALO + 8),
            vmem(2, rows + 48),
            vmem(1, 2, rows),
            vmem(2, rows + 16),
            vmem(8),
            vmem(min(slots, 2), rows + 16),
        ],
    )
    sums = lax.all_to_all(sums, ("gx", "gy"), 0, 0)
    return call(finish, ((1, rows, LANES), (1, rows, LANES)), start, z, res, image, y, image_y, sums)


def solution(mesh):
    in_specs = (
        P("layer", "gx", "gy"),
        P("layer", "gx", "gy"),
        P(None, "gx", "gy"),
        P("layer"),
        P(),
        P(),
    )
    out_specs = (P("layer", "gx", "gy"), P("layer", "gx", "gy"))

    def run(*args):
        return tuple(jax.shard_map(shards, mesh=mesh, in_specs=in_specs, out_specs=out_specs, check_vma=False)(*args))

    return run
```

```python
import functools

import jax
import jax.numpy as jnp
import numpy as np
from jax import lax
from jax.experimental import pallas as pl
from jax.experimental.pallas import tpu as pltpu
from jax.sharding import PartitionSpec as P

GUIDES = 8
SHIFT_MAX = 16
LANES = 128
HALF = LANES // 2
QUART = LANES // 4
F32 = jnp.float32
BF16 = jnp.bfloat16
DOT = functools.partial(jnp.dot, preferred_element_type=F32)

X_HALO, R_HALO, V_HALO, V_NEAR, Z_HALO, Y_HALO = 56, 24, 72, 40, 88, 40
DEPTH1, DEPTH2 = 24, 56
VMEM_LIMIT = 16 << 20


def lane_iota(shape=(1, LANES)):
    return lax.broadcasted_iota(jnp.int32, shape, len(shape) - 1)


def roll(x, amount):
    amount = amount % LANES if isinstance(amount, int) else amount & (LANES - 1)
    if isinstance(amount, int) and amount == 0:
        return x
    return pltpu.roll(x, amount, x.ndim - 1)


def spans(low, high, size):
    return [(r, min(size, high - r)) for r in range(low, high, size)]


class Meta:
    def __init__(self, ref):
        self.top_ok, self.bottom_ok, self.left_ok, self.right_ok = (ref[k].astype(F32) for k in range(4))
        self.layer, self.gx_odd, self.gy_odd = ref[4], ref[5], ref[6]


def exact_dot(values, matrix):
    high = values.astype(BF16)
    rest = values - high.astype(F32)
    mid = rest.astype(BF16)
    low = (rest - mid.astype(F32)).astype(BF16)
    return DOT(high, matrix) + (DOT(mid, matrix) + DOT(low, matrix))


def selection(shape, wanted_of):
    source = lax.broadcasted_iota(jnp.int32, shape, 0)
    target = lax.broadcasted_iota(jnp.int32, shape, 1)
    return wanted_of(source, target).astype(F32).astype(BF16)


def send_rows(meta, own_of, halo, rows, out_a, out_b, base):
    for r, n in spans(0, halo, 32):
        up, down = own_of(r, n), own_of(rows - halo + r, n)
        odd = meta.gx_odd == 1
        out_a[pl.ds(base + r, n), :] = jnp.where(odd, up, down)
        out_b[pl.ds(base + r, n), :] = jnp.where(odd, down, up)


def rows_with_halo(meta, own_of, a_of, b_of, skip, halo, rows, size=16):
    odd = meta.gx_odd == 1
    for r, n in spans(0, halo, size):
        yield r - halo, n, lambda t, r=r, n=n: jnp.where(odd, a_of(t, skip + r, n), b_of(t, skip + r, n)) * meta.top_ok
    for r, n in spans(0, rows, size):
        yield r, n, lambda t, r=r, n=n: own_of(t, r, n)
    for r, n in spans(0, halo, size):
        yield rows + r, n, lambda t, r=r, n=n: jnp.where(odd, b_of(t, r, n), a_of(t, r, n)) * meta.bottom_ok


def side_mask(meta):
    return ((lane_iota() >> 5) & 1) == meta.gy_odd


def send_columns(mask, even, odd):
    moved = roll(odd, -QUART)
    return jnp.where(mask, moved, even), jnp.where(mask, even, moved)


def with_columns(meta, mask, even, odd, from_a, from_b):
    lane = lane_iota()
    near = ((lane >> 5) & 1) == 0
    side_even = jnp.where(mask, from_a, from_b) * jnp.where(near, meta.right_ok, meta.left_ok)
    side_odd = jnp.where(mask, from_b, from_a) * jnp.where(near, meta.left_ok, meta.right_ok)
    side_even, side_odd = roll(side_even, HALF), roll(side_odd, -QUART)
    low = lane < HALF
    return (
        (jnp.where(low, even, side_even), jnp.where(low, odd, side_odd)),
        (jnp.where(low, side_even, even), jnp.where(low, side_odd, odd)),
    )


def merge(first, second):
    return jnp.where(lane_iota() < HALF, first, second)


def rows_of(ref, start):
    return lambda r, n: ref[pl.ds(start + r, n), :]


def five_point(ref, at, n):
    even, odd = ref[0, pl.ds(at, n), :], ref[1, pl.ds(at, n), :]
    sum_even = ref[0, pl.ds(at - 1, n), :] + ref[0, pl.ds(at + 1, n), :] + (odd + roll(odd, 1))
    sum_odd = ref[1, pl.ds(at - 1, n), :] + ref[1, pl.ds(at + 1, n), :] + (even + roll(even, -1))
    return sum_even - 4.0 * even, sum_odd - 4.0 * odd, even, odd


def five_coarse(ref, at, n, step):
    here = ref[pl.ds(at, n), :]
    sides = roll(here, step) + roll(here, -step)
    return ref[pl.ds(at - 1, n), :] + ref[pl.ds(at + 1, n), :] + sides - 4.0 * here, here


def mask_rows(meta, position, row_at, n, rows):
    row = row_at + lax.broadcasted_iota(jnp.int32, (n, LANES), 0)
    lane = (lane_iota((n, LANES)) - HALF * position) & (LANES - 1)
    by_row = jnp.where(row < 0, meta.top_ok, jnp.where(row >= rows, meta.bottom_ok, 1.0))
    return by_row * jnp.where(lane < HALF, 1.0, jnp.where(lane < 3 * QUART, meta.right_ok, meta.left_ok))


def guide_loop(meta, table_ref, guides, slots, x=None, valid=None, m=None, acc=None, p_rows=None, outs=None, out_slots=None, footprints=None, square_ref=None, rows=None):
    def coefficients(g, slot):
        layer = lax.rem(meta.layer - slot + slots, slots)
        at = (g * slots + layer) * 2
        there = guides * slots * 2
        return (
            table_ref[at],
            table_ref[at + 1],
            table_ref[there + at].astype(F32) * (1.0 / 256.0),
            table_ref[there + at + 1].astype(F32) * (1.0 / 256.0),
        )

    def between(ref, index, at, step, n, u):
        here = ref[index + (pl.ds(at, n), slice(None))]
        return here + u * (ref[index + (pl.ds(at + step, n), slice(None))] - here)

    def forward(g):
        home = HALF * (g & 1)
        x_ref, x_base = x
        fixed = []
        for slot in range(slots):
            a, b, u, v = coefficients(g, slot)
            amount = home - HALF * (slot & 1) - lax.shift_right_arithmetic(b, 1)
            fixed.append((a, u, v, b & 1, amount & (LANES - 1)))
        squares = []
        for r, n in spans(*p_rows, 16):
            even = odd = None
            for slot in range(slots):
                a, u, v, parity, amount = fixed[slot]
                c0, c1, c2 = (between(x_ref, (slot, parity + k), r + x_base + a, 1, n, u) for k in range(3))
                this_even = roll(c0 + v * (c1 - c0), amount)
                this_odd = roll(c1 + v * (c2 - c1), amount)
                even = this_even if even is None else even + this_even
                odd = this_odd if odd is None else odd + this_odd
            if footprints is not None:
                out_ref, out_base = footprints
                out_ref[g, 0, pl.ds(r + out_base, n), :] = even
                out_ref[g, 1, pl.ds(r + out_base, n), :] = odd
                continue
            (valid_ref, v_base), (m_ref, m_base) = valid, m
            m_even = even * valid_ref[g, 0, pl.ds(r + v_base, n), :]
            m_odd = odd * valid_ref[g, 1, pl.ds(r + v_base, n), :]
            m_ref[0, pl.ds(r + m_base, n), :] = m_even
            m_ref[1, pl.ds(r + m_base, n), :] = m_odd
            if square_ref is not None:
                for k in range(0, n, 8):
                    if 0 <= r + k < rows:
                        sl = slice(k, k + 8)
                        squares.append(m_even[sl] * even[sl] + m_odd[sl] * odd[sl])
        if squares:
            own = (((lane_iota() - home) & (LANES - 1)) < HALF).astype(F32)
            square_ref[...] += own * total_of(squares)

    def backward(g):
        home = HALF * (g & 1)
        (m_ref, m_base), (acc_ref, acc_base) = m, acc
        lead = () if x is not None else (g,)
        for slot in range(out_slots):
            a, b, u, v = coefficients(g, slot)
            back = -b - 1
            parity = back & 1
            amount = HALF * (slot & 1) - home - lax.shift_right_arithmetic(back, 1)
            for r, n in spans(*outs, 16):
                at = r + m_base - a
                plane_a = between(m_ref, (*lead, parity), at, -1, n, u)
                plane_b = between(m_ref, (*lead, 1 - parity), at, -1, n, u)
                q0, q1, q2 = roll(plane_a, amount), roll(plane_b, amount - parity), roll(plane_a, amount - 1)
                acc_ref[slot, 0, pl.ds(r + acc_base, n), :] += q1 + v * (q0 - q1)
                acc_ref[slot, 1, pl.ds(r + acc_base, n), :] += q2 + v * (q1 - q2)

    def body(g, carry):
        if x is not None:
            forward(g)
        if acc is not None:
            backward(g)
        return carry

    lax.fori_loop(0, guides, body, 0, unroll=4 if x is None or acc is None else 2)


def store_field(x_ref, slot, at, n, even, odd):
    for plane, value in enumerate((even, odd, roll(even, -1), roll(odd, -1))):
        x_ref[slot, plane, pl.ds(at, n), :] = value


def zero_rows(ref, index, ranges):
    for low, high in ranges:
        if high > low:
            ref[index + (pl.ds(low, high - low), slice(None))] = jnp.zeros((high - low, LANES), F32)


def clear_planes(ref, index):
    for plane in range(2):
        for r, n in spans(0, ref.shape[-2], 64):
            ref[index + (plane, pl.ds(r, n), slice(None))] = jnp.zeros((n, LANES), F32)


def vcycle(h_ref, out_ref, weight, depth, rows, masks, work):
    g_ref, w_ref, t_ref, h1, g1, w1, t1, h2, g2 = work
    mask0, mask1, mask2 = masks
    size0 = rows + 2 * depth
    size1, size2 = size0 // 2, size0 // 4
    lane = lane_iota()
    s0 = 0.5 / (4.0 + 20.0 * weight)
    weight1, weight2 = weight * (1.0 / 16.0), weight * (1.0 / 256.0)
    s1 = 0.5 / (4.0 + 20.0 * weight1)
    s2 = 0.5 / (4.0 + 20.0 * weight2)

    for r, n in spans(8, 8 + size0, 16):
        lap_even, lap_odd, _, _ = five_point(h_ref, r, n)
        mask = mask0[pl.ds(r, n), :]
        g_ref[0, pl.ds(r, n), :] = mask * lap_even
        g_ref[1, pl.ds(r, n), :] = mask * lap_odd
    yield
    for r, n in spans(8, 8 + size0, 16):
        bi_even, bi_odd, _, _ = five_point(g_ref, r, n)
        h_both = h_ref[0, pl.ds(r, n), :] + h_ref[1, pl.ds(r, n), :]
        t_ref[pl.ds(r, n), :] = mask0[pl.ds(r, n), :] * (
            h_both - s0 * (4.0 * h_both + weight * (bi_even + bi_odd))
        )
    h1[pl.ds(8, size1), :] = 0.25 * (t_ref[pl.ds(8, size1, stride=2), :] + t_ref[pl.ds(9, size1, stride=2), :])
    yield
    for r, n in spans(8, 8 + size1, 32):
        lap, _ = five_coarse(h1, r, n, 1)
        g1[pl.ds(r, n), :] = mask1[pl.ds(r, n), :] * lap
    yield
    for r, n in spans(8, 8 + size1, 32):
        bi, _ = five_coarse(g1, r, n, 1)
        here = h1[pl.ds(r, n), :]
        t1[pl.ds(r, n), :] = mask1[pl.ds(r, n), :] * (here - s1 * (4.0 * here + weight1 * bi))
    both = t1[pl.ds(8, size2, stride=2), :] + t1[pl.ds(9, size2, stride=2), :]
    h2[pl.ds(8, size2), :] = 0.25 * (both + jnp.where((lane & 1) == 0, roll(both, -1), roll(both, 1)))
    yield
    lap, _ = five_coarse(h2, 8, size2, 2)
    g2[pl.ds(8, size2), :] = mask2[pl.ds(8, size2), :] * lap
    yield
    bi, _ = five_coarse(g2, 8, size2, 2)
    here = h2[pl.ds(8, size2), :]
    e2 = mask2[pl.ds(8, size2), :] * (s2 * (2.0 * here - s2 * (4.0 * here + weight2 * bi)))
    yield
    t1[pl.ds(8, size2, stride=2), :] = e2
    t1[pl.ds(9, size2, stride=2), :] = e2
    yield
    for r, n in spans(8, 8 + size1, 32):
        w1[pl.ds(r, n), :] = s1 * h1[pl.ds(r, n), :] + t1[pl.ds(r, n), :]
    yield
    for r, n in spans(8, 8 + size1, 32):
        lap, _ = five_coarse(w1, r, n, 1)
        g1[pl.ds(r, n), :] = mask1[pl.ds(r, n), :] * lap
    yield
    for r, n in spans(8, 8 + size1, 32):
        bi, _ = five_coarse(g1, r, n, 1)
        here = w1[pl.ds(r, n), :]
        t1[pl.ds(r, n), :] = mask1[pl.ds(r, n), :] * (
            here + s1 * (h1[pl.ds(r, n), :] - 4.0 * here - weight1 * bi)
        )
    e1 = t1[pl.ds(8, size1), :]
    yield
    t_ref[pl.ds(8, size1, stride=2), :] = e1
    t_ref[pl.ds(9, size1, stride=2), :] = e1
    yield
    for r, n in spans(8, 8 + size0, 16):
        copied = t_ref[pl.ds(r, n), :]
        for plane in range(2):
            w_ref[plane, pl.ds(r, n), :] = s0 * h_ref[plane, pl.ds(r, n), :] + copied
    yield
    for r, n in spans(8, 8 + size0, 16):
        lap_even, lap_odd, _, _ = five_point(w_ref, r, n)
        mask = mask0[pl.ds(r, n), :]
        g_ref[0, pl.ds(r, n), :] = mask * lap_even
        g_ref[1, pl.ds(r, n), :] = mask * lap_odd
    yield
    for r, n in spans(8, 8 + size0, 16):
        bi = five_point(g_ref, r, n)[:2]
        mask = mask0[pl.ds(r, n), :]
        for plane in range(2):
            here = w_ref[plane, pl.ds(r, n), :]
            out_ref[plane, pl.ds(r, n), :] = mask * (
                here + s0 * (h_ref[plane, pl.ds(r, n), :] - 4.0 * here - weight * bi[plane])
            )


def in_step(runs):
    runs = list(runs)
    while runs:
        runs = [run for run in runs if next(run, runs) is not runs]


def vcycle_scratch(depth, rows, slots):
    size0 = rows + 2 * depth
    one = lambda size: pltpu.VMEM((size + 16, LANES), F32)
    two = pltpu.VMEM((2, size0 + 16, LANES), F32)
    size1, size2 = size0 // 2, size0 // 4
    work = [two, two, one(size0), one(size1), one(size1), one(size1), one(size1), one(size2), one(size2)]
    positions = min(slots, 2)
    return work * positions + [pltpu.VMEM((positions, size + 16, LANES), F32) for size in (size0, size1, size2)]


def prepare_vcycle(meta, depth, rows, masks, work):
    size0 = rows + 2 * depth
    sizes = (size0, size0 // 2, size0 // 4)
    for level, (mask, size) in enumerate(zip(masks, sizes)):
        for position in range(mask.shape[0]):
            for r, n in spans(0, size + 16, 64):
                mask[position, pl.ds(r, n), :] = mask_rows(
                    meta, position, r - 8 - (depth >> level), n, rows >> level
                )
    for k in range(0, len(work), 9):
        g_ref, w_ref, t_ref, h1, g1, w1, t1, h2, g2 = work[k : k + 9]
        for plane in range(2):
            zero_rows(w_ref, (plane,), ((0, 8), (size0 + 8, size0 + 16)))
        for ref, size in ((h1, sizes[1]), (g1, sizes[1]), (w1, sizes[1]), (h2, sizes[2]), (g2, sizes[2])):
            zero_rows(ref, (), ((0, 8), (size + 8, size + 16)))


def bilaplace_into(x_ref, x_base, g_ref, low, high, mask_of):
    for r, n in spans(low - 8, high + 8, 16):
        lap_even, lap_odd, _, _ = five_point(x_ref, r + x_base, n)
        mask = mask_of(r, n)
        g_ref[0, pl.ds(r - low + 8, n), :] = mask * lap_even
        g_ref[1, pl.ds(r - low + 8, n), :] = mask * lap_odd


def total_of(parts):
    while len(parts) > 1:
        parts = [sum(parts[k : k + 2][1:], parts[k]) for k in range(0, len(parts), 2)]
    return parts[0]


def fold(values):
    return total_of([values[k : k + 8] for k in range(0, values.shape[0], 8)])


def order_inputs(meta_ref, reg_ref, start_ref, rhs_ref, xr_ref, a_ref, b_ref):
    meta = Meta(meta_ref)
    rows = start_ref.shape[1]
    matrix = selection(
        (LANES, LANES), lambda s, t: s == 2 * (t & (HALF - 1)) + (t >= HALF).astype(jnp.int32)
    )
    xr_ref[pl.ds(0, rows), :] = exact_dot(start_ref[0], matrix)
    xr_ref[pl.ds(rows, rows), :] = exact_dot(rhs_ref[0], matrix)
    xr_ref[pl.ds(2 * rows, 8), :] = jnp.full((8, LANES), reg_ref[0], F32)
    send_rows(meta, lambda r, n: xr_ref[pl.ds(r, n), :], X_HALO, rows, a_ref, b_ref, 0)
    send_rows(meta, lambda r, n: xr_ref[pl.ds(rows + r, n), :], R_HALO, rows, a_ref, b_ref, X_HALO)


def order_valid(meta_ref, valid_ref, _, __, own_ref, a_ref, b_ref):
    meta = Meta(meta_ref)
    guides, rows = valid_ref.shape[:2]
    matrix = selection(
        (2 * LANES, 2 * LANES),
        lambda s, t: s
        == ((t >> 6) & 1) * LANES + 2 * (t & (HALF - 1)) + (t >= LANES).astype(jnp.int32),
    )
    for q in range((guides + 1) // 2):
        pair = [valid_ref[min(2 * q + k, guides - 1)].astype(F32).astype(BF16) for k in range(2)]
        planes = DOT(jnp.concatenate(pair, axis=1), matrix)
        for t in range(2):
            own_ref[q, t] = planes[:, t * LANES : (t + 1) * LANES]
            own = lambda r, n: own_ref[q, t, pl.ds(r, n), :]
            send_rows(meta, own, V_NEAR, rows, a_ref, b_ref, (2 * q + t) * V_NEAR)


def input_rows(meta, slots, xrs, a_refs, b_refs, q, own_at, at, halo, rows):
    one, two = 2 * q, min(2 * q + 1, slots - 1)

    def of(refs, start):
        def get(t, r, n):
            first, second = refs[one][pl.ds(start + r, n), :], refs[two][pl.ds(start + r, n), :]
            return merge(first, roll(second, HALF)) if t == 0 else merge(roll(first, HALF), second)

        return get

    return rows_with_halo(meta, of(xrs, own_at), of(a_refs, at), of(b_refs, at), 0, halo, rows)


def pair_rows(meta, own_ref, a_ref, b_ref, q, stride, at, skip, halo, rows, size=16):
    return rows_with_halo(
        meta,
        lambda t, r, n: own_ref[q, t, pl.ds(r, n), :],
        lambda t, r, n: a_ref[pl.ds((2 * q + t) * stride + at + r, n), :],
        lambda t, r, n: b_ref[pl.ds((2 * q + t) * stride + at + r, n), :],
        skip, halo, rows, size,
    )


def pack_columns(meta, mask, groups, out_a, out_b):
    base = 0
    for halo, groups_rows in groups:
        low = None
        for r, n, get in groups_rows:
            low = r if low is None else low
            a, b = send_columns(mask, get(0), get(1))
            out_a[pl.ds(base + r - low, n), :] = a
            out_b[pl.ds(base + r - low, n), :] = b
            end = base + r - low + n
        base = end


def pack_inputs(slots, meta_ref, *refs):
    xrs, xa, xb = refs[:slots], refs[slots : 2 * slots], refs[2 * slots : 3 * slots]
    _, _, out_a, out_b = refs[3 * slots :]
    meta = Meta(meta_ref)
    mask = side_mask(meta)
    rows = (xrs[0].shape[0] - 8) // 2
    pairs = range((slots + 1) // 2)
    groups = [(X_HALO, input_rows(meta, slots, xrs, xa, xb, q, 0, 0, X_HALO, rows)) for q in pairs]
    groups += [(R_HALO, input_rows(meta, slots, xrs, xa, xb, q, rows, X_HALO, R_HALO, rows)) for q in pairs]
    pack_columns(meta, mask, groups, out_a, out_b)


def pack_valid(meta_ref, v_ref, va, vb, _, __, v_a, v_b, far_a, far_b):
    meta = Meta(meta_ref)
    mask = side_mask(meta)
    maps, _, rows, _ = v_ref.shape
    pack_columns(
        meta, mask,
        [(V_NEAR, pair_rows(meta, v_ref, va, vb, q, V_NEAR, 0, 0, V_NEAR, rows)) for q in range(maps)],
        v_a, v_b,
    )
    gap = V_HALO - V_NEAR
    odd = meta.gx_odd == 1
    for q in range(maps):
        for t in range(2):
            for r, n in spans(0, gap, 32):
                up = v_ref[q, t, pl.ds(V_NEAR + r, n), :]
                down = v_ref[q, t, pl.ds(rows - V_HALO + r, n), :]
                far_a[pl.ds((2 * q + t) * gap + r, n), :] = jnp.where(odd, up, down)
                far_b[pl.ds((2 * q + t) * gap + r, n), :] = jnp.where(odd, down, up)


def far_rows(meta, fa, fb, q):
    gap = V_HALO - V_NEAR
    odd = meta.gx_odd == 1
    for below in range(2):
        scale = meta.bottom_ok if below else meta.top_ok
        for r, n in spans(0, gap, 16):

            def get(t, r=r, n=n):
                rows_at = pl.ds((2 * q + t) * gap + r, n)
                first, second = (fa, fb) if below == 0 else (fb, fa)
                return jnp.where(odd, first[rows_at, :], second[rows_at, :]) * scale

            yield below * gap + r, n, get


def pack_far(meta_ref, fa, fb, _, __, out_a, out_b):
    meta = Meta(meta_ref)
    mask = side_mask(meta)
    gap = V_HALO - V_NEAR
    for q in range(out_a.shape[0] // (2 * gap)):
        for at, n, get in far_rows(meta, fa, fb, q):
            a, b = send_columns(mask, get(0), get(1))
            out_a[pl.ds(2 * gap * q + at, n), :] = a
            out_b[pl.ds(2 * gap * q + at, n), :] = b


def spread_valid(meta, mask, v_ref, va, vb, near_a, near_b, guides, halo, put):
    maps, _, rows, _ = v_ref.shape
    for q in range(maps):
        for r, n, get in pair_rows(meta, v_ref, va, vb, q, V_NEAR, 0, 0, V_NEAR, rows):
            at = pl.ds((rows + 2 * V_NEAR) * q + r + V_NEAR, n)
            fields = with_columns(meta, mask, get(0), get(1), near_a[at, :], near_b[at, :])
            for k, planes in enumerate(fields[: guides - 2 * q]):
                for t in range(2):
                    put(2 * q + k, t, r + halo, n, planes[t])


def spread_all(meta_ref, v_ref, va, vb, near_a, near_b, fa, fb, far_a, far_b, out_ref):
    meta = Meta(meta_ref)
    mask = side_mask(meta)
    guides = out_ref.shape[0]

    def put(g, t, at, n, value):
        out_ref[g, t, pl.ds(at, n), :] = value

    spread_valid(meta, mask, v_ref, va, vb, near_a, near_b, guides, V_HALO, put)
    maps, _, rows, _ = v_ref.shape
    gap = V_HALO - V_NEAR
    for q in range(maps):
        for at, n, get in far_rows(meta, fa, fb, q):
            rows_at = pl.ds(2 * gap * q + at, n)
            where = at if at < gap else at - gap + V_HALO + rows + V_NEAR
            fields = with_columns(meta, mask, get(0), get(1), far_a[rows_at, :], far_b[rows_at, :])
            for k, planes in enumerate(fields[: guides - 2 * q]):
                for t in range(2):
                    put(2 * q + k, t, where, n, planes[t])


def load_fields(meta, mask, slots, q, rows_iter, a_ref, b_ref, base, shift, x_ref, x_base):
    for r, n, get in rows_iter:
        at = base + r + shift
        fields = with_columns(meta, mask, get(0), get(1), a_ref[pl.ds(at, n), :], b_ref[pl.ds(at, n), :])
        for k, planes in enumerate(fields):
            if 2 * q + k < slots:
                store_field(x_ref, 2 * q + k, r + x_base, n, *planes)


def stage_inputs(slots, meta_ref, table_ref, ga, gb, *refs):
    xrs, xa, xb = refs[:slots], refs[slots : 2 * slots], refs[2 * slots : 3 * slots]
    foot_ref, part_ref, reg_ref, x_ref, g_all, mask_ref = refs[3 * slots :]
    meta = Meta(meta_ref)
    mask = side_mask(meta)
    rows = (xrs[0].shape[0] - 8) // 2
    pairs = (slots + 1) // 2
    x_base = X_HALO + 8
    total = rows + 2 * X_HALO
    total_r = rows + 2 * R_HALO
    for k in range(slots):
        reg_ref[pl.ds(8 * k, 8), :] = xrs[k][pl.ds(2 * rows, 8), :]
        for plane in range(4):
            zero_rows(x_ref, (k, plane), ((0, 8), (total + 8, total + 16)))
    for q in range(pairs):
        load_fields(
            meta, mask, slots, q, input_rows(meta, slots, xrs, xa, xb, q, 0, 0, X_HALO, rows),
            ga, gb, q * total, X_HALO, x_ref, x_base,
        )
    for position in range(mask_ref.shape[0]):
        for r, n in spans(0, rows + 2 * DEPTH1 + 16, 32):
            mask_ref[position, pl.ds(r, n), :] = mask_rows(meta, position, r - DEPTH1 - 8, n, rows)
    guide_loop(
        meta, table_ref, foot_ref.shape[0], slots, (x_ref, x_base),
        p_rows=(-V_NEAR, rows + V_NEAR), footprints=(foot_ref, V_NEAR),
    )
    for k in range(slots):
        bilaplace_into(
            x_ref.at[k], x_base, g_all.at[k], -DEPTH1, rows + DEPTH1,
            lambda r, n: mask_ref[k & 1, pl.ds(r + DEPTH1 + 8, n), :],
        )
    for q in range(pairs):
        base = pairs * total + q * total_r + R_HALO
        for r, n, get in input_rows(meta, slots, xrs, xa, xb, q, rows, X_HALO, R_HALO, rows):
            fields = with_columns(
                meta, mask, get(0), get(1), ga[pl.ds(base + r, n), :], gb[pl.ds(base + r, n), :]
            )
            at = r + DEPTH1 + 8
            for k, planes in enumerate(fields[: slots - 2 * q]):
                slot = 2 * q + k
                weight = reg_ref[pl.ds(8 * slot, 1), :]
                bi = five_point(g_all.at[slot], at, n)[:2]
                for t in range(2):
                    part_ref[slot, t, pl.ds(r + DEPTH1, n), :] = (
                        planes[t] - weight * bi[t] - 0.1 * x_ref[slot, t, pl.ds(r + x_base, n), :]
                    )


def stage_first(slots, meta_ref, table_ref, v_ref, va, vb, na, nb, foot_ref, part_ref, reg_ref, *refs):
    z_ref, out_a, out_b, res_ref, dot_ref = refs[:5]
    m_ref, acc_ref, z_planes, *rest = refs[5:]
    work, masks = rest[:-3], rest[-3:]
    meta = Meta(meta_ref)
    mask = side_mask(meta)
    maps, _, rows, _ = v_ref.shape
    guides = foot_ref.shape[0]
    pairs = (slots + 1) // 2
    m_base, acc_base = V_NEAR + 8, DEPTH1 + 8
    prepare_vcycle(meta, DEPTH1, rows, masks, work)
    for k in range(slots):
        clear_planes(acc_ref, (k,))
    for g in range(guides):
        for plane in range(2):
            zero_rows(m_ref, (g, plane), ((0, 8), (rows + 2 * V_NEAR + 8, rows + 2 * V_NEAR + 16)))

    def put(g, t, at, n, value):
        m_ref[g, t, pl.ds(at + 8, n), :] = value * foot_ref[g, t, pl.ds(at, n), :]

    spread_valid(meta, mask, v_ref, va, vb, na, nb, guides, V_NEAR, put)
    guide_loop(
        meta, table_ref, guides, slots, m=(m_ref, m_base), acc=(acc_ref, acc_base),
        outs=(-DEPTH1, rows + DEPTH1), out_slots=slots,
    )

    def finish_slot(k):
        weight = reg_ref[pl.ds(8 * k, 1), :]
        own_masks = [m.at[k & 1] for m in masks]
        own_work = work[9 * (k & 1) :][:9]
        h_ref = acc_ref.at[k]
        for at, n in spans(8, rows + 2 * DEPTH1 + 8, 16):
            inside = own_masks[0][pl.ds(at, n), :]
            for t in range(2):
                h_ref[t, pl.ds(at, n), :] = inside * (
                    part_ref[k, t, pl.ds(at - 8, n), :] - h_ref[t, pl.ds(at, n), :]
                )
        for t in range(2):
            zero_rows(own_work[0], (t,), ((0, 8), (rows + 2 * DEPTH1 + 8, rows + 2 * DEPTH1 + 16)))
        yield
        yield from vcycle(h_ref, z_planes.at[k], weight, DEPTH1, rows, own_masks, own_work)

    for q in range(pairs):
        in_step(finish_slot(k) for k in range(2 * q, min(2 * q + 2, slots)))
    dots = []
    for q in range(pairs):
        one, two = 2 * q, min(2 * q + 1, slots - 1)
        for r, n in spans(0, rows, 16):
            rows_at = pl.ds(r + DEPTH1 + 8, n)
            for t in range(2):
                z = merge(z_planes[one, t, rows_at, :], z_planes[two, t, rows_at, :])
                res = merge(acc_ref[one, t, rows_at, :], acc_ref[two, t, rows_at, :])
                z_ref[q, t, pl.ds(r, n), :] = z
                if q == 0:
                    res_ref[t, pl.ds(r, n), :] = res
                dots.append(fold(own_lanes(slots, q) * (z * res)))
        for t in range(2):
            send_rows(
                meta, lambda r, n: z_ref[q, t, pl.ds(r, n), :], Z_HALO, rows, out_a, out_b, (2 * q + t) * Z_HALO
            )
    dot_ref[...] = total_of(dots)


def own_lanes(slots, q):
    return 1.0 if 2 * q + 1 < slots else (lane_iota() < HALF).astype(F32)


def pack_second(meta_ref, z_ref, za, zb, _, __, a_ref, b_ref):
    meta = Meta(meta_ref)
    pairs, _, rows, _ = z_ref.shape
    groups = [(Z_HALO, pair_rows(meta, z_ref, za, zb, q, Z_HALO, 0, 0, Z_HALO, rows)) for q in range(pairs)]
    pack_columns(meta, side_mask(meta), groups, a_ref, b_ref)


def stage_second(slots, meta_ref, table_ref, z_ref, reg_ref, valid_ref, za, zb, ga, gb, *refs):
    y_ref, out_a, out_b, image_ref, dot_zq, dot_yq = refs[:6]
    x_ref, m_ref, acc_ref, y_planes, *rest = refs[6:]
    work, masks = rest[:-3], rest[-3:]
    meta = Meta(meta_ref)
    mask = side_mask(meta)
    pairs, _, rows, _ = z_ref.shape
    x_base, m_base, acc_base = Z_HALO, V_HALO + 8, DEPTH2 + 8
    prepare_vcycle(meta, DEPTH2, rows, masks, work)
    total = rows + 2 * Z_HALO
    for q in range(pairs):
        load_fields(
            meta, mask, slots, q, pair_rows(meta, z_ref, za, zb, q, Z_HALO, 0, 0, Z_HALO, rows),
            ga, gb, q * total, Z_HALO, x_ref, x_base,
        )
    for k in range(slots):
        for plane in range(4):
            zero_rows(x_ref, (k, plane), ((total, total + 8),))
        clear_planes(acc_ref, (k,))
    for plane in range(2):
        zero_rows(m_ref, (plane,), ((0, 8), (rows + 2 * V_HALO + 8, rows + 2 * V_HALO + 16)))
    guide_loop(
        meta, table_ref, valid_ref.shape[0], slots,
        (x_ref, x_base), (valid_ref, V_HALO), (m_ref, m_base), (acc_ref, acc_base),
        (-V_HALO, rows + V_HALO), (-DEPTH2, rows + DEPTH2), slots,
    )

    def finish_slot(k):
        weight = reg_ref[pl.ds(8 * k, 1), :]
        own_masks = [m.at[k & 1] for m in masks]
        own_work = work[9 * (k & 1) :][:9]
        g_ref = own_work[0]
        bilaplace_into(
            x_ref.at[k], x_base, g_ref, -DEPTH2, rows + DEPTH2,
            lambda r, n: own_masks[0][pl.ds(r + DEPTH2 + 8, n), :],
        )
        yield
        h_ref = acc_ref.at[k]
        for r, n in spans(-DEPTH2, rows + DEPTH2, 16):
            at = r + DEPTH2 + 8
            bi = five_point(g_ref, at, n)[:2]
            inside = own_masks[0][pl.ds(at, n), :]
            for t in range(2):
                h_ref[t, pl.ds(at, n), :] = inside * (
                    h_ref[t, pl.ds(at, n), :] + weight * bi[t] + 0.1 * x_ref[k, t, pl.ds(r + x_base, n), :]
                )
        for t in range(2):
            zero_rows(g_ref, (t,), ((0, 8), (rows + 2 * DEPTH2 + 8, rows + 2 * DEPTH2 + 16)))
        yield
        yield from vcycle(h_ref, y_planes.at[k], weight, DEPTH2, rows, own_masks, own_work)

    for q in range(pairs):
        in_step(finish_slot(k) for k in range(2 * q, min(2 * q + 2, slots)))
    zq, yq = [], []
    total_y = rows + 2 * Y_HALO
    for q in range(pairs):
        one, two = 2 * q, min(2 * q + 1, slots - 1)
        for r, n in spans(-Y_HALO, rows + Y_HALO, 8):
            rows_at = pl.ds(r + DEPTH2 + 8, n)
            y = [merge(y_planes[one, t, rows_at, :], y_planes[two, t, rows_at, :]) for t in range(2)]
            at = pl.ds(q * total_y + r + Y_HALO, n)
            out_a[at, :], out_b[at, :] = send_columns(mask, *y)
            for t in range(2):
                y_ref[q, t, pl.ds(r + Y_HALO, n), :] = y[t]
                if 0 <= r < rows:
                    image = merge(acc_ref[one, t, rows_at, :], acc_ref[two, t, rows_at, :])
                    z = z_ref[q, t, pl.ds(r, n), :]
                    own = own_lanes(slots, q)
                    zq.append(own * (z * image))
                    yq.append(own * (y[t] * image))
                    if q == 0:
                        image_ref[t, pl.ds(r, n), :] = image
    dot_zq[...], dot_yq[...] = total_of(zq), total_of(yq)


def stage_third(slots, meta_ref, table_ref, y_ref, reg_ref, valid_ref, dot_rz, dot_zq, dot_yq, ga, gb, *refs):
    image_ref, sums_ref, x_ref, m_ref, acc_ref, g_ref, square_ref, mask_ref = refs
    meta = Meta(meta_ref)
    mask = side_mask(meta)
    pairs, _, total, _ = y_ref.shape
    rows = total - 2 * Y_HALO
    x_base, m_base = Y_HALO, 24
    for q in range(pairs):
        load_fields(
            meta, mask, slots, q,
            [(r, n, lambda t, r=r, n=n: y_ref[q, t, pl.ds(r, n), :]) for r, n in spans(0, total, 16)],
            ga, gb, q * total, 0, x_ref, 0,
        )
    for k in range(slots):
        for plane in range(4):
            zero_rows(x_ref, (k, plane), ((total, total + 8),))
    clear_planes(acc_ref, (0,))
    square_ref[...] = jnp.zeros((8, LANES), F32)
    for position in range(mask_ref.shape[0]):
        for r, n in spans(-8, rows + 8, 48):
            mask_ref[position, pl.ds(r + 8, n), :] = mask_rows(meta, position, r, n, rows)
    guide_loop(
        meta, table_ref, valid_ref.shape[0], slots,
        (x_ref, x_base), (valid_ref, V_HALO), (m_ref, m_base), (acc_ref, 0),
        (-24, rows + 24), (0, rows), 1, square_ref=square_ref, rows=rows,
    )
    squares = []
    for k in reversed(range(slots)):
        weight = reg_ref[pl.ds(8 * k, 1), :]
        bilaplace_into(
            x_ref.at[k], x_base, g_ref, 0, rows, lambda r, n: mask_ref[k & 1, pl.ds(r + 8, n), :]
        )
        own = (((lane_iota() - HALF * (k & 1)) & (LANES - 1)) < HALF).astype(F32)
        for r, n in spans(0, rows, 16):
            x = x_ref[k, 0, pl.ds(r + x_base, n), :], x_ref[k, 1, pl.ds(r + x_base, n), :]
            if k == 0:
                bi_even, bi_odd, g_even, g_odd = five_point(g_ref, r + 8, n)
                image_ref[0, pl.ds(r, n), :] = acc_ref[0, 0, pl.ds(r, n), :] + weight * bi_even + 0.1 * x[0]
                image_ref[1, pl.ds(r, n), :] = acc_ref[0, 1, pl.ds(r, n), :] + weight * bi_odd + 0.1 * x[1]
            else:
                g_even, g_odd = g_ref[0, pl.ds(r + 8, n), :], g_ref[1, pl.ds(r + 8, n), :]
            squares.append(
                own * fold(weight * (g_even * g_even + g_odd * g_odd) + 0.1 * (x[0] * x[0] + x[1] * x[1]))
            )
    square_ref[...] += total_of(squares)
    packed = jnp.zeros((1, LANES), F32)
    for at, part in enumerate((dot_rz[...], dot_zq[...], dot_yq[...], square_ref[...])):
        part = jnp.sum(part, axis=0, keepdims=True)
        part = part + roll(part, HALF)
        part = part + roll(part, QUART)
        packed = jnp.where((lane_iota() >> 5) == at, part, packed)
    for d in range(sums_ref.shape[0]):
        sums_ref[d] = packed


def finish(start_ref, z_ref, res_ref, q_ref, y_ref, p_ref, sums_ref, solution_ref, residual_ref):
    rows = start_ref.shape[1]
    total = sums_ref[0]
    for d in range(1, sums_ref.shape[0]):
        total = total + sums_ref[d]
    rz, zq, yq, yp = (
        jnp.sum(jnp.where((lane_iota() >> 5) == k, total, 0.0), axis=1, keepdims=True) for k in range(4)
    )
    alpha = rz / zq
    rz_next = alpha * alpha * yq - rz
    grown = 1.0 + rz_next / rz
    alpha_next = rz_next / (grown * grown * zq - 2.0 * alpha * grown * yq + alpha * alpha * yp)
    matrix = selection(
        (2 * LANES, LANES), lambda s, t: s == (t >> 1) + LANES * (t & 1)
    )
    c_z = alpha + alpha_next * grown
    c_y = alpha_next * alpha
    step, rest = [], []
    for t in range(2):
        step.append(c_z * z_ref[0, t] - c_y * y_ref[0, t, pl.ds(Y_HALO, rows), :])
        rest.append(res_ref[t] - (c_z * q_ref[t] - c_y * p_ref[t]))
    solution_ref[0] = start_ref[0] + exact_dot(jnp.concatenate(step, axis=1), matrix)
    residual_ref[0] = exact_dot(jnp.concatenate(rest, axis=1), matrix)


def call(kernel, outs, *args, scratch=(), scalars=0, unread=0):
    n_in, n_out = len(args), len(outs)
    spaces = [pltpu.SMEM] * scalars + [pltpu.VMEM] * (n_in - scalars - unread) + [pl.ANY] * unread
    return pl.pallas_call(
        kernel,
        out_shape=[jax.ShapeDtypeStruct(shape, F32) for shape in outs],
        in_specs=[pl.BlockSpec(memory_space=space) for space in spaces],
        out_specs=[pl.BlockSpec(memory_space=pltpu.VMEM)] * n_out,
        scratch_shapes=list(scratch),
        compiler_params=pltpu.CompilerParams(vmem_limit_bytes=VMEM_LIMIT),
    )(*args)


def swap(a, b, axis):
    axes = ("layer", "gx", "gy")
    sizes = [lax.axis_size(name) for name in axes]
    moved = axes.index(axis)
    n = sizes[moved]

    def pairs(partner):
        found = []
        for source in np.ndindex(*sizes):
            target = list(source)
            other = partner(source[moved])
            if 0 <= other < n:
                target[moved] = other
            elif source[0] ^ 1 < sizes[0]:
                target[0] ^= 1
            found.append(tuple(int(np.ravel_multi_index(place, sizes)) for place in (source, tuple(target))))
        return found

    return (
        lax.ppermute(a, axes, pairs(lambda i: i ^ 1)),
        lax.ppermute(b, axes, pairs(lambda i: i - 1 if i % 2 == 0 else i + 1)),
    )


def shards(rhs, start, valid, reg, shifts, frac):
    rows = rhs.shape[1]
    guides = valid.shape[0]
    slots = lax.axis_size("layer")
    gx, gy = lax.axis_index("gx"), lax.axis_index("gy")
    n_gx, n_gy = lax.axis_size("gx"), lax.axis_size("gy")
    at = jnp.arange(8, dtype=jnp.int32)
    meta = jnp.zeros((8,), jnp.int32)
    for k, value in enumerate(
        (gx > 0, gx < n_gx - 1, gy > 0, gy < n_gy - 1, lax.axis_index("layer"), gx & 1, gy & 1)
    ):
        meta = jnp.where(at == k, value.astype(jnp.int32), meta)
    table = jnp.concatenate([shifts.reshape(-1), frac.reshape(-1)])
    pairs, maps = (slots + 1) // 2, (guides + 1) // 2
    vmem = lambda *shape: pltpu.VMEM((*shape, LANES), F32)

    strip = (X_HALO + R_HALO, LANES)
    xr, xa, xb = call(order_inputs, ((2 * rows + 8, LANES), strip, strip), meta, reg, start, rhs, scalars=2)
    round_layers = lambda x: [x] + [
        lax.ppermute(x, "layer", [(i, (i + k) % slots) for i in range(slots)]) for k in range(1, slots)
    ]
    xa, xb = swap(xa, xb, "gx")
    xrs = round_layers(xr)
    near, far = (maps * 2 * V_NEAR, LANES), (maps * 2 * (V_HALO - V_NEAR), LANES)
    v_own, va, vb = call(
        order_valid, ((maps, 2, rows, LANES), near, near), meta, valid, xa, xb, scalars=1, unread=2
    )
    va, vb = swap(va, vb, "gx")
    xas, xbs = round_layers(xa), round_layers(xb)
    strip = (2 * pairs * (rows + X_HALO + R_HALO), LANES)
    v_strip = (maps * (rows + 2 * V_NEAR), LANES)
    ga, gb = call(
        functools.partial(pack_inputs, slots), (strip, strip),
        meta, *xrs, *xas, *xbs, table, v_own,
        scalars=1, unread=2,
    )
    ga, gb = swap(ga, gb, "gy")
    na, nb, fa, fb = call(
        pack_valid, (v_strip, v_strip, far, far), meta, v_own, va, vb, ga, gb, scalars=1, unread=2
    )
    na, nb = swap(na, nb, "gy")
    fa, fb = swap(fa, fb, "gx")

    tile = (pairs, 2, rows, LANES)
    size = rows + 2 * DEPTH1 + 16
    positions = min(slots, 2)
    footprints, part, weights = call(
        functools.partial(stage_inputs, slots),
        ((guides, 2, rows + 2 * V_NEAR, LANES), (slots, 2, rows + 2 * DEPTH1, LANES), (8 * slots, LANES)),
        meta, table, ga, gb, *xrs, *xas, *xbs,
        scalars=2,
        scratch=[vmem(slots, 4, rows + 2 * X_HALO + 16), vmem(slots, 2, size), vmem(positions, size)],
    )
    strip = (pairs * 2 * Z_HALO, LANES)
    z, za, zb, res, dot_rz = call(
        functools.partial(stage_first, slots),
        (tile, strip, strip, (2, rows, LANES), (8, LANES)),
        meta, table, v_own, va, vb, na, nb, footprints, part, weights,
        scalars=2,
        scratch=[
            vmem(guides, 2, rows + 2 * V_NEAR + 16),
            vmem(slots, 2, size),
            vmem(slots, 2, size),
            *vcycle_scratch(DEPTH1, rows, slots),
        ],
    )
    ha, hb = call(pack_far, (far, far), meta, fa, fb, z, weights, scalars=1, unread=2)
    za, zb = swap(za, zb, "gx")
    ha, hb = swap(ha, hb, "gy")
    (spread,) = call(
        spread_all,
        ((guides, 2, rows + 2 * V_HALO, LANES),),
        meta, v_own, va, vb, na, nb, fa, fb, ha, hb,
        scalars=1,
    )
    strip = (pairs * (rows + 2 * Z_HALO), LANES)
    ka, kb = call(pack_second, (strip, strip), meta, z, za, zb, ha, hb, scalars=1, unread=2)
    ka, kb = swap(ka, kb, "gy")

    size = rows + 2 * DEPTH2 + 16
    strip = (pairs * (rows + 2 * Y_HALO), LANES)
    y, ya, yb, image, dot_zq, dot_yq = call(
        functools.partial(stage_second, slots),
        ((pairs, 2, rows + 2 * Y_HALO, LANES), strip, strip, (2, rows, LANES), (8, LANES), (8, LANES)),
        meta, table, z, weights, spread, za, zb, ka, kb,
        scalars=2,
        scratch=[
            vmem(slots, 4, rows + 2 * Z_HALO + 8),
            vmem(2, rows + 2 * V_HALO + 16),
            vmem(slots, 2, size),
            vmem(slots, 2, size),
            *vcycle_scratch(DEPTH2, rows, slots),
        ],
    )
    ya, yb = swap(ya, yb, "gy")

    image_y, sums = call(
        functools.partial(stage_third, slots),
        ((2, rows, LANES), (n_gx * n_gy, 1, LANES)),
        meta, table, y, weights, spread, dot_rz, dot_zq, dot_yq, ya, yb,
        scalars=2,
        scratch=[
            vmem(slots, 4, rows + 2 * Y_HALO + 8),
            vmem(2, rows + 48),
            vmem(1, 2, rows),
            vmem(2, rows + 16),
            vmem(8),
            vmem(min(slots, 2), rows + 16),
        ],
    )
    sums = lax.all_to_all(sums, ("gx", "gy"), 0, 0)
    return call(finish, ((1, rows, LANES), (1, rows, LANES)), start, z, res, image, y, image_y, sums)


def solution(mesh):
    in_specs = (
        P("layer", "gx", "gy"),
        P("layer", "gx", "gy"),
        P(None, "gx", "gy"),
        P("layer"),
        P(),
        P(),
    )
    out_specs = (P("layer", "gx", "gy"), P("layer", "gx", "gy"))

    def run(*args):
        return tuple(jax.shard_map(shards, mesh=mesh, in_specs=in_specs, out_specs=out_specs, check_vma=False)(*args))

    return run
```
